32 devices in a mesh: seq: 8 (over z, y), head: 4 (over x, core).
Axes of the slice: x: 2, y: 2, z: 4, core: 2. Of those that a mesh axis runs over, the one named last changes fastest.
Arguments:
- queries: bfloat16 [1024, 12288], P('seq', 'head'), may hold values from -32 to 32
- keys: bfloat16 [1024, 768], P('seq', 'head'), may hold values from -4 to 4
- values: bfloat16 [1024, 512], P('seq', 'head'), may hold values from -6 to 6
- features: bfloat16 [1024, 2560], P('seq', 'head'), may hold values from -6 to 6
- positions: int32 [1024], P('seq'), may hold values from 0 to 767, as said below
- gate_weight: bfloat16 [2560, 128], replicated, may hold values from -0.125 to 0.125
- key_in: bfloat16 [4, 6144, 128], P('head'), may hold values from -0.078125 to 0.078125
- key_out: bfloat16 [4, 128, 192], P('head'), may hold values from -0.5 to 0.5
- value_in: bfloat16 [4, 4096, 128], P('head'), may hold values from -0.09375 to 0.09375
- value_out: bfloat16 [4, 128, 128], P('head'), may hold values from -0.5 to 0.5
Outputs:
- mixed: bfloat16 [1024, 8192], P('seq', 'head')
The draws below stay inside these ranges and needn't reach their ends.
Inputs may be any that keep to these rules, and one draw needn't show every extreme that they name: positions rise by one from token to token and fall to 0 where one of at most three documents begins inside the slab; the first document began before or at the slab's first token and ends inside the slab.
All inputs are finite; a program needn't handle non-finite values.
Results may differ from the reference program's by a relative error of at most 0.0056.
Values may be sent and summed in bfloat16 or wider, within the bound.
No kernel may reach another device: no remote copies, remote signals or barrier semaphores. Data moves between devices by JAX's collectives and lax.ppermute only.
A program may use at most 64 MiB of HBM per device.

```python
import jax
import jax.numpy as jnp
from jax import lax

D = 2560
QH = 16
DK = 192
DV = 128
CH = 128
STRIDE = 16
BLOCK = 32
WINDOW = 512
TOKENS = 1024
HEADS = 64
CODES = 64
N_HEAD = 4


def key_table(key):
    raw = jax.random.normal(jax.random.fold_in(key, 11), (TOKENS, N_HEAD * DK), jnp.float32)
    return jnp.clip(raw, -4.0, 4.0)


def draw_keys(key, part):
    return key_table(key).astype(jnp.bfloat16)


def draw_queries(key, part):
    raw = jax.random.normal(jax.random.fold_in(key, 23), (TOKENS, N_HEAD * QH * DK), jnp.float32)
    result = jnp.clip(raw, -6.0, 6.0)
    return result.astype(jnp.bfloat16)


def draw_positions(key, part):
    quarter = TOKENS // 4
    offset = jax.random.randint(jax.random.fold_in(key, 41), (), 0, quarter, jnp.int32)
    first_cut = 3 * quarter - offset
    room = TOKENS - first_cut - 1
    extra = jax.random.randint(jax.random.fold_in(key, 43), (2,), 0, 1 << 30, jnp.int32)
    later = first_cut + 1 + extra % room
    cuts = jnp.concatenate([first_cut[None], later], 0)
    token_ids = jnp.arange(TOKENS, dtype=jnp.int32)
    begins = jnp.where(cuts[None, :] <= token_ids[:, None], cuts[None, :], -offset)
    begins = jnp.maximum(jnp.max(begins, axis=1), -offset)
    return (token_ids - begins).astype(jnp.int32)


def block_scale(rng, extent, shards, low, high):
    gain = 1.0
    for axis_at, parts in shards:
        draws = jax.random.uniform(jax.random.fold_in(jax.random.fold_in(rng, 6), axis_at), (parts,), jnp.float32, low / len(shards), high / len(shards))
        gain = gain * jnp.repeat(jnp.exp(draws), extent[axis_at] // parts).reshape((-1,) + (1,) * (len(extent) - 1 - axis_at))
    return gain


def bell_draw(own_key, dims, scale, most, pieces=(), kind=jnp.bfloat16):
    entries = scale * jax.random.normal(own_key, dims, jnp.float32)
    if pieces:
        entries = entries * block_scale(own_key, dims, pieces, -0.22, 0.18)
    return jnp.clip(entries, -most, most).astype(kind)


def setup_inputs(seed: int = 0) -> dict:
    seeds = jax.random.split(jax.random.key(seed), 11)
    queries = draw_queries(jax.random.fold_in(seeds[10], 71), 0)
    keys = draw_keys(jax.random.fold_in(seeds[10], 71), 0)
    values = bell_draw(seeds[2], (TOKENS, N_HEAD * DV), 1.0, 6.0, ((0, 8), (1, 4)))
    features = bell_draw(seeds[3], (TOKENS, D), 1.0, 6.0, ((0, 8), (1, 4)))
    positions = draw_positions(jax.random.fold_in(seeds[10], 71), 0)
    gate_weight = bell_draw(seeds[5], (D, 2 * HEADS), D ** -0.5, 0.125)
    key_in = bell_draw(seeds[6], (N_HEAD, BLOCK * DK, CH), (BLOCK * DK) ** -0.5, 0.078125, ((0, 4),))
    key_out = bell_draw(seeds[7], (N_HEAD, CH, DK), CH ** -0.5, 0.5, ((0, 4),))
    value_in = bell_draw(seeds[8], (N_HEAD, BLOCK * DV, CH), (BLOCK * DV) ** -0.5, 0.09375, ((0, 4),))
    value_out = bell_draw(seeds[9], (N_HEAD, CH, DV), CH ** -0.5, 0.5, ((0, 4),))
    return dict(queries=queries, keys=keys, values=values, features=features, positions=positions, gate_weight=gate_weight, key_in=key_in, key_out=key_out, value_in=value_in, value_out=value_out)


NEG = -1.0e30


def contract(left, right):
    return lax.dot_general(left, right, (((1,), (1,)), ((), ())), preferred_element_type=jnp.float32)


def spread_rows(visible, heads):
    count, width = visible.shape
    return jnp.broadcast_to(visible[:, None, :], (count, heads, width)).reshape(count * heads, width)


def attend(rows, keys_used, values_used, visible):
    scores = contract(rows, keys_used) * (DK ** -0.5)
    top = jnp.max(jnp.where(visible, scores, NEG), axis=1, keepdims=True)
    weights = jnp.where(visible, jnp.exp(scores - top), 0.0)
    total = jnp.sum(weights, axis=1, keepdims=True)
    summed = jnp.dot(weights.astype(jnp.bfloat16), values_used, preferred_element_type=jnp.float32)
    return summed / jnp.maximum(total, 1.0)


def compress(rows, tail, weight_in, weight_out):
    width = rows.shape[1]
    halves = jnp.concatenate([rows, tail], 0).reshape(-1, STRIDE * width)
    split = STRIDE * width
    pre = jnp.dot(halves[:-1], weight_in[:split], preferred_element_type=jnp.float32)
    pre = pre + jnp.dot(halves[1:], weight_in[split:], preferred_element_type=jnp.float32)
    hidden = jax.nn.gelu(pre).astype(jnp.bfloat16)
    return jnp.dot(hidden, weight_out, preferred_element_type=jnp.float32).astype(jnp.bfloat16)


def reference(queries, keys, values, features, positions, gate_weight, key_in, key_out, value_in, value_out):
    token_ids = jnp.arange(TOKENS, dtype=jnp.int32)
    doc_start = token_ids - positions
    logits = jnp.dot(features, gate_weight, preferred_element_type=jnp.float32)
    span = min(512, TOKENS)
    code_ids = jnp.arange(CODES, dtype=jnp.int32)
    results = []
    for group in range(N_HEAD):
        q_group = queries[:, group * QH * DK:(group + 1) * QH * DK]
        k_group = keys[:, group * DK:(group + 1) * DK]
        v_group = values[:, group * DV:(group + 1) * DV]
        code_keys = compress(k_group, jnp.zeros((STRIDE, DK), jnp.bfloat16), key_in[group], key_out[group])
        code_values = compress(v_group, jnp.zeros((STRIDE, DV), jnp.bfloat16), value_in[group], value_out[group])
        padded_keys = jnp.concatenate([jnp.zeros((WINDOW, DK), jnp.bfloat16), k_group], 0)
        padded_values = jnp.concatenate([jnp.zeros((WINDOW, DV), jnp.bfloat16), v_group], 0)
        group_logits = logits[:, group * 2 * QH:(group + 1) * 2 * QH]

        def one_block(block_id):
            start = (block_id * span).astype(jnp.int32)
            rows = lax.dynamic_slice_in_dim(q_group, start, span, 0).reshape(span * QH, DK)
            tokens_here = start + jnp.arange(span, dtype=jnp.int32)
            starts_here = lax.dynamic_slice_in_dim(doc_start, start, span, 0)
            first = STRIDE * code_ids
            seen = (first[None, :] + BLOCK - 1 <= tokens_here[:, None]) & (first[None, :] >= starts_here[:, None])
            coarse = attend(rows, code_keys, code_values, spread_rows(seen, QH))
            near_keys = lax.dynamic_slice_in_dim(padded_keys, start, WINDOW + span, 0)
            near_values = lax.dynamic_slice_in_dim(padded_values, start, WINDOW + span, 0)
            key_ids = start - WINDOW + jnp.arange(WINDOW + span, dtype=jnp.int32)
            near = (key_ids[None, :] >= 0) & (key_ids[None, :] <= tokens_here[:, None])
            near = near & (key_ids[None, :] > tokens_here[:, None] - WINDOW) & (key_ids[None, :] >= starts_here[:, None])
            local = attend(rows, near_keys, near_values, spread_rows(near, QH))
            gates = jax.nn.sigmoid(lax.dynamic_slice_in_dim(group_logits, start, span, 0))
            mixed = gates[:, :QH, None] * coarse.reshape(span, QH, DV) + gates[:, QH:, None] * local.reshape(span, QH, DV)
            return mixed.reshape(span, QH * DV).astype(jnp.bfloat16)

        blocks = lax.map(one_block, jnp.arange(TOKENS // span, dtype=jnp.int32))
        results.append(blocks.reshape(TOKENS, QH * DV))
    return jnp.concatenate(results, 1)
```

```python
import functools

import jax
import jax.numpy as jnp
from jax import lax
from jax.experimental import pallas as pl
from jax.experimental.pallas import tpu as pltpu
from jax.sharding import PartitionSpec as P

QH = 16
DK = 192
DV = 128
STRIDE = 16
BLOCK = 32
WINDOW = 512
LANES = 128
PAD = 256
GROUP = 4

NEG = -1e30
SCALE = DK ** (-0.5) * 1.4426950408889634

f32 = jnp.float32
bf16 = jnp.bfloat16


def up(value, step):
    return -(-value // step) * step


def swap(value, axis, by):
    length = lax.axis_size(axis)
    return lax.ppermute(value, axis, [(i, i ^ by) for i in range(length)])


def turn(value, axis, by):
    length = lax.axis_size(axis)
    return lax.ppermute(value, axis, [(i, (i + by) % length) for i in range(length)])


def dot(left, right):
    return jnp.dot(left, right, preferred_element_type=f32)


def dot_t(left, right):
    return lax.dot_general(left, right, (((1,), (1,)), ((), ())), preferred_element_type=f32)


def logit_kernel(head, features, columns, *outs_and_scratch):
    outs, total = outs_and_scratch[:-1], outs_and_scratch[-1]
    total[...] = lax.dot_general(
        columns[...], features[...], (((0,), (1,)), ((), ())), preferred_element_type=f32
    )
    for step, out in enumerate(outs):
        first = (head[0] ^ step if len(outs) & (len(outs) - 1) == 0 else (head[0] + step) % len(outs)) * (2 * QH)
        out[...] = total[pl.ds(pl.multiple_of(first, 2 * QH), 2 * QH), :]


def gate_logits(features, gate_weight, group, heads):
    count, depth = features.shape
    part = jax.ShapeDtypeStruct((2 * QH, count), f32)
    parts = pl.pallas_call(
        logit_kernel,
        grid_spec=pltpu.PrefetchScalarGridSpec(
            num_scalar_prefetch=1,
            grid=(1,),
            in_specs=[
                pl.BlockSpec((count, depth), lambda i, head: (0, 0)),
                pl.BlockSpec((depth, gate_weight.shape[1]), lambda i, head: (head[0], 0)),
            ],
            out_specs=[pl.BlockSpec((2 * QH, count), lambda i, head: (0, 0))] * heads,
            scratch_shapes=[pltpu.VMEM((gate_weight.shape[1], count), f32)],
        ),
        out_shape=[part] * heads,
        name="gate_logits",
    )(group[None], features, gate_weight)
    if heads & (heads - 1) == 0:
        return [parts[0]] + [swap(parts[d], "head", d) for d in range(1, heads)]
    return [parts[0]] + [turn(parts[d], "head", d) for d in range(1, heads)]


def gelu(x):
    return 0.5 * x * (1.0 + jnp.tanh(0.7978845608028654 * (x + 0.044715 * x * x * x)))


def halves(rows, planes, size, weight, width):
    strides = size // STRIDE
    total = jnp.zeros((strides, 2 * LANES), f32)
    for place in range(STRIDE):
        part = jnp.concatenate(
            [rows[pl.ds(plane * size + place, strides, stride=STRIDE), :] for plane in planes], 1
        ).astype(bf16)[:, :width]
        both = jnp.concatenate(
            [
                weight[pl.ds(place * width, width), :],
                weight[pl.ds((STRIDE + place) * width, width), :],
            ],
            1,
        )
        total = total + dot(part, both)
    return total[:, :LANES], total[:, LANES:]


def hidden_of(first, second):
    strides = first.shape[0]
    later = pltpu.roll(second, strides - 1, axis=0)
    last = lax.broadcasted_iota(jnp.int32, later.shape, 0) == strides - 1
    return gelu(first + jnp.where(last, 0.0, later)).astype(bf16)


def unpack(block, rows, size, at):
    count = block.shape[1]
    for plane in range(2):
        part = block[plane * LANES : min((plane + 1) * LANES, DK), :].astype(f32).T
        rows[pl.ds(plane * size + at, count), : part.shape[1]] = part
    rows[pl.ds(2 * size + at, count), :] = block[DK:, :].astype(f32)


def codes_of(rows, size, key_in, key_out, value_in, value_out):
    key_hidden = hidden_of(*halves(rows, (0, 1), size, key_in, DK))
    code_keys = dot_t(key_out[...], key_hidden).astype(bf16)
    value_hidden = hidden_of(*halves(rows, (2,), size, value_in, DV))
    code_values = dot(value_hidden, value_out[...]).astype(bf16)
    return code_keys, code_values


def attend_body(
    here, count, reach, get_block, code_keys, code_values, codes, positions, q, parts, out, scratch
):
    even, odd, near_values, far_values, near_bias, far_bias, gates = scratch
    near = (reach + 1) * count
    far = even.shape[1] - near
    lengths = jnp.broadcast_to(positions[...].astype(f32), (count, count)).T.astype(jnp.int32)

    def lens(width):
        return jnp.concatenate([lengths] * (width // count), 1) if width > count else lengths

    def ids(width, axis):
        return lax.broadcasted_iota(jnp.int32, (count, width), axis)

    token = here * count + ids(near, 0)
    key = (here - reach) * count + ids(near, 1)
    seen = (key <= token) & (key > token - WINDOW) & (key >= token - lens(near)) & (key >= 0)
    near_bias[...] = jnp.where(seen, 0.0, NEG)
    token = here * count + ids(far, 0)
    first = STRIDE * ids(far, 1)
    seen = (first + (BLOCK - 1) <= token) & (first >= token - lens(far)) & (ids(far, 1) < codes)
    far_bias[...] = jnp.where(seen, 0.0, NEG)
    some = jnp.max(jnp.where(seen, 1.0, 0.0), axis=1, keepdims=True)

    total = parts[0][...]
    for part in parts[1:]:
        total = total + part[...]
    total = jax.nn.sigmoid(total)
    total = jnp.concatenate([total, jnp.zeros((LANES - 2 * QH, count), f32)], 0).T
    coarse_lane = lax.broadcasted_iota(jnp.int32, total.shape, 1) < QH
    gates[...] = jnp.where(coarse_lane, total * some, total)

    even[DK:, :] = jnp.zeros((PAD - DK, near + far), bf16)
    odd[: PAD - DK, :] = jnp.zeros((PAD - DK, near + far), bf16)
    near_values[:, DV:] = jnp.ones((near, DV), bf16)
    far_values[:, DV:] = jnp.ones((far, DV), bf16)
    for step in range(reach + 1):
        block = get_block(jnp.maximum(here - reach + step, 0), step)
        lanes = slice(step * count, (step + 1) * count)
        even[:DK, lanes] = block[:DK, :]
        odd[PAD - DK :, lanes] = block[:DK, :]
        near_values[lanes, :DV] = block[DK:, :]
    even[:DK, near:] = code_keys
    odd[PAD - DK :, near:] = code_keys
    far_values[:, :DV] = code_values

    pair = 2 * DK
    for side in (0, 1):
        keys = (even, odd)[side]
        for chunk in range(0, QH // 2, GROUP):
            rows = jnp.concatenate(
                [
                    q[:, (chunk + j) * pair + side * LANES : (chunk + j) * pair + side * LANES + PAD]
                    for j in range(GROUP)
                ],
                0,
            )
            scores = dot(rows, keys[...])

            def branch(scores, bias, values):
                width = scores.shape[1]
                scores = scores.reshape(GROUP, count, width) + bias[...][None]
                top = jnp.max(scores, axis=2, keepdims=True)
                weights = jnp.exp2((scores - top) * SCALE).astype(bf16)
                summed = dot(weights.reshape(GROUP * count, width), values[...])
                return summed[:, :DV] / jnp.maximum(summed[:, DV:], 1.0)

            local = branch(scores[:, :near], near_bias, near_values)
            coarse = branch(scores[:, near:], far_bias, far_values)
            for j in range(GROUP):
                head = 2 * (chunk + j) + side
                at = slice(j * count, (j + 1) * count)
                mixed = (
                    gates[:, head : head + 1] * coarse[at]
                    + gates[:, QH + head : QH + head + 1] * local[at]
                )
                out[:, head * DV : (head + 1) * DV] = mixed.astype(bf16)


def attend_scratch(count, reach, far):
    near = (reach + 1) * count
    return [
        pltpu.VMEM((PAD, near + far), bf16),
        pltpu.VMEM((PAD, near + far), bf16),
        pltpu.VMEM((near, 2 * DV), bf16),
        pltpu.VMEM((far, 2 * DV), bf16),
        pltpu.VMEM((count, near), f32),
        pltpu.VMEM((count, far), f32),
        pltpu.VMEM((count, LANES), f32),
    ]


def whole_kernel(slots, heads, count, reach, here_ref, *refs):
    positions, q_hbm = refs[:2]
    blocks = refs[2 : 2 + slots]
    weights = refs[2 + slots : 6 + slots]
    parts = refs[6 + slots : 6 + slots + heads]
    out = refs[6 + slots + heads]
    q, held, key_in, key_out, value_in, value_out, rows, sems = refs[
        7 + slots + heads : 15 + slots + heads
    ]
    scratch = refs[15 + slots + heads :]
    here = here_ref[0]
    copies = [
        pltpu.make_async_copy(block, held.at[here ^ d], sems.at[d]) for d, block in enumerate(blocks)
    ]
    places = (key_in, key_out, value_in, value_out)
    copies += [
        pltpu.make_async_copy(source, place, sems.at[slots + i])
        for i, (source, place) in enumerate(zip(weights, places))
    ]
    copies.append(pltpu.make_async_copy(q_hbm, q, sems.at[slots + 4]))
    for copy in copies:
        copy.start()
    for copy in copies[:slots]:
        copy.wait()
    for slot in range(slots):
        unpack(held[slot], rows, slots * count, slot * count)
    for copy in copies[slots:]:
        copy.wait()
    codes = slots * count // STRIDE
    far = up(codes, LANES)
    code_keys, code_values = codes_of(rows, slots * count, key_in, key_out, value_in, value_out)
    if far > codes:
        code_keys = jnp.concatenate([code_keys, jnp.zeros((DK, far - codes), bf16)], 1)
        code_values = jnp.concatenate([code_values, jnp.zeros((far - codes, DV), bf16)], 0)
    attend_body(
        here, count, reach, lambda at, step: held[at], code_keys, code_values, codes,
        positions, q, parts, out, scratch,
    )


def whole_slab(here, positions, queries, blocks, weights, parts, reach):
    count = queries.shape[0]
    slots, heads = len(blocks), len(parts)
    far = up(slots * count // STRIDE, LANES)
    anywhere = pl.BlockSpec(memory_space=pl.ANY)
    vmem = pl.BlockSpec(memory_space=pltpu.VMEM)
    return pl.pallas_call(
        functools.partial(whole_kernel, slots, heads, count, reach),
        in_specs=[pl.BlockSpec(memory_space=pltpu.SMEM), vmem]
        + [anywhere] * (1 + slots + 4)
        + [vmem] * heads,
        out_specs=vmem,
        out_shape=jax.ShapeDtypeStruct((count, QH * DV), bf16),
        scratch_shapes=[
            pltpu.VMEM(queries.shape, bf16),
            pltpu.VMEM((slots, DK + DV, count), bf16),
        ]
        + [pltpu.VMEM(w.shape, bf16) for w in weights]
        + [
            pltpu.VMEM((3 * slots * count, LANES), f32),
            pltpu.SemaphoreType.DMA((slots + 5,)),
        ]
        + attend_scratch(count, reach, far),
        name="whole_slab",
    )(here[None], positions[None, :], queries, *blocks, *weights, *parts)


def codes_kernel(before, block, key_in, key_out, value_in, value_out, out, rows):
    count = block.shape[1]
    unpack(before[...], rows, 2 * count, 0)
    unpack(block[...], rows, 2 * count, count)
    code_keys, code_values = codes_of(rows, 2 * count, key_in, key_out, value_in, value_out)
    out[:, :DK] = code_keys.astype(f32).T
    out[:, DK:] = code_values.astype(f32)


def near_kernel(heads, count, reach, codes, here_ref, *refs):
    positions, q = refs[:2]
    blocks = refs[2 : 3 + reach]
    code_keys, code_values = refs[3 + reach : 5 + reach]
    parts = refs[5 + reach : 5 + reach + heads]
    out = refs[5 + reach + heads]
    attend_body(
        here_ref[0], count, reach, lambda at, step: blocks[step][...], code_keys[...], code_values[...],
        codes, positions, q, parts, out, refs[6 + reach + heads :],
    )


def long_slab(here, positions, queries, block, weights, parts, reach, length):
    count = queries.shape[0]
    strides = count // STRIDE
    smem, vmem = pl.BlockSpec(memory_space=pltpu.SMEM), pl.BlockSpec(memory_space=pltpu.VMEM)
    earlier = [turn(block, "seq", reach - k) for k in range(reach)]
    made = pl.pallas_call(
        codes_kernel,
        in_specs=[vmem] * 6,
        out_specs=vmem,
        out_shape=jax.ShapeDtypeStruct((2 * strides, DK + DV), f32),
        scratch_shapes=[pltpu.VMEM((6 * count, LANES), f32)],
        name="codes",
    )(earlier[-1], block, *weights)
    mine = made[strides - 1 : 2 * strides - 1].astype(bf16)
    every = lax.all_gather(mine, "seq", axis=0, tiled=True)[1:]
    codes = length * count // STRIDE
    far = up(codes, LANES)
    every = jnp.concatenate([every, jnp.zeros((far - every.shape[0], DK + DV), bf16)], 0)
    return pl.pallas_call(
        functools.partial(near_kernel, len(parts), count, reach, codes),
        in_specs=[smem] + [vmem] * (5 + reach + len(parts)),
        out_specs=vmem,
        out_shape=jax.ShapeDtypeStruct((count, QH * DV), bf16),
        scratch_shapes=attend_scratch(count, reach, far),
        name="long_slab",
    )(here[None], positions[None, :], queries, *earlier, block, every[:, :DK].T, every[:, DK:], *parts)


def on_device(
    queries, keys, values, features, positions, gate_weight, key_in, key_out, value_in, value_out
):
    count = keys.shape[0]
    length, heads = lax.axis_size("seq"), lax.axis_size("head")
    here = lax.axis_index("seq")
    group = lax.axis_index("head")
    reach = -(-WINDOW // count)
    block = jnp.concatenate([keys.T, values], 0)
    weights = (key_in[0], key_out[0].T, value_in[0], value_out[0])
    if length != 8:
        parts = gate_logits(features, gate_weight, group, heads)
        return long_slab(here, positions, queries, block, weights, parts, reach, length)
    slots = {0: block, 1: swap(block, "seq", 1)}
    for d in (2, 4, 6):
        slots[d] = swap(block, "seq", d)
    for d in (2, 4, 6):
        slots[d + 1] = swap(slots[d], "seq", 1)
    parts = gate_logits(features, gate_weight, group, heads)
    blocks = [slots[d] for d in range(length)]
    return whole_slab(here, positions, queries, blocks, weights, parts, reach)


def solution(mesh):
    return jax.shard_map(
        on_device,
        mesh=mesh,
        in_specs=(
            P("seq", "head"),
            P("seq", "head"),
            P("seq", "head"),
            P("seq", "head"),
            P("seq"),
            P(),
            P("head", None, None),
            P("head", None, None),
            P("head", None, None),
            P("head", None, None),
        ),
        out_specs=P("seq", "head"),
        check_vma=False,
    )
```

```python
import functools

import jax
import jax.numpy as jnp
from jax import lax
from jax.experimental import pallas as pl
from jax.experimental.pallas import tpu as pltpu
from jax.sharding import PartitionSpec as P

QH = 16
DK = 192
DV = 128
STRIDE = 16
BLOCK = 32
WINDOW = 512
LANES = 128
PAD = 256
GROUP = 4
VMEM_LIMIT = 24 << 20

NEG = -1e30
SCALE = DK ** (-0.5) * 1.4426950408889634

f32 = jnp.float32
bf16 = jnp.bfloat16


def up(value, step):
    return -(-value // step) * step


def swap(value, axis, by):
    length = lax.axis_size(axis)
    return lax.ppermute(value, axis, [(i, i ^ by) for i in range(length)])


def turn(value, axis, by):
    length = lax.axis_size(axis)
    return lax.ppermute(value, axis, [(i, (i + by) % length) for i in range(length)])


def dot(left, right):
    return jnp.dot(left, right, preferred_element_type=f32)


def dot_t(left, right):
    return lax.dot_general(left, right, (((1,), (1,)), ((), ())), preferred_element_type=f32)


def place_vmem(value):
    return pltpu.with_memory_space_constraint(value, pltpu.VMEM)


def place_hbm(value):
    return pltpu.with_memory_space_constraint(value, pltpu.HBM)


def prepare_kernel(heads, kept, group, features_hbm, columns_hbm, *refs):
    sources = refs[:kept]
    outs = refs[kept : kept + heads]
    places = refs[kept + heads : 2 * kept + heads]
    features, columns, total, sems = refs[2 * kept + heads :]
    depth = features.shape[1]
    first = pl.multiple_of(group[0] * depth, LANES)
    copies = [
        pltpu.make_async_copy(features_hbm, features, sems.at[0]),
        pltpu.make_async_copy(columns_hbm.at[pl.ds(first, depth), :], columns, sems.at[1]),
    ]
    copies += [
        pltpu.make_async_copy(source, place, sems.at[2 + i])
        for i, (source, place) in enumerate(zip(sources, places))
    ]
    for copy in copies:
        copy.start()
    copies[0].wait()
    copies[1].wait()
    total[...] = lax.dot_general(
        columns[...], features[...], (((0,), (1,)), ((), ())), preferred_element_type=f32
    )
    for step, out in enumerate(outs):
        other = group[0] ^ step if heads & (heads - 1) == 0 else lax.rem(group[0] + step, heads)
        out[...] = total[pl.ds(pl.multiple_of(other * (2 * QH), 2 * QH), 2 * QH), :]
    for copy in copies[2:]:
        copy.wait()


def prepare(features, gate_weight, group, heads, kept):
    count, depth = features.shape
    columns = gate_weight.shape[1]
    vmem, hbm = pl.BlockSpec(memory_space=pltpu.VMEM), pl.BlockSpec(memory_space=pltpu.HBM)
    made = pl.pallas_call(
        functools.partial(prepare_kernel, heads, len(kept)),
        in_specs=[pl.BlockSpec(memory_space=pltpu.SMEM)] + [hbm] * (2 + len(kept)),
        out_specs=[vmem] * (heads + len(kept)),
        out_shape=[jax.ShapeDtypeStruct((2 * QH, count), f32)] * heads
        + [jax.ShapeDtypeStruct(value.shape, value.dtype) for value in kept],
        scratch_shapes=[
            pltpu.VMEM((count, depth), bf16),
            pltpu.VMEM((depth, columns), bf16),
            pltpu.VMEM((columns, count), f32),
            pltpu.SemaphoreType.DMA((2 + len(kept),)),
        ],
        compiler_params=pltpu.CompilerParams(vmem_limit_bytes=VMEM_LIMIT),
        name="prepare",
    )(group[None], place_hbm(features), place_hbm(gate_weight), *[place_hbm(v) for v in kept])
    return made[:heads], made[heads:]


def exchange(parts):
    heads = len(parts)
    if heads & (heads - 1) == 0:
        return [parts[0]] + [swap(parts[d], "head", d) for d in range(1, heads)]
    return [parts[0]] + [turn(parts[d], "head", d) for d in range(1, heads)]


def gelu(x):
    return 0.5 * x * (1.0 + jnp.tanh(0.7978845608028654 * (x + 0.044715 * x * x * x)))


def halves(rows, planes, size, weight, width):
    strides = size // STRIDE
    total = jnp.zeros((strides, 2 * LANES), f32)
    for place in range(STRIDE):
        part = jnp.concatenate(
            [rows[pl.ds(plane * size + place, strides, stride=STRIDE), :] for plane in planes], 1
        ).astype(bf16)[:, :width]
        both = jnp.concatenate(
            [
                weight[pl.ds(place * width, width), :],
                weight[pl.ds((STRIDE + place) * width, width), :],
            ],
            1,
        )
        total = total + dot(part, both)
    return total[:, :LANES], total[:, LANES:]


def hidden_of(first, second):
    strides = first.shape[0]
    later = pltpu.roll(second, strides - 1, axis=0)
    last = lax.broadcasted_iota(jnp.int32, later.shape, 0) == strides - 1
    return gelu(first + jnp.where(last, 0.0, later)).astype(bf16)


def unpack(block, rows, size, at):
    count = block.shape[1]
    for plane in range(2):
        part = block[plane * LANES : min((plane + 1) * LANES, DK), :].astype(f32).T
        rows[pl.ds(plane * size + at, count), : part.shape[1]] = part
    rows[pl.ds(2 * size + at, count), :] = block[DK:, :].astype(f32)


def codes_of(rows, size, key_in, key_out, value_in, value_out):
    key_hidden = hidden_of(*halves(rows, (0, 1), size, key_in, DK))
    code_keys = dot_t(key_out[...], key_hidden).astype(bf16)
    value_hidden = hidden_of(*halves(rows, (2,), size, value_in, DV))
    code_values = dot(value_hidden, value_out[...]).astype(bf16)
    return code_keys, code_values


def attend_body(
    here, count, reach, get_block, code_keys, code_values, codes, positions, q, parts, out, scratch
):
    even, odd, near_values, far_values, near_bias, far_bias, gates = scratch
    near = (reach + 1) * count
    far = even.shape[1] - near
    lengths = jnp.broadcast_to(positions[...].astype(f32), (count, count)).T.astype(jnp.int32)

    def lens(width):
        return jnp.concatenate([lengths] * (width // count), 1) if width > count else lengths

    def ids(width, axis):
        return lax.broadcasted_iota(jnp.int32, (count, width), axis)

    token = here * count + ids(near, 0)
    key = (here - reach) * count + ids(near, 1)
    seen = (key <= token) & (key > token - WINDOW) & (key >= token - lens(near)) & (key >= 0)
    near_bias[...] = jnp.where(seen, 0.0, NEG)
    token = here * count + ids(far, 0)
    first = STRIDE * ids(far, 1)
    seen = (first + (BLOCK - 1) <= token) & (first >= token - lens(far)) & (ids(far, 1) < codes)
    far_bias[...] = jnp.where(seen, 0.0, NEG)
    some = jnp.max(jnp.where(seen, 1.0, 0.0), axis=1, keepdims=True)

    total = parts[0][...]
    for part in parts[1:]:
        total = total + part[...]
    total = jax.nn.sigmoid(total)
    total = jnp.concatenate([total, jnp.zeros((LANES - 2 * QH, count), f32)], 0).T
    coarse_lane = lax.broadcasted_iota(jnp.int32, total.shape, 1) < QH
    gates[...] = jnp.where(coarse_lane, total * some, total)

    even[DK:, :] = jnp.zeros((PAD - DK, near + far), bf16)
    odd[: PAD - DK, :] = jnp.zeros((PAD - DK, near + far), bf16)
    near_values[:, DV:] = jnp.ones((near, DV), bf16)
    far_values[:, DV:] = jnp.ones((far, DV), bf16)
    for step in range(reach + 1):
        block = get_block(jnp.maximum(here - reach + step, 0), step)
        lanes = slice(step * count, (step + 1) * count)
        even[:DK, lanes] = block[:DK, :]
        odd[PAD - DK :, lanes] = block[:DK, :]
        near_values[lanes, :DV] = block[DK:, :]
    even[:DK, near:] = code_keys
    odd[PAD - DK :, near:] = code_keys
    far_values[:, :DV] = code_values

    pair = 2 * DK
    for side in (0, 1):
        keys = (even, odd)[side]
        for chunk in range(0, QH // 2, GROUP):
            rows = jnp.concatenate(
                [
                    q[:, (chunk + j) * pair + side * LANES : (chunk + j) * pair + side * LANES + PAD]
                    for j in range(GROUP)
                ],
                0,
            )
            scores = dot(rows, keys[...])

            def branch(scores, bias, values):
                width = scores.shape[1]
                scores = scores.reshape(GROUP, count, width) + bias[...][None]
                top = jnp.max(scores, axis=2, keepdims=True)
                weights = jnp.exp2((scores - top) * SCALE).astype(bf16)
                summed = dot(weights.reshape(GROUP * count, width), values[...])
                return summed[:, :DV] / jnp.maximum(summed[:, DV:], 1.0)

            local = branch(scores[:, :near], near_bias, near_values)
            coarse = branch(scores[:, near:], far_bias, far_values)
            for j in range(GROUP):
                head = 2 * (chunk + j) + side
                at = slice(j * count, (j + 1) * count)
                mixed = (
                    gates[:, head : head + 1] * coarse[at]
                    + gates[:, QH + head : QH + head + 1] * local[at]
                )
                out[:, head * DV : (head + 1) * DV] = mixed.astype(bf16)


def attend_scratch(count, reach, far):
    near = (reach + 1) * count
    return [
        pltpu.VMEM((PAD, near + far), bf16),
        pltpu.VMEM((PAD, near + far), bf16),
        pltpu.VMEM((near, 2 * DV), bf16),
        pltpu.VMEM((far, 2 * DV), bf16),
        pltpu.VMEM((count, near), f32),
        pltpu.VMEM((count, far), f32),
        pltpu.VMEM((count, LANES), f32),
    ]


def whole_kernel(slots, heads, count, reach, here_ref, *refs):
    positions, q = refs[:2]
    blocks = refs[2 : 2 + slots]
    weights = refs[2 + slots : 6 + slots]
    parts = refs[6 + slots : 6 + slots + heads]
    out, held, rows, *scratch = refs[6 + slots + heads :]
    here = here_ref[0]
    for slot, block in enumerate(blocks):
        held[here ^ slot] = block[...]
    for slot in range(slots):
        unpack(held[slot], rows, slots * count, slot * count)
    codes = slots * count // STRIDE
    far = up(codes, LANES)
    code_keys, code_values = codes_of(rows, slots * count, *weights)
    if far > codes:
        code_keys = jnp.concatenate([code_keys, jnp.zeros((DK, far - codes), bf16)], 1)
        code_values = jnp.concatenate([code_values, jnp.zeros((far - codes, DV), bf16)], 0)
    attend_body(
        here, count, reach, lambda at, step: held[at], code_keys, code_values, codes,
        positions, q, parts, out, scratch,
    )


def whole_slab(here, positions, queries, blocks, weights, parts, reach):
    count = queries.shape[0]
    slots, heads = len(blocks), len(parts)
    far = up(slots * count // STRIDE, LANES)
    vmem = pl.BlockSpec(memory_space=pltpu.VMEM)
    return pl.pallas_call(
        functools.partial(whole_kernel, slots, heads, count, reach),
        in_specs=[pl.BlockSpec(memory_space=pltpu.SMEM), vmem]
        + [vmem] * (1 + slots + 4)
        + [vmem] * heads,
        out_specs=vmem,
        out_shape=jax.ShapeDtypeStruct((count, QH * DV), bf16),
        scratch_shapes=[
            pltpu.VMEM((slots, DK + DV, count), bf16),
            pltpu.VMEM((3 * slots * count, LANES), f32),
        ]
        + attend_scratch(count, reach, far),
        compiler_params=pltpu.CompilerParams(vmem_limit_bytes=VMEM_LIMIT),
        name="whole_slab",
    )(
        here[None],
        positions[None, :],
        *[place_vmem(value) for value in (queries, *blocks, *weights, *parts)],
    )


def codes_kernel(before, block, key_in, key_out, value_in, value_out, out, rows):
    count = block.shape[1]
    unpack(before[...], rows, 2 * count, 0)
    unpack(block[...], rows, 2 * count, count)
    code_keys, code_values = codes_of(rows, 2 * count, key_in, key_out, value_in, value_out)
    out[:, :DK] = code_keys.astype(f32).T
    out[:, DK:] = code_values.astype(f32)


def near_kernel(heads, count, reach, codes, here_ref, *refs):
    positions, q = refs[:2]
    blocks = refs[2 : 3 + reach]
    code_keys, code_values = refs[3 + reach : 5 + reach]
    parts = refs[5 + reach : 5 + reach + heads]
    out = refs[5 + reach + heads]
    attend_body(
        here_ref[0], count, reach, lambda at, step: blocks[step][...], code_keys[...], code_values[...],
        codes, positions, q, parts, out, refs[6 + reach + heads :],
    )


def long_slab(here, positions, queries, block, weights, parts, reach, length):
    count = queries.shape[0]
    strides = count // STRIDE
    smem, vmem = pl.BlockSpec(memory_space=pltpu.SMEM), pl.BlockSpec(memory_space=pltpu.VMEM)
    earlier = [turn(block, "seq", reach - k) for k in range(reach)]
    made = pl.pallas_call(
        codes_kernel,
        in_specs=[vmem] * 6,
        out_specs=vmem,
        out_shape=jax.ShapeDtypeStruct((2 * strides, DK + DV), f32),
        scratch_shapes=[pltpu.VMEM((6 * count, LANES), f32)],
        name="codes",
    )(earlier[-1], block, *weights)
    mine = made[strides - 1 : 2 * strides - 1].astype(bf16)
    every = lax.all_gather(mine, "seq", axis=0, tiled=True)[1:]
    codes = length * count // STRIDE
    far = up(codes, LANES)
    every = jnp.concatenate([every, jnp.zeros((far - every.shape[0], DK + DV), bf16)], 0)
    return pl.pallas_call(
        functools.partial(near_kernel, len(parts), count, reach, codes),
        in_specs=[smem] + [vmem] * (5 + reach + len(parts)),
        out_specs=vmem,
        out_shape=jax.ShapeDtypeStruct((count, QH * DV), bf16),
        scratch_shapes=attend_scratch(count, reach, far),
        name="long_slab",
    )(here[None], positions[None, :], queries, *earlier, block, every[:, :DK].T, every[:, DK:], *parts)


def on_device(
    queries, keys, values, features, positions, gate_weight, key_in, key_out, value_in, value_out
):
    count = keys.shape[0]
    length, heads = lax.axis_size("seq"), lax.axis_size("head")
    here = lax.axis_index("seq")
    group = lax.axis_index("head")
    reach = -(-WINDOW // count)
    block = jnp.concatenate([keys.T, values], 0)
    weights = (key_in[0], key_out[0].T, value_in[0], value_out[0])
    if length != 8:
        parts = exchange(prepare(features, gate_weight, group, heads, ())[0])
        return long_slab(here, positions, queries, block, weights, parts, reach, length)
    slots = {0: block, 1: swap(block, "seq", 1)}
    for d in (2, 4, 6):
        slots[d] = swap(block, "seq", d)
    parts, (queries, *weights) = prepare(
        features, gate_weight, group, heads, (queries, *weights)
    )
    slots[2], slots[4], slots[6], *parts = lax.optimization_barrier(
        (slots[2], slots[4], slots[6], *parts)
    )
    for d in (2, 4, 6):
        slots[d + 1] = swap(slots[d], "seq", 1)
    parts = exchange(parts)
    blocks = [slots[d] for d in range(length)]
    return whole_slab(here, positions, queries, blocks, weights, parts, reach)


def solution(mesh):
    return jax.shard_map(
        on_device,
        mesh=mesh,
        in_specs=(
            P("seq", "head"),
            P("seq", "head"),
            P("seq", "head"),
            P("seq", "head"),
            P("seq"),
            P(),
            P("head", None, None),
            P("head", None, None),
            P("head", None, None),
            P("head", None, None),
        ),
        out_specs=P("seq", "head"),
        check_vma=False,
    )
```

```python
import functools

import jax
import jax.numpy as jnp
from jax import lax
from jax.experimental import pallas as pl
from jax.experimental.pallas import tpu as pltpu
from jax.sharding import PartitionSpec as P

QH = 16
DK = 192
DV = 128
STRIDE = 16
BLOCK = 32
WINDOW = 512
LANES = 128
PAD = 256
GROUP = 4
VMEM_LIMIT = 24 << 20
MOST_SLOTS = 8

NEG = -1e30
SCALE = DK ** (-0.5) * 1.4426950408889634

f32 = jnp.float32
bf16 = jnp.bfloat16


def up(value, step):
    return -(-value // step) * step


def swap(value, axis, by):
    length = lax.axis_size(axis)
    return lax.ppermute(value, axis, [(i, i ^ by) for i in range(length)])


def turn(value, axis, by):
    length = lax.axis_size(axis)
    return lax.ppermute(value, axis, [(i, (i + by) % length) for i in range(length)])


def dot(left, right):
    return jnp.dot(left, right, preferred_element_type=f32)


def dot_t(left, right):
    return lax.dot_general(left, right, (((1,), (1,)), ((), ())), preferred_element_type=f32)


def place_vmem(value):
    return pltpu.with_memory_space_constraint(value, pltpu.VMEM)


def place_hbm(value):
    return pltpu.with_memory_space_constraint(value, pltpu.HBM)


def logits_of(group, heads, features, columns, total, outs):
    total[...] = lax.dot_general(
        columns[...], features[...], (((0,), (1,)), ((), ())), preferred_element_type=f32
    )
    for step, out in enumerate(outs):
        other = group ^ step if heads & (heads - 1) == 0 else lax.rem(group + step, heads)
        out[...] = total[pl.ds(pl.multiple_of(other * (2 * QH), 2 * QH), 2 * QH), :]


def feature_copies(group, features_hbm, columns_hbm, features, columns, sems):
    depth = features.shape[1]
    first = pl.multiple_of(group * depth, LANES)
    return [
        pltpu.make_async_copy(features_hbm, features, sems.at[0]),
        pltpu.make_async_copy(columns_hbm.at[pl.ds(first, depth), :], columns, sems.at[1]),
    ]


def logit_kernel(heads, group, features_hbm, columns_hbm, *refs):
    outs, (features, columns, total, sems) = refs[:heads], refs[heads:]
    copies = feature_copies(group[0], features_hbm, columns_hbm, features, columns, sems)
    for copy in copies:
        copy.start()
    for copy in copies:
        copy.wait()
    logits_of(group[0], heads, features, columns, total, outs)


def prepare_kernel(heads, kept, offsets, codes, here_ref, group_ref, features_hbm, columns_hbm, positions_hbm, *refs):
    here, group = here_ref[0], group_ref[0]
    sources = refs[:kept]
    outs = refs[kept : kept + heads]
    bias, some, second = refs[kept + heads : kept + heads + 3]
    places = refs[kept + heads + 3 : 2 * kept + heads + 1]
    features, columns, total, positions, sems = refs[2 * kept + heads + 1 :]
    places = [*places, second.at[pl.ds(0, DK), :], second.at[pl.ds(DK, sources[-1].shape[0]), :]]
    copies = feature_copies(group, features_hbm, columns_hbm, features, columns, sems)
    copies.append(pltpu.make_async_copy(positions_hbm, positions, sems.at[2]))
    copies += [
        pltpu.make_async_copy(source, place, sems.at[3 + i])
        for i, (source, place) in enumerate(zip(sources, places))
    ]
    for copy in copies:
        copy.start()
    for copy in copies[:3]:
        copy.wait()
    logits_of(group, heads, features, columns, total, outs)
    count = positions.shape[1]
    lengths = jnp.broadcast_to(positions[...].astype(f32), (count, count)).T.astype(jnp.int32)
    token = here * count + lax.broadcasted_iota(jnp.int32, (count, count), 0)
    lane = lax.broadcasted_iota(jnp.int32, (count, count), 1)
    for step, offset in enumerate(offsets):
        key = (here - offset) * count + lane
        seen = (key <= token) & (key > token - WINDOW) & (key >= token - lengths) & (key >= 0)
        bias[:, step * count : (step + 1) * count] = jnp.where(seen, 0.0, NEG)
    near = len(offsets) * count
    most = jnp.full((count, LANES), NEG, f32)
    for start in range(near, bias.shape[1], LANES):
        code = start - near + lax.broadcasted_iota(jnp.int32, (count, LANES), 1)
        token = here * count + lax.broadcasted_iota(jnp.int32, (count, LANES), 0)
        length = lengths if count == LANES else jnp.broadcast_to(lengths[:, :1], (count, LANES))
        first = STRIDE * code
        seen = (first + (BLOCK - 1) <= token) & (first >= token - length) & (code < codes)
        part = jnp.where(seen, 0.0, NEG)
        bias[:, start : start + LANES] = part
        most = jnp.maximum(most, part)
    some[...] = jnp.where(
        jnp.broadcast_to(jnp.max(most, axis=1, keepdims=True), (count, LANES)) > 0.5 * NEG, 1.0, 0.0
    )
    for copy in copies[3:]:
        copy.wait()


def gate_shapes(count, depth, columns):
    return [
        pltpu.VMEM((count, depth), bf16),
        pltpu.VMEM((depth, columns), bf16),
        pltpu.VMEM((columns, count), f32),
    ]


def gate_logits(features, gate_weight, group, heads):
    count, depth = features.shape
    vmem, hbm = pl.BlockSpec(memory_space=pltpu.VMEM), pl.BlockSpec(memory_space=pltpu.HBM)
    return pl.pallas_call(
        functools.partial(logit_kernel, heads),
        in_specs=[pl.BlockSpec(memory_space=pltpu.SMEM), hbm, hbm],
        out_specs=[vmem] * heads,
        out_shape=[jax.ShapeDtypeStruct((2 * QH, count), f32)] * heads,
        scratch_shapes=gate_shapes(count, depth, gate_weight.shape[1])
        + [pltpu.SemaphoreType.DMA((2,))],
        compiler_params=pltpu.CompilerParams(vmem_limit_bytes=VMEM_LIMIT),
        name="gate_logits",
    )(group[None], features, gate_weight)


def prepare(here, group, positions, features, gate_weight, heads, offsets, codes, kept):
    count, depth = features.shape
    vmem, hbm = pl.BlockSpec(memory_space=pltpu.VMEM), pl.BlockSpec(memory_space=pltpu.HBM)
    wide = len(offsets) * count + up(codes, LANES)
    last = kept[-2:]
    made = pl.pallas_call(
        functools.partial(prepare_kernel, heads, len(kept), offsets, codes),
        in_specs=[pl.BlockSpec(memory_space=pltpu.SMEM)] * 2 + [hbm] * (3 + len(kept)),
        out_specs=[vmem] * (heads + 1 + len(kept)),
        out_shape=[jax.ShapeDtypeStruct((2 * QH, count), f32)] * heads
        + [
            jax.ShapeDtypeStruct((count, wide), f32),
            jax.ShapeDtypeStruct((count, LANES), f32),
            jax.ShapeDtypeStruct((last[0].shape[0] + last[1].shape[0], last[1].shape[1]), bf16),
        ]
        + [jax.ShapeDtypeStruct(value.shape, value.dtype) for value in kept[:-2]],
        scratch_shapes=gate_shapes(count, depth, gate_weight.shape[1])
        + [pltpu.VMEM((1, count), jnp.int32), pltpu.SemaphoreType.DMA((3 + len(kept),))],
        compiler_params=pltpu.CompilerParams(vmem_limit_bytes=VMEM_LIMIT),
        name="prepare",
    )(
        here[None],
        group[None],
        *[place_hbm(value) for value in (features, gate_weight, positions[None, :], *kept)],
    )
    return made[:heads], made[heads:]


def exchange(parts):
    heads = len(parts)
    if heads & (heads - 1) == 0:
        return [parts[0]] + [swap(parts[d], "head", d) for d in range(1, heads)]
    return [parts[0]] + [turn(parts[d], "head", d) for d in range(1, heads)]


def gelu(x):
    return 0.5 * x * (1.0 + jnp.tanh(0.7978845608028654 * (x + 0.044715 * x * x * x)))


def halves(rows, planes, size, weight, width):
    strides = size // STRIDE
    total = jnp.zeros((strides, 2 * LANES), f32)
    for place in range(STRIDE):
        part = jnp.concatenate(
            [rows[pl.ds(plane * size + place, strides, stride=STRIDE), :] for plane in planes], 1
        ).astype(bf16)[:, :width]
        both = jnp.concatenate(
            [
                weight[pl.ds(place * width, width), :],
                weight[pl.ds((STRIDE + place) * width, width), :],
            ],
            1,
        )
        total = total + dot(part, both)
    return total


def hidden_of(first, second):
    strides = first.shape[0]
    later = pltpu.roll(second, strides - 1, axis=0)
    last = lax.broadcasted_iota(jnp.int32, later.shape, 0) == strides - 1
    return gelu(first + jnp.where(last, 0.0, later)).astype(bf16)


def unpack(block, rows, size, at):
    count = block.shape[1]
    for plane in range(2):
        part = block[plane * LANES : min((plane + 1) * LANES, DK), :].astype(f32).T
        rows[pl.ds(plane * size + at, count), : part.shape[1]] = part
    rows[pl.ds(2 * size + at, count), :] = block[DK:, :].astype(f32)


def codes_of(rows, size, key_in, key_out, value_in, value_out):
    shares = halves(rows, (0, 1), size, key_in, DK)
    key_hidden = hidden_of(shares[:, :LANES], shares[:, LANES:])
    code_keys = dot_t(key_out[...], key_hidden).astype(bf16)
    shares = halves(rows, (2,), size, value_in, DV)
    value_hidden = hidden_of(shares[:, :LANES], shares[:, LANES:])
    code_values = dot(value_hidden, value_out[...]).astype(bf16)
    return code_keys, code_values


def attend_body(
    here, count, reach, get_block, code_keys, code_values, codes, positions, q, parts, out, scratch
):
    even, odd, near_values, far_values, near_bias, far_bias, gates = scratch
    near = (reach + 1) * count
    far = even.shape[1] - near
    lengths = jnp.broadcast_to(positions[...].astype(f32), (count, count)).T.astype(jnp.int32)

    def lens(width):
        return jnp.concatenate([lengths] * (width // count), 1) if width > count else lengths

    def ids(width, axis):
        return lax.broadcasted_iota(jnp.int32, (count, width), axis)

    token = here * count + ids(near, 0)
    key = (here - reach) * count + ids(near, 1)
    seen = (key <= token) & (key > token - WINDOW) & (key >= token - lens(near)) & (key >= 0)
    near_bias[...] = jnp.where(seen, 0.0, NEG)
    token = here * count + ids(far, 0)
    first = STRIDE * ids(far, 1)
    seen = (first + (BLOCK - 1) <= token) & (first >= token - lens(far)) & (ids(far, 1) < codes)
    far_bias[...] = jnp.where(seen, 0.0, NEG)
    some = jnp.max(jnp.where(seen, 1.0, 0.0), axis=1, keepdims=True)

    total = parts[0][...]
    for part in parts[1:]:
        total = total + part[...]
    total = jax.nn.sigmoid(total)
    total = jnp.concatenate([total, jnp.zeros((LANES - 2 * QH, count), f32)], 0).T
    coarse_lane = lax.broadcasted_iota(jnp.int32, total.shape, 1) < QH
    gates[...] = jnp.where(coarse_lane, total * some, total)

    even[DK:, :] = jnp.zeros((PAD - DK, near + far), bf16)
    odd[: PAD - DK, :] = jnp.zeros((PAD - DK, near + far), bf16)
    near_values[:, DV:] = jnp.ones((near, DV), bf16)
    far_values[:, DV:] = jnp.ones((far, DV), bf16)
    for step in range(reach + 1):
        block = get_block(jnp.maximum(here - reach + step, 0), step)
        lanes = slice(step * count, (step + 1) * count)
        even[:DK, lanes] = block[:DK, :]
        odd[PAD - DK :, lanes] = block[:DK, :]
        near_values[lanes, :DV] = block[DK:, :]
    even[:DK, near:] = code_keys
    odd[PAD - DK :, near:] = code_keys
    far_values[:, :DV] = code_values

    pair = 2 * DK
    for side in (0, 1):
        keys = (even, odd)[side]
        for chunk in range(0, QH // 2, GROUP):
            rows = jnp.concatenate(
                [
                    q[:, (chunk + j) * pair + side * LANES : (chunk + j) * pair + side * LANES + PAD]
                    for j in range(GROUP)
                ],
                0,
            )
            scores = dot(rows, keys[...])

            def branch(scores, bias, values):
                width = scores.shape[1]
                scores = scores.reshape(GROUP, count, width) + bias[...][None]
                top = jnp.max(scores, axis=2, keepdims=True)
                weights = jnp.exp2((scores - top) * SCALE).astype(bf16)
                summed = dot(weights.reshape(GROUP * count, width), values[...])
                return summed[:, :DV] / jnp.maximum(summed[:, DV:], 1.0)

            local = branch(scores[:, :near], near_bias, near_values)
            coarse = branch(scores[:, near:], far_bias, far_values)
            for j in range(GROUP):
                head = 2 * (chunk + j) + side
                at = slice(j * count, (j + 1) * count)
                mixed = (
                    gates[:, head : head + 1] * coarse[at]
                    + gates[:, QH + head : QH + head + 1] * local[at]
                )
                out[:, head * DV : (head + 1) * DV] = mixed.astype(bf16)


def attend_scratch(count, reach, far):
    near = (reach + 1) * count
    return [
        pltpu.VMEM((PAD, near + far), bf16),
        pltpu.VMEM((PAD, near + far), bf16),
        pltpu.VMEM((near, 2 * DV), bf16),
        pltpu.VMEM((far, 2 * DV), bf16),
        pltpu.VMEM((count, near), f32),
        pltpu.VMEM((count, far), f32),
        pltpu.VMEM((count, LANES), f32),
    ]


def gate_columns(parts, some):
    total = parts[0][...]
    for part in parts[1:]:
        total = total + part[...]
    total = jax.nn.sigmoid(total)
    total = jnp.concatenate([total, jnp.zeros((LANES - 2 * QH, total.shape[1]), f32)], 0).T
    coarse_lane = lax.broadcasted_iota(jnp.int32, total.shape, 1) < QH
    return jnp.where(coarse_lane, total * some, total)


def fill_keys(even, odd, lanes, keys):
    even[:DK, lanes] = keys
    even[DK:, lanes] = jnp.zeros((PAD - DK, keys.shape[1]), bf16)
    odd[: PAD - DK, lanes] = jnp.zeros((PAD - DK, keys.shape[1]), bf16)
    odd[PAD - DK :, lanes] = keys


def query_rows(q, side, chunk):
    starts = [(chunk + j) * 2 * DK + side * LANES for j in range(GROUP)]
    return jnp.concatenate([q[:, start : start + PAD] for start in starts], 0)


def place_of(here, offset):
    block = here - offset
    return jnp.where(block >= 0, (block ^ here) >> 1, 0)


def early_kernel(slots, count, offsets, here_ref, q, bias, key_in, value_in, *refs):
    blocks, (shares, summed, tops) = refs[:slots], refs[slots : slots + 3]
    held, rows, even, odd, values = refs[slots + 3 :]
    here = here_ref[0]
    for i, block in enumerate(blocks):
        held[i] = block[...]
        unpack(block, rows, slots * count, i * count)
    near = len(offsets) * count
    for step, offset in enumerate(offsets):
        block = held[place_of(here, offset)]
        lanes = slice(step * count, (step + 1) * count)
        fill_keys(even, odd, lanes, block[:DK, :])
        values[lanes, :DV] = block[DK:, :]
    values[:, DV:] = jnp.ones((near, DV), bf16)
    shares[:, : 2 * LANES] = halves(rows, (0, 1), slots * count, key_in, DK)
    shares[:, 2 * LANES :] = halves(rows, (2,), slots * count, value_in, DV)
    for side in (0, 1):
        for chunk in range(0, QH // 2, GROUP):
            scores = dot(query_rows(q, side, chunk), (even, odd)[side][...])
            scores = scores.reshape(GROUP, count, near) + bias[:, :near][None]
            top = jnp.max(scores, axis=2, keepdims=True)
            weights = jnp.exp2((scores - top) * SCALE).astype(bf16)
            at = pl.ds((side * QH // 2 + chunk) * count, GROUP * count)
            summed[at, :] = dot(weights.reshape(GROUP * count, near), values[...])
            tops[at, :] = jnp.broadcast_to(top, (GROUP, count, LANES)).reshape(GROUP * count, LANES)


def late_kernel(
    slots, heads, count, offsets, done, here_ref, q, bias, some, second, key_in, value_in, shares, summed, tops, *refs
):
    blocks, parts, out = refs[:slots], refs[slots : slots + heads], refs[slots + heads]
    held, rows, even, odd, values, far_values, key_shares, value_shares, gates = refs[slots + heads + 1 :]
    here = here_ref[0]
    strides = count // STRIDE
    for i, block in enumerate(blocks):
        held[i] = block[...]
        unpack(block, rows, slots * count, i * count)
    near = len(offsets) * count
    for step, offset in enumerate(offsets):
        block = held[place_of(here, offset)]
        lanes = slice(step * count, (step + 1) * count)
        fill_keys(even, odd, lanes, block[:DK, :])
        values[lanes, :DV] = block[DK:, :]
    values[:, DV:] = jnp.ones((near, DV), bf16)
    key_late = halves(rows, (0, 1), slots * count, key_in, DK)
    value_late = halves(rows, (2,), slots * count, value_in, DV)
    for i in range(slots):
        mine = slice(i * strides, (i + 1) * strides)
        at = pl.ds(pl.multiple_of((here ^ (2 * i)) * strides, strides), strides)
        key_shares[at, :] = shares[mine, : 2 * LANES]
        value_shares[at, :] = shares[mine, 2 * LANES :]
        at = pl.ds(pl.multiple_of((here ^ (2 * i + 1)) * strides, strides), strides)
        key_shares[at, :] = key_late[mine]
        value_shares[at, :] = value_late[mine]
    codes = 2 * slots * strides
    far = far_values.shape[0]
    key_hidden = hidden_of(key_shares[:, :LANES], key_shares[:, LANES:])
    code_keys = dot_t(second[:DK, :], key_hidden).astype(bf16)
    value_hidden = hidden_of(value_shares[:, :LANES], value_shares[:, LANES:])
    code_values = dot(value_hidden, second[DK:, :]).astype(bf16)
    if far > codes:
        code_keys = jnp.concatenate([code_keys, jnp.zeros((DK, far - codes), bf16)], 1)
        code_values = jnp.concatenate([code_values, jnp.zeros((far - codes, DV), bf16)], 0)
    fill_keys(even, odd, slice(near, near + far), code_keys)
    far_values[:, :DV] = code_values
    far_values[:, DV:] = jnp.ones((far, DV), bf16)
    gates[...] = gate_columns(parts, some[...])
    size = GROUP * count
    for side in (0, 1):
        for chunk in range(0, QH // 2, GROUP):
            at = pl.ds((side * QH // 2 + chunk) * count, size)
            scores = dot(query_rows(q, side, chunk), (even, odd)[side][...])
            scores = scores.reshape(GROUP, count, near + far) + bias[:, done:][None]
            local, coarse = scores[:, :, :near], scores[:, :, near:]
            before = tops[at, :].reshape(GROUP, count, LANES)
            top = jnp.maximum(before, jnp.max(local, axis=2, keepdims=True))
            tops_near = jnp.concatenate([top] * (near // LANES), 2)
            weights = jnp.exp2((local - tops_near) * SCALE).astype(bf16)
            fade = jnp.exp2((before - top) * SCALE).reshape(size, LANES)
            old = summed[at, :] * jnp.concatenate([fade] * (2 * DV // LANES), 1)
            new = old + dot(weights.reshape(size, near), values[...])
            local = new[:, :DV] / jnp.maximum(new[:, DV:], 1.0)
            top = jnp.max(coarse, axis=2, keepdims=True)
            weights = jnp.exp2((coarse - top) * SCALE).astype(bf16)
            new = dot(weights.reshape(size, far), far_values[...])
            coarse = new[:, :DV] / jnp.maximum(new[:, DV:], 1.0)
            for j in range(GROUP):
                head = 2 * (chunk + j) + side
                mine = slice(j * count, (j + 1) * count)
                mixed = (
                    gates[:, head : head + 1] * coarse[mine]
                    + gates[:, QH + head : QH + head + 1] * local[mine]
                )
                out[:, head * DV : (head + 1) * DV] = mixed.astype(bf16)


def small_slab(here, group, positions, queries, block, features, gate_weight, weights, length, heads, reach):
    count = queries.shape[0]
    codes = length * count // STRIDE
    far = up(codes, LANES)
    first = tuple(range(reach - reach % 2, -1, -2))
    then = tuple(range(reach - (reach + 1) % 2, 0, -2))
    slots = {0: block, 1: swap(block, "seq", 1)}
    later = range(2, length, 2)
    for d in later:
        slots[d] = swap(block, "seq", d)
    key_in, key_out, value_in, value_out = weights
    parts, (bias, some, second, queries, key_in, value_in) = prepare(
        here, group, positions, features, gate_weight, heads, first + then, codes,
        (queries, key_in, value_in, key_out, value_out),
    )
    *came, parts = lax.optimization_barrier((*[slots[d] for d in later], parts))
    for d, value in zip(later, came):
        slots[d] = value
        slots[d + 1] = swap(value, "seq", 1)
    parts = exchange(parts)
    half = length // 2
    smem, vmem = pl.BlockSpec(memory_space=pltpu.SMEM), pl.BlockSpec(memory_space=pltpu.VMEM)
    params = pltpu.CompilerParams(vmem_limit_bytes=VMEM_LIMIT)
    rows = [
        pltpu.VMEM((half, DK + DV, count), bf16),
        pltpu.VMEM((3 * half * count, LANES), f32),
    ]
    near = len(first) * count
    shares, summed, tops = pl.pallas_call(
        functools.partial(early_kernel, half, count, first),
        in_specs=[smem] + [vmem] * (4 + half),
        out_specs=[vmem] * 3,
        out_shape=[
            jax.ShapeDtypeStruct((codes // 2, 4 * LANES), f32),
            jax.ShapeDtypeStruct((QH * count, 2 * DV), f32),
            jax.ShapeDtypeStruct((QH * count, LANES), f32),
        ],
        scratch_shapes=rows
        + [pltpu.VMEM((PAD, near), bf16)] * 2
        + [pltpu.VMEM((near, 2 * DV), bf16)],
        compiler_params=params,
        cost_estimate=pl.CostEstimate(flops=4 << 30, transcendentals=1 << 20, bytes_accessed=1 << 22),
        name="early",
    )(here[None], queries, bias, key_in, value_in, *[slots[d] for d in range(0, length, 2)])
    done = near
    near = len(then) * count
    return pl.pallas_call(
        functools.partial(late_kernel, half, heads, count, then, done),
        in_specs=[smem] + [vmem] * (9 + half + heads),
        out_specs=vmem,
        out_shape=jax.ShapeDtypeStruct((count, QH * DV), bf16),
        scratch_shapes=rows
        + [pltpu.VMEM((PAD, near + far), bf16)] * 2
        + [pltpu.VMEM((near, 2 * DV), bf16), pltpu.VMEM((far, 2 * DV), bf16)]
        + [pltpu.VMEM((codes, 2 * LANES), f32)] * 2
        + [pltpu.VMEM((count, LANES), f32)],
        compiler_params=params,
        name="late",
    )(
        here[None], queries, bias, some, second, key_in, value_in, shares, summed, tops,
        *[slots[d] for d in range(1, length, 2)], *parts,
    )


def codes_kernel(before, block, key_in, key_out, value_in, value_out, out, rows):
    count = block.shape[1]
    unpack(before[...], rows, 2 * count, 0)
    unpack(block[...], rows, 2 * count, count)
    code_keys, code_values = codes_of(rows, 2 * count, key_in, key_out, value_in, value_out)
    out[:, :DK] = code_keys.astype(f32).T
    out[:, DK:] = code_values.astype(f32)


def near_kernel(heads, count, reach, codes, here_ref, *refs):
    positions, q = refs[:2]
    blocks = refs[2 : 3 + reach]
    code_keys, code_values = refs[3 + reach : 5 + reach]
    parts = refs[5 + reach : 5 + reach + heads]
    out = refs[5 + reach + heads]
    attend_body(
        here_ref[0], count, reach, lambda at, step: blocks[step][...], code_keys[...], code_values[...],
        codes, positions, q, parts, out, refs[6 + reach + heads :],
    )


def long_slab(here, positions, queries, block, weights, parts, reach, length):
    count = queries.shape[0]
    strides = count // STRIDE
    smem, vmem = pl.BlockSpec(memory_space=pltpu.SMEM), pl.BlockSpec(memory_space=pltpu.VMEM)
    earlier = [turn(block, "seq", reach - k) for k in range(reach)]
    made = pl.pallas_call(
        codes_kernel,
        in_specs=[vmem] * 6,
        out_specs=vmem,
        out_shape=jax.ShapeDtypeStruct((2 * strides, DK + DV), f32),
        scratch_shapes=[pltpu.VMEM((6 * count, LANES), f32)],
        name="codes",
    )(earlier[-1], block, *weights)
    mine = made[strides - 1 : 2 * strides - 1].astype(bf16)
    every = lax.all_gather(mine, "seq", axis=0, tiled=True)[1:]
    codes = length * count // STRIDE
    far = up(codes, LANES)
    every = jnp.concatenate([every, jnp.zeros((far - every.shape[0], DK + DV), bf16)], 0)
    return pl.pallas_call(
        functools.partial(near_kernel, len(parts), count, reach, codes),
        in_specs=[smem] + [vmem] * (5 + reach + len(parts)),
        out_specs=vmem,
        out_shape=jax.ShapeDtypeStruct((count, QH * DV), bf16),
        scratch_shapes=attend_scratch(count, reach, far),
        name="long_slab",
    )(here[None], positions[None, :], queries, *earlier, block, every[:, :DK].T, every[:, DK:], *parts)


def on_device(
    queries, keys, values, features, positions, gate_weight, key_in, key_out, value_in, value_out
):
    count = keys.shape[0]
    length, heads = lax.axis_size("seq"), lax.axis_size("head")
    here = lax.axis_index("seq")
    group = lax.axis_index("head")
    reach = -(-WINDOW // count)
    block = jnp.concatenate([keys.T, values], 0)
    weights = (key_in[0], key_out[0].T, value_in[0], value_out[0])
    if length <= MOST_SLOTS and length > 1 and length & (length - 1) == 0:
        return small_slab(
            here, group, positions, queries, block, features, gate_weight, weights, length, heads, reach
        )
    parts = exchange(gate_logits(features, gate_weight, group, heads))
    return long_slab(here, positions, queries, block, weights, parts, reach, length)


def solution(mesh):
    return jax.shard_map(
        on_device,
        mesh=mesh,
        in_specs=(
            P("seq", "head"),
            P("seq", "head"),
            P("seq", "head"),
            P("seq", "head"),
            P("seq"),
            P(),
            P("head", None, None),
            P("head", None, None),
            P("head", None, None),
            P("head", None, None),
        ),
        out_specs=P("seq", "head"),
        check_vma=False,
    )
```

```python
import functools

import jax
import jax.numpy as jnp
from jax import lax
from jax.experimental import pallas as pl
from jax.experimental.pallas import tpu as pltpu
from jax.sharding import PartitionSpec as P

QH = 16
DK = 192
DV = 128
STRIDE = 16
BLOCK = 32
WINDOW = 512
LANES = 128
PAD = 256
GROUP = 4
VMEM_LIMIT = 24 << 20
MOST_SLOTS = 8

NEG = -1e30
SCALE = DK ** (-0.5) * 1.4426950408889634

f32 = jnp.float32
bf16 = jnp.bfloat16


def up(value, step):
    return -(-value // step) * step


def swap(value, axis, by):
    length = lax.axis_size(axis)
    return lax.ppermute(value, axis, [(i, i ^ by) for i in range(length)])


def turn(value, axis, by):
    length = lax.axis_size(axis)
    return lax.ppermute(value, axis, [(i, (i + by) % length) for i in range(length)])


def dot(left, right):
    return jnp.dot(left, right, preferred_element_type=f32)


def dot_t(left, right):
    return lax.dot_general(left, right, (((1,), (1,)), ((), ())), preferred_element_type=f32)


def place_vmem(value):
    return pltpu.with_memory_space_constraint(value, pltpu.VMEM)


def place_hbm(value):
    return pltpu.with_memory_space_constraint(value, pltpu.HBM)


def logits_of(group, heads, features, columns, total, outs):
    total[...] = lax.dot_general(
        columns[...], features[...], (((0,), (1,)), ((), ())), preferred_element_type=f32
    )
    for step, out in enumerate(outs):
        other = group ^ step if heads & (heads - 1) == 0 else lax.rem(group + step, heads)
        out[...] = total[pl.ds(pl.multiple_of(other * (2 * QH), 2 * QH), 2 * QH), :]


def feature_copies(group, features_hbm, columns_hbm, features, columns, sems):
    depth = features.shape[1]
    first = pl.multiple_of(group * depth, LANES)
    return [
        pltpu.make_async_copy(features_hbm, features, sems.at[0]),
        pltpu.make_async_copy(columns_hbm.at[pl.ds(first, depth), :], columns, sems.at[1]),
    ]


def logit_kernel(heads, group, features_hbm, columns_hbm, *refs):
    outs, (features, columns, total, sems) = refs[:heads], refs[heads:]
    copies = feature_copies(group[0], features_hbm, columns_hbm, features, columns, sems)
    for copy in copies:
        copy.start()
    for copy in copies:
        copy.wait()
    logits_of(group[0], heads, features, columns, total, outs)


def prepare_kernel(heads, kept, offsets, codes, here_ref, group_ref, features_hbm, columns_hbm, positions_hbm, *refs):
    here, group = here_ref[0], group_ref[0]
    sources = refs[:kept]
    outs = refs[kept : kept + heads]
    bias, some, second = refs[kept + heads : kept + heads + 3]
    places = refs[kept + heads + 3 : 2 * kept + heads + 1]
    features, columns, total, positions, sems = refs[2 * kept + heads + 1 :]
    places = [*places, second.at[pl.ds(0, DK), :], second.at[pl.ds(DK, sources[-1].shape[0]), :]]
    copies = feature_copies(group, features_hbm, columns_hbm, features, columns, sems)
    copies.append(pltpu.make_async_copy(positions_hbm, positions, sems.at[2]))
    copies += [
        pltpu.make_async_copy(source, place, sems.at[3 + i])
        for i, (source, place) in enumerate(zip(sources, places))
    ]
    for copy in copies:
        copy.start()
    for copy in copies[:3]:
        copy.wait()
    logits_of(group, heads, features, columns, total, outs)
    count = positions.shape[1]
    lengths = jnp.broadcast_to(positions[...].astype(f32), (count, count)).T.astype(jnp.int32)
    token = here * count + lax.broadcasted_iota(jnp.int32, (count, count), 0)
    lane = lax.broadcasted_iota(jnp.int32, (count, count), 1)
    for step, offset in enumerate(offsets):
        key = (here - offset) * count + lane
        seen = (key <= token) & (key > token - WINDOW) & (key >= token - lengths) & (key >= 0)
        bias[:, step * count : (step + 1) * count] = jnp.where(seen, 0.0, NEG)
    near = len(offsets) * count
    most = jnp.full((count, LANES), NEG, f32)
    for start in range(near, bias.shape[1], LANES):
        code = start - near + lax.broadcasted_iota(jnp.int32, (count, LANES), 1)
        token = here * count + lax.broadcasted_iota(jnp.int32, (count, LANES), 0)
        length = lengths if count == LANES else jnp.broadcast_to(lengths[:, :1], (count, LANES))
        first = STRIDE * code
        seen = (first + (BLOCK - 1) <= token) & (first >= token - length) & (code < codes)
        part = jnp.where(seen, 0.0, NEG)
        bias[:, start : start + LANES] = part
        most = jnp.maximum(most, part)
    some[...] = jnp.where(
        jnp.broadcast_to(jnp.max(most, axis=1, keepdims=True), (count, LANES)) > 0.5 * NEG, 1.0, 0.0
    )
    for copy in copies[3:]:
        copy.wait()


def gate_shapes(count, depth, columns):
    return [
        pltpu.VMEM((count, depth), bf16),
        pltpu.VMEM((depth, columns), bf16),
        pltpu.VMEM((columns, count), f32),
    ]


def gate_logits(features, gate_weight, group, heads):
    count, depth = features.shape
    vmem, hbm = pl.BlockSpec(memory_space=pltpu.VMEM), pl.BlockSpec(memory_space=pltpu.HBM)
    return pl.pallas_call(
        functools.partial(logit_kernel, heads),
        in_specs=[pl.BlockSpec(memory_space=pltpu.SMEM), hbm, hbm],
        out_specs=[vmem] * heads,
        out_shape=[jax.ShapeDtypeStruct((2 * QH, count), f32)] * heads,
        scratch_shapes=gate_shapes(count, depth, gate_weight.shape[1])
        + [pltpu.SemaphoreType.DMA((2,))],
        compiler_params=pltpu.CompilerParams(vmem_limit_bytes=VMEM_LIMIT),
        name="gate_logits",
    )(group[None], features, gate_weight)


def prepare(here, group, positions, features, gate_weight, heads, offsets, codes, kept):
    count, depth = features.shape
    vmem, hbm = pl.BlockSpec(memory_space=pltpu.VMEM), pl.BlockSpec(memory_space=pltpu.HBM)
    wide = len(offsets) * count + up(codes, LANES)
    last = kept[-2:]
    made = pl.pallas_call(
        functools.partial(prepare_kernel, heads, len(kept), offsets, codes),
        in_specs=[pl.BlockSpec(memory_space=pltpu.SMEM)] * 2 + [hbm] * (3 + len(kept)),
        out_specs=[vmem] * (heads + 1 + len(kept)),
        out_shape=[jax.ShapeDtypeStruct((2 * QH, count), f32)] * heads
        + [
            jax.ShapeDtypeStruct((count, wide), f32),
            jax.ShapeDtypeStruct((count, LANES), f32),
            jax.ShapeDtypeStruct((last[0].shape[0] + last[1].shape[0], last[1].shape[1]), bf16),
        ]
        + [jax.ShapeDtypeStruct(value.shape, value.dtype) for value in kept[:-2]],
        scratch_shapes=gate_shapes(count, depth, gate_weight.shape[1])
        + [pltpu.VMEM((1, count), jnp.int32), pltpu.SemaphoreType.DMA((3 + len(kept),))],
        compiler_params=pltpu.CompilerParams(vmem_limit_bytes=VMEM_LIMIT),
        name="prepare",
    )(
        here[None],
        group[None],
        *[place_hbm(value) for value in (features, gate_weight, positions[None, :], *kept)],
    )
    return made[:heads], made[heads:]


def exchange(parts):
    heads = len(parts)
    if heads & (heads - 1) == 0:
        return [parts[0]] + [swap(parts[d], "head", d) for d in range(1, heads)]
    return [parts[0]] + [turn(parts[d], "head", d) for d in range(1, heads)]


def gelu(x):
    return 0.5 * x * (1.0 + jnp.tanh(0.7978845608028654 * (x + 0.044715 * x * x * x)))


def halves(rows, planes, size, weight, width):
    strides = size // STRIDE
    total = jnp.zeros((strides, 2 * LANES), f32)
    for place in range(STRIDE):
        part = jnp.concatenate(
            [rows[pl.ds(plane * size + place, strides, stride=STRIDE), :] for plane in planes], 1
        ).astype(bf16)[:, :width]
        both = jnp.concatenate(
            [
                weight[pl.ds(place * width, width), :],
                weight[pl.ds((STRIDE + place) * width, width), :],
            ],
            1,
        )
        total = total + dot(part, both)
    return total


def hidden_of(first, second):
    strides = first.shape[0]
    later = pltpu.roll(second, strides - 1, axis=0)
    last = lax.broadcasted_iota(jnp.int32, later.shape, 0) == strides - 1
    return gelu(first + jnp.where(last, 0.0, later)).astype(bf16)


def unpack(block, rows, size, at):
    count = block.shape[1]
    for plane in range(2):
        part = block[plane * LANES : min((plane + 1) * LANES, DK), :].astype(f32).T
        rows[pl.ds(plane * size + at, count), : part.shape[1]] = part
    rows[pl.ds(2 * size + at, count), :] = block[DK:, :].astype(f32)


def codes_of(rows, size, key_in, key_out, value_in, value_out):
    shares = halves(rows, (0, 1), size, key_in, DK)
    key_hidden = hidden_of(shares[:, :LANES], shares[:, LANES:])
    code_keys = dot_t(key_out[...], key_hidden).astype(bf16)
    shares = halves(rows, (2,), size, value_in, DV)
    value_hidden = hidden_of(shares[:, :LANES], shares[:, LANES:])
    code_values = dot(value_hidden, value_out[...]).astype(bf16)
    return code_keys, code_values


def attend_body(
    here, count, reach, get_block, code_keys, code_values, codes, positions, q, parts, out, scratch
):
    even, odd, near_values, far_values, near_bias, far_bias, gates = scratch
    near = (reach + 1) * count
    far = even.shape[1] - near
    lengths = jnp.broadcast_to(positions[...].astype(f32), (count, count)).T.astype(jnp.int32)

    def lens(width):
        return jnp.concatenate([lengths] * (width // count), 1) if width > count else lengths

    def ids(width, axis):
        return lax.broadcasted_iota(jnp.int32, (count, width), axis)

    token = here * count + ids(near, 0)
    key = (here - reach) * count + ids(near, 1)
    seen = (key <= token) & (key > token - WINDOW) & (key >= token - lens(near)) & (key >= 0)
    near_bias[...] = jnp.where(seen, 0.0, NEG)
    token = here * count + ids(far, 0)
    first = STRIDE * ids(far, 1)
    seen = (first + (BLOCK - 1) <= token) & (first >= token - lens(far)) & (ids(far, 1) < codes)
    far_bias[...] = jnp.where(seen, 0.0, NEG)
    some = jnp.max(jnp.where(seen, 1.0, 0.0), axis=1, keepdims=True)

    total = parts[0][...]
    for part in parts[1:]:
        total = total + part[...]
    total = jax.nn.sigmoid(total)
    total = jnp.concatenate([total, jnp.zeros((LANES - 2 * QH, count), f32)], 0).T
    coarse_lane = lax.broadcasted_iota(jnp.int32, total.shape, 1) < QH
    gates[...] = jnp.where(coarse_lane, total * some, total)

    even[DK:, :] = jnp.zeros((PAD - DK, near + far), bf16)
    odd[: PAD - DK, :] = jnp.zeros((PAD - DK, near + far), bf16)
    near_values[:, DV:] = jnp.ones((near, DV), bf16)
    far_values[:, DV:] = jnp.ones((far, DV), bf16)
    for step in range(reach + 1):
        block = get_block(jnp.maximum(here - reach + step, 0), step)
        lanes = slice(step * count, (step + 1) * count)
        even[:DK, lanes] = block[:DK, :]
        odd[PAD - DK :, lanes] = block[:DK, :]
        near_values[lanes, :DV] = block[DK:, :]
    even[:DK, near:] = code_keys
    odd[PAD - DK :, near:] = code_keys
    far_values[:, :DV] = code_values

    pair = 2 * DK
    for side in (0, 1):
        keys = (even, odd)[side]
        for chunk in range(0, QH // 2, GROUP):
            rows = jnp.concatenate(
                [
                    q[:, (chunk + j) * pair + side * LANES : (chunk + j) * pair + side * LANES + PAD]
                    for j in range(GROUP)
                ],
                0,
            )
            scores = dot(rows, keys[...])

            def branch(scores, bias, values):
                width = scores.shape[1]
                scores = scores.reshape(GROUP, count, width) + bias[...][None]
                top = jnp.max(scores, axis=2, keepdims=True)
                weights = jnp.exp2((scores - top) * SCALE).astype(bf16)
                summed = dot(weights.reshape(GROUP * count, width), values[...])
                return summed[:, :DV] / jnp.maximum(summed[:, DV:], 1.0)

            local = branch(scores[:, :near], near_bias, near_values)
            coarse = branch(scores[:, near:], far_bias, far_values)
            for j in range(GROUP):
                head = 2 * (chunk + j) + side
                at = slice(j * count, (j + 1) * count)
                mixed = (
                    gates[:, head : head + 1] * coarse[at]
                    + gates[:, QH + head : QH + head + 1] * local[at]
                )
                out[:, head * DV : (head + 1) * DV] = mixed.astype(bf16)


def attend_scratch(count, reach, far):
    near = (reach + 1) * count
    return [
        pltpu.VMEM((PAD, near + far), bf16),
        pltpu.VMEM((PAD, near + far), bf16),
        pltpu.VMEM((near, 2 * DV), bf16),
        pltpu.VMEM((far, 2 * DV), bf16),
        pltpu.VMEM((count, near), f32),
        pltpu.VMEM((count, far), f32),
        pltpu.VMEM((count, LANES), f32),
    ]


def gate_columns(parts, some):
    total = parts[0][...]
    for part in parts[1:]:
        total = total + part[...]
    total = jax.nn.sigmoid(total)
    total = jnp.concatenate([total, jnp.zeros((LANES - 2 * QH, total.shape[1]), f32)], 0).T
    coarse_lane = lax.broadcasted_iota(jnp.int32, total.shape, 1) < QH
    return jnp.where(coarse_lane, total * some, total)


def fill_keys(even, odd, lanes, keys):
    even[:DK, lanes] = keys
    even[DK:, lanes] = jnp.zeros((PAD - DK, keys.shape[1]), bf16)
    odd[: PAD - DK, lanes] = jnp.zeros((PAD - DK, keys.shape[1]), bf16)
    odd[PAD - DK :, lanes] = keys


def query_rows(q, side, chunk):
    starts = [(chunk + j) * 2 * DK + side * LANES for j in range(GROUP)]
    return jnp.concatenate([q[:, start : start + PAD] for start in starts], 0)


def place_of(here, offset):
    block = here - offset
    return jnp.where(block >= 0, (block ^ here) >> 1, 0)


def early_kernel(slots, count, offsets, here_ref, q, bias, key_in, value_in, *refs):
    blocks, (shares, summed, tops) = refs[:slots], refs[slots : slots + 3]
    held, rows, even, odd, values = refs[slots + 3 :]
    here = here_ref[0]
    for i, block in enumerate(blocks):
        held[i] = block[...]
        unpack(block, rows, slots * count, i * count)
    near = len(offsets) * count
    for step, offset in enumerate(offsets):
        block = held[place_of(here, offset)]
        lanes = slice(step * count, (step + 1) * count)
        fill_keys(even, odd, lanes, block[:DK, :])
        values[lanes, :DV] = block[DK:, :]
    values[:, DV:] = jnp.ones((near, DV), bf16)
    shares[:, : 2 * LANES] = halves(rows, (0, 1), slots * count, key_in, DK)
    shares[:, 2 * LANES :] = halves(rows, (2,), slots * count, value_in, DV)
    for side in (0, 1):
        for chunk in range(0, QH // 2, GROUP):
            scores = dot(query_rows(q, side, chunk), (even, odd)[side][...])
            scores = scores.reshape(GROUP, count, near) + bias[:, :near][None]
            top = jnp.max(scores, axis=2, keepdims=True)
            weights = jnp.exp2((scores - top) * SCALE).astype(bf16)
            at = pl.ds((side * QH // 2 + chunk) * count, GROUP * count)
            summed[at, :] = dot(weights.reshape(GROUP * count, near), values[...])
            tops[at, :] = jnp.broadcast_to(top, (GROUP, count, LANES)).reshape(GROUP * count, LANES)


def late_kernel(
    slots, heads, count, offsets, done, here_ref, q, bias, some, second, key_in, value_in, shares, summed, tops, *refs
):
    blocks, parts, out = refs[:slots], refs[slots : slots + heads], refs[slots + heads]
    held, rows, even, odd, values, far_values, key_shares, value_shares, gates = refs[slots + heads + 1 :]
    here = here_ref[0]
    strides = count // STRIDE
    for i, block in enumerate(blocks):
        held[i] = block[...]
        unpack(block, rows, slots * count, i * count)
    near = len(offsets) * count
    for step, offset in enumerate(offsets):
        block = held[place_of(here, offset)]
        lanes = slice(step * count, (step + 1) * count)
        fill_keys(even, odd, lanes, block[:DK, :])
        values[lanes, :DV] = block[DK:, :]
    values[:, DV:] = jnp.ones((near, DV), bf16)
    key_late = halves(rows, (0, 1), slots * count, key_in, DK)
    value_late = halves(rows, (2,), slots * count, value_in, DV)
    for i in range(slots):
        mine = slice(i * strides, (i + 1) * strides)
        at = pl.ds(pl.multiple_of((here ^ (2 * i)) * strides, strides), strides)
        key_shares[at, :] = shares[mine, : 2 * LANES]
        value_shares[at, :] = shares[mine, 2 * LANES :]
        at = pl.ds(pl.multiple_of((here ^ (2 * i + 1)) * strides, strides), strides)
        key_shares[at, :] = key_late[mine]
        value_shares[at, :] = value_late[mine]
    codes = 2 * slots * strides
    far = far_values.shape[0]
    key_hidden = hidden_of(key_shares[:, :LANES], key_shares[:, LANES:])
    code_keys = dot_t(second[:DK, :], key_hidden).astype(bf16)
    value_hidden = hidden_of(value_shares[:, :LANES], value_shares[:, LANES:])
    code_values = dot(value_hidden, second[DK:, :]).astype(bf16)
    if far > codes:
        code_keys = jnp.concatenate([code_keys, jnp.zeros((DK, far - codes), bf16)], 1)
        code_values = jnp.concatenate([code_values, jnp.zeros((far - codes, DV), bf16)], 0)
    fill_keys(even, odd, slice(near, near + far), code_keys)
    far_values[:, :DV] = code_values
    far_values[:, DV:] = jnp.ones((far, DV), bf16)
    gates[...] = gate_columns(parts, some[...])
    size = GROUP * count
    for side in (0, 1):
        for chunk in range(0, QH // 2, GROUP):
            at = pl.ds((side * QH // 2 + chunk) * count, size)
            scores = dot(query_rows(q, side, chunk), (even, odd)[side][...])
            scores = scores.reshape(GROUP, count, near + far) + bias[:, done:][None]
            local, coarse = scores[:, :, :near], scores[:, :, near:]
            before = tops[at, :].reshape(GROUP, count, LANES)
            top = jnp.maximum(before, jnp.max(local, axis=2, keepdims=True))
            tops_near = jnp.concatenate([top] * (near // LANES), 2)
            weights = jnp.exp2((local - tops_near) * SCALE).astype(bf16)
            fade = jnp.exp2((before - top) * SCALE).reshape(size, LANES)
            old = summed[at, :] * jnp.concatenate([fade] * (2 * DV // LANES), 1)
            new = old + dot(weights.reshape(size, near), values[...])
            local = new[:, :DV] / jnp.maximum(new[:, DV:], 1.0)
            top = jnp.max(coarse, axis=2, keepdims=True)
            weights = jnp.exp2((coarse - top) * SCALE).astype(bf16)
            new = dot(weights.reshape(size, far), far_values[...])
            coarse = new[:, :DV] / jnp.maximum(new[:, DV:], 1.0)
            for j in range(GROUP):
                head = 2 * (chunk + j) + side
                mine = slice(j * count, (j + 1) * count)
                mixed = (
                    gates[:, head : head + 1] * coarse[mine]
                    + gates[:, QH + head : QH + head + 1] * local[mine]
                )
                out[:, head * DV : (head + 1) * DV] = mixed.astype(bf16)


def small_slab(here, group, positions, queries, block, features, gate_weight, weights, length, heads, reach):
    count = queries.shape[0]
    codes = length * count // STRIDE
    far = up(codes, LANES)
    first = tuple(range(reach - reach % 2, -1, -2))
    then = tuple(range(reach - (reach + 1) % 2, 0, -2))
    slots = {0: block, 1: swap(block, "seq", 1)}
    later = range(2, length, 2)
    for d in later:
        slots[d] = swap(block, "seq", d)
    key_in, key_out, value_in, value_out = weights
    parts, (bias, some, second, queries, key_in, value_in) = prepare(
        here, group, positions, features, gate_weight, heads, first + then, codes,
        (queries, key_in, value_in, key_out, value_out),
    )
    *came, _ = lax.optimization_barrier((*[slots[d] for d in later], parts))
    parts = exchange(parts)
    for d, value in zip(later, came):
        slots[d] = value
        slots[d + 1] = swap(value, "seq", 1)
    half = length // 2
    smem, vmem = pl.BlockSpec(memory_space=pltpu.SMEM), pl.BlockSpec(memory_space=pltpu.VMEM)
    params = pltpu.CompilerParams(vmem_limit_bytes=VMEM_LIMIT)
    rows = [
        pltpu.VMEM((half, DK + DV, count), bf16),
        pltpu.VMEM((3 * half * count, LANES), f32),
    ]
    near = len(first) * count
    shares, summed, tops = pl.pallas_call(
        functools.partial(early_kernel, half, count, first),
        in_specs=[smem] + [vmem] * (4 + half),
        out_specs=[vmem] * 3,
        out_shape=[
            jax.ShapeDtypeStruct((codes // 2, 4 * LANES), f32),
            jax.ShapeDtypeStruct((QH * count, 2 * DV), f32),
            jax.ShapeDtypeStruct((QH * count, LANES), f32),
        ],
        scratch_shapes=rows
        + [pltpu.VMEM((PAD, near), bf16)] * 2
        + [pltpu.VMEM((near, 2 * DV), bf16)],
        compiler_params=params,
        cost_estimate=pl.CostEstimate(flops=4 << 30, transcendentals=1 << 20, bytes_accessed=1 << 22),
        name="early",
    )(here[None], queries, bias, key_in, value_in, *[slots[d] for d in range(0, length, 2)])
    done = near
    near = len(then) * count
    return pl.pallas_call(
        functools.partial(late_kernel, half, heads, count, then, done),
        in_specs=[smem] + [vmem] * (9 + half + heads),
        out_specs=vmem,
        out_shape=jax.ShapeDtypeStruct((count, QH * DV), bf16),
        scratch_shapes=rows
        + [pltpu.VMEM((PAD, near + far), bf16)] * 2
        + [pltpu.VMEM((near, 2 * DV), bf16), pltpu.VMEM((far, 2 * DV), bf16)]
        + [pltpu.VMEM((codes, 2 * LANES), f32)] * 2
        + [pltpu.VMEM((count, LANES), f32)],
        compiler_params=params,
        name="late",
    )(
        here[None], queries, bias, some, second, key_in, value_in, shares, summed, tops,
        *[slots[d] for d in range(1, length, 2)], *parts,
    )


def codes_kernel(before, block, key_in, key_out, value_in, value_out, out, rows):
    count = block.shape[1]
    unpack(before[...], rows, 2 * count, 0)
    unpack(block[...], rows, 2 * count, count)
    code_keys, code_values = codes_of(rows, 2 * count, key_in, key_out, value_in, value_out)
    out[:, :DK] = code_keys.astype(f32).T
    out[:, DK:] = code_values.astype(f32)


def near_kernel(heads, count, reach, codes, here_ref, *refs):
    positions, q = refs[:2]
    blocks = refs[2 : 3 + reach]
    code_keys, code_values = refs[3 + reach : 5 + reach]
    parts = refs[5 + reach : 5 + reach + heads]
    out = refs[5 + reach + heads]
    attend_body(
        here_ref[0], count, reach, lambda at, step: blocks[step][...], code_keys[...], code_values[...],
        codes, positions, q, parts, out, refs[6 + reach + heads :],
    )


def long_slab(here, positions, queries, block, weights, parts, reach, length):
    count = queries.shape[0]
    strides = count // STRIDE
    smem, vmem = pl.BlockSpec(memory_space=pltpu.SMEM), pl.BlockSpec(memory_space=pltpu.VMEM)
    earlier = [turn(block, "seq", reach - k) for k in range(reach)]
    made = pl.pallas_call(
        codes_kernel,
        in_specs=[vmem] * 6,
        out_specs=vmem,
        out_shape=jax.ShapeDtypeStruct((2 * strides, DK + DV), f32),
        scratch_shapes=[pltpu.VMEM((6 * count, LANES), f32)],
        name="codes",
    )(earlier[-1], block, *weights)
    mine = made[strides - 1 : 2 * strides - 1].astype(bf16)
    every = lax.all_gather(mine, "seq", axis=0, tiled=True)[1:]
    codes = length * count // STRIDE
    far = up(codes, LANES)
    every = jnp.concatenate([every, jnp.zeros((far - every.shape[0], DK + DV), bf16)], 0)
    return pl.pallas_call(
        functools.partial(near_kernel, len(parts), count, reach, codes),
        in_specs=[smem] + [vmem] * (5 + reach + len(parts)),
        out_specs=vmem,
        out_shape=jax.ShapeDtypeStruct((count, QH * DV), bf16),
        scratch_shapes=attend_scratch(count, reach, far),
        name="long_slab",
    )(here[None], positions[None, :], queries, *earlier, block, every[:, :DK].T, every[:, DK:], *parts)


def on_device(
    queries, keys, values, features, positions, gate_weight, key_in, key_out, value_in, value_out
):
    count = keys.shape[0]
    length, heads = lax.axis_size("seq"), lax.axis_size("head")
    here = lax.axis_index("seq")
    group = lax.axis_index("head")
    reach = -(-WINDOW // count)
    block = jnp.concatenate([keys.T, values], 0)
    weights = (key_in[0], key_out[0].T, value_in[0], value_out[0])
    if length <= MOST_SLOTS and length > 1 and length & (length - 1) == 0:
        return small_slab(
            here, group, positions, queries, block, features, gate_weight, weights, length, heads, reach
        )
    parts = exchange(gate_logits(features, gate_weight, group, heads))
    return long_slab(here, positions, queries, block, weights, parts, reach, length)


def solution(mesh):
    return jax.shard_map(
        on_device,
        mesh=mesh,
        in_specs=(
            P("seq", "head"),
            P("seq", "head"),
            P("seq", "head"),
            P("seq", "head"),
            P("seq"),
            P(),
            P("head", None, None),
            P("head", None, None),
            P("head", None, None),
            P("head", None, None),
        ),
        out_specs=P("seq", "head"),
        check_vma=False,
    )
```

```python
import functools

import jax
import jax.numpy as jnp
from jax import lax
from jax.experimental import pallas as pl
from jax.experimental.pallas import tpu as pltpu
from jax.sharding import PartitionSpec as P

QH = 16
DK = 192
DV = 128
STRIDE = 16
BLOCK = 32
WINDOW = 512
LANES = 128
PAD = 256
GROUP = 4
VMEM_LIMIT = 24 << 20
MOST_SLOTS = 8

NEG = -1e30
SCALE = DK ** (-0.5) * 1.4426950408889634

f32 = jnp.float32
bf16 = jnp.bfloat16


def up(value, step):
    return -(-value // step) * step


def swap(value, axis, by):
    length = lax.axis_size(axis)
    return lax.ppermute(value, axis, [(i, i ^ by) for i in range(length)])


def turn(value, axis, by):
    length = lax.axis_size(axis)
    return lax.ppermute(value, axis, [(i, (i + by) % length) for i in range(length)])


def dot(left, right):
    return jnp.dot(left, right, preferred_element_type=f32)


def dot_t(left, right):
    return lax.dot_general(left, right, (((1,), (1,)), ((), ())), preferred_element_type=f32)


def place_hbm(value):
    return pltpu.with_memory_space_constraint(value, pltpu.HBM)


def logits_of(group, heads, features, columns, total, outs):
    total[...] = lax.dot_general(
        columns[...], features[...], (((0,), (1,)), ((), ())), preferred_element_type=f32
    )
    for step, out in enumerate(outs):
        other = group ^ step if heads & (heads - 1) == 0 else lax.rem(group + step, heads)
        out[...] = total[pl.ds(pl.multiple_of(other * (2 * QH), 2 * QH), 2 * QH), :]


def feature_copies(group, features_hbm, columns_hbm, features, columns, sems):
    depth = features.shape[1]
    first = pl.multiple_of(group * depth, LANES)
    return [
        pltpu.make_async_copy(features_hbm, features, sems.at[0]),
        pltpu.make_async_copy(columns_hbm.at[pl.ds(first, depth), :], columns, sems.at[1]),
    ]


def logit_kernel(heads, group, features_hbm, columns_hbm, *refs):
    outs, (features, columns, total, sems) = refs[:heads], refs[heads:]
    copies = feature_copies(group[0], features_hbm, columns_hbm, features, columns, sems)
    for copy in copies:
        copy.start()
    for copy in copies:
        copy.wait()
    logits_of(group[0], heads, features, columns, total, outs)


def prepare_kernel(heads, kept, offsets, codes, here_ref, group_ref, features_hbm, columns_hbm, positions_hbm, *refs):
    here, group = here_ref[0], group_ref[0]
    sources = refs[:kept]
    outs = refs[kept : kept + heads]
    bias, some, second = refs[kept + heads : kept + heads + 3]
    places = refs[kept + heads + 3 : 2 * kept + heads + 1]
    features, columns, total, positions, sems = refs[2 * kept + heads + 1 :]
    places = [*places, second.at[pl.ds(0, DK), :], second.at[pl.ds(DK, sources[-1].shape[0]), :]]
    copies = feature_copies(group, features_hbm, columns_hbm, features, columns, sems)
    copies.append(pltpu.make_async_copy(positions_hbm, positions, sems.at[2]))
    copies += [
        pltpu.make_async_copy(source, place, sems.at[3 + i])
        for i, (source, place) in enumerate(zip(sources, places))
    ]
    for copy in copies:
        copy.start()
    for copy in copies[:3]:
        copy.wait()
    logits_of(group, heads, features, columns, total, outs)
    count = positions.shape[1]
    lengths = jnp.broadcast_to(positions[...].astype(f32), (count, count)).T.astype(jnp.int32)
    token = here * count + lax.broadcasted_iota(jnp.int32, (count, count), 0)
    lane = lax.broadcasted_iota(jnp.int32, (count, count), 1)
    for step, offset in enumerate(offsets):
        key = (here - offset) * count + lane
        seen = (key <= token) & (key > token - WINDOW) & (key >= token - lengths) & (key >= 0)
        bias[:, step * count : (step + 1) * count] = jnp.where(seen, 0.0, NEG)
    near = len(offsets) * count
    most = jnp.full((count, LANES), NEG, f32)
    for start in range(near, bias.shape[1], LANES):
        code = start - near + lax.broadcasted_iota(jnp.int32, (count, LANES), 1)
        token = here * count + lax.broadcasted_iota(jnp.int32, (count, LANES), 0)
        length = lengths if count == LANES else jnp.broadcast_to(lengths[:, :1], (count, LANES))
        first = STRIDE * code
        seen = (first + (BLOCK - 1) <= token) & (first >= token - length) & (code < codes)
        part = jnp.where(seen, 0.0, NEG)
        bias[:, start : start + LANES] = part
        most = jnp.maximum(most, part)
    some[...] = jnp.where(
        jnp.broadcast_to(jnp.max(most, axis=1, keepdims=True), (count, LANES)) > 0.5 * NEG, 1.0, 0.0
    )
    for copy in copies[3:]:
        copy.wait()


def gate_shapes(count, depth, columns):
    return [
        pltpu.VMEM((count, depth), bf16),
        pltpu.VMEM((depth, columns), bf16),
        pltpu.VMEM((columns, count), f32),
    ]


def gate_logits(features, gate_weight, group, heads):
    count, depth = features.shape
    vmem, hbm = pl.BlockSpec(memory_space=pltpu.VMEM), pl.BlockSpec(memory_space=pltpu.HBM)
    return pl.pallas_call(
        functools.partial(logit_kernel, heads),
        in_specs=[pl.BlockSpec(memory_space=pltpu.SMEM), hbm, hbm],
        out_specs=[vmem] * heads,
        out_shape=[jax.ShapeDtypeStruct((2 * QH, count), f32)] * heads,
        scratch_shapes=gate_shapes(count, depth, gate_weight.shape[1])
        + [pltpu.SemaphoreType.DMA((2,))],
        compiler_params=pltpu.CompilerParams(vmem_limit_bytes=VMEM_LIMIT),
        name="gate_logits",
    )(group[None], features, gate_weight)


def prepare(here, group, positions, features, gate_weight, heads, offsets, codes, kept):
    count, depth = features.shape
    vmem, hbm = pl.BlockSpec(memory_space=pltpu.VMEM), pl.BlockSpec(memory_space=pltpu.HBM)
    wide = len(offsets) * count + up(codes, LANES)
    last = kept[-2:]
    made = pl.pallas_call(
        functools.partial(prepare_kernel, heads, len(kept), offsets, codes),
        in_specs=[pl.BlockSpec(memory_space=pltpu.SMEM)] * 2 + [hbm] * (3 + len(kept)),
        out_specs=[vmem] * (heads + 1 + len(kept)),
        out_shape=[jax.ShapeDtypeStruct((2 * QH, count), f32)] * heads
        + [
            jax.ShapeDtypeStruct((count, wide), f32),
            jax.ShapeDtypeStruct((count, LANES), f32),
            jax.ShapeDtypeStruct((last[0].shape[0] + last[1].shape[0], last[1].shape[1]), bf16),
        ]
        + [jax.ShapeDtypeStruct(value.shape, value.dtype) for value in kept[:-2]],
        scratch_shapes=gate_shapes(count, depth, gate_weight.shape[1])
        + [pltpu.VMEM((1, count), jnp.int32), pltpu.SemaphoreType.DMA((3 + len(kept),))],
        compiler_params=pltpu.CompilerParams(vmem_limit_bytes=VMEM_LIMIT),
        name="prepare",
    )(
        here[None],
        group[None],
        *[place_hbm(value) for value in (features, gate_weight, positions[None, :], *kept)],
    )
    return made[:heads], made[heads:]


def exchange(parts):
    heads = len(parts)
    if heads & (heads - 1) == 0:
        return [parts[0]] + [swap(parts[d], "head", d) for d in range(1, heads)]
    return [parts[0]] + [turn(parts[d], "head", d) for d in range(1, heads)]


def gelu(x):
    return 0.5 * x * (1.0 + jnp.tanh(0.7978845608028654 * (x + 0.044715 * x * x * x)))


def halves(rows, planes, size, weight, width):
    strides = size // STRIDE
    total = jnp.zeros((strides, 2 * LANES), f32)
    for place in range(STRIDE):
        part = jnp.concatenate(
            [rows[pl.ds(plane * size + place, strides, stride=STRIDE), :] for plane in planes], 1
        ).astype(bf16)[:, :width]
        both = jnp.concatenate(
            [
                weight[pl.ds(place * width, width), :],
                weight[pl.ds((STRIDE + place) * width, width), :],
            ],
            1,
        )
        total = total + dot(part, both)
    return total


def hidden_of(first, second):
    strides = first.shape[0]
    later = pltpu.roll(second, strides - 1, axis=0)
    last = lax.broadcasted_iota(jnp.int32, later.shape, 0) == strides - 1
    return gelu(first + jnp.where(last, 0.0, later)).astype(bf16)


def unpack(block, rows, size, at):
    count = block.shape[1]
    for plane in range(2):
        part = block[plane * LANES : min((plane + 1) * LANES, DK), :].astype(f32).T
        rows[pl.ds(plane * size + at, count), : part.shape[1]] = part
    rows[pl.ds(2 * size + at, count), :] = block[DK:, :].astype(f32)


def codes_of(rows, size, key_in, key_out, value_in, value_out):
    shares = halves(rows, (0, 1), size, key_in, DK)
    key_hidden = hidden_of(shares[:, :LANES], shares[:, LANES:])
    code_keys = dot_t(key_out[...], key_hidden).astype(bf16)
    shares = halves(rows, (2,), size, value_in, DV)
    value_hidden = hidden_of(shares[:, :LANES], shares[:, LANES:])
    code_values = dot(value_hidden, value_out[...]).astype(bf16)
    return code_keys, code_values


def attend_body(
    here, count, reach, get_block, code_keys, code_values, codes, positions, q, parts, out, scratch
):
    even, odd, near_values, far_values, near_bias, far_bias, gates = scratch
    near = (reach + 1) * count
    far = even.shape[1] - near
    lengths = jnp.broadcast_to(positions[...].astype(f32), (count, count)).T.astype(jnp.int32)

    def lens(width):
        return jnp.concatenate([lengths] * (width // count), 1) if width > count else lengths

    def ids(width, axis):
        return lax.broadcasted_iota(jnp.int32, (count, width), axis)

    token = here * count + ids(near, 0)
    key = (here - reach) * count + ids(near, 1)
    seen = (key <= token) & (key > token - WINDOW) & (key >= token - lens(near)) & (key >= 0)
    near_bias[...] = jnp.where(seen, 0.0, NEG)
    token = here * count + ids(far, 0)
    first = STRIDE * ids(far, 1)
    seen = (first + (BLOCK - 1) <= token) & (first >= token - lens(far)) & (ids(far, 1) < codes)
    far_bias[...] = jnp.where(seen, 0.0, NEG)
    some = jnp.max(jnp.where(seen, 1.0, 0.0), axis=1, keepdims=True)

    total = parts[0][...]
    for part in parts[1:]:
        total = total + part[...]
    total = jax.nn.sigmoid(total)
    total = jnp.concatenate([total, jnp.zeros((LANES - 2 * QH, count), f32)], 0).T
    coarse_lane = lax.broadcasted_iota(jnp.int32, total.shape, 1) < QH
    gates[...] = jnp.where(coarse_lane, total * some, total)

    even[DK:, :] = jnp.zeros((PAD - DK, near + far), bf16)
    odd[: PAD - DK, :] = jnp.zeros((PAD - DK, near + far), bf16)
    near_values[:, DV:] = jnp.ones((near, DV), bf16)
    far_values[:, DV:] = jnp.ones((far, DV), bf16)
    for step in range(reach + 1):
        block = get_block(jnp.maximum(here - reach + step, 0), step)
        lanes = slice(step * count, (step + 1) * count)
        even[:DK, lanes] = block[:DK, :]
        odd[PAD - DK :, lanes] = block[:DK, :]
        near_values[lanes, :DV] = block[DK:, :]
    even[:DK, near:] = code_keys
    odd[PAD - DK :, near:] = code_keys
    far_values[:, :DV] = code_values

    pair = 2 * DK
    for side in (0, 1):
        keys = (even, odd)[side]
        for chunk in range(0, QH // 2, GROUP):
            rows = jnp.concatenate(
                [
                    q[:, (chunk + j) * pair + side * LANES : (chunk + j) * pair + side * LANES + PAD]
                    for j in range(GROUP)
                ],
                0,
            )
            scores = dot(rows, keys[...])

            def branch(scores, bias, values):
                width = scores.shape[1]
                scores = scores.reshape(GROUP, count, width) + bias[...][None]
                top = jnp.max(scores, axis=2, keepdims=True)
                weights = jnp.exp2((scores - top) * SCALE).astype(bf16)
                summed = dot(weights.reshape(GROUP * count, width), values[...])
                return summed[:, :DV] / jnp.maximum(summed[:, DV:], 1.0)

            local = branch(scores[:, :near], near_bias, near_values)
            coarse = branch(scores[:, near:], far_bias, far_values)
            for j in range(GROUP):
                head = 2 * (chunk + j) + side
                at = slice(j * count, (j + 1) * count)
                mixed = (
                    gates[:, head : head + 1] * coarse[at]
                    + gates[:, QH + head : QH + head + 1] * local[at]
                )
                out[:, head * DV : (head + 1) * DV] = mixed.astype(bf16)


def attend_scratch(count, reach, far):
    near = (reach + 1) * count
    return [
        pltpu.VMEM((PAD, near + far), bf16),
        pltpu.VMEM((PAD, near + far), bf16),
        pltpu.VMEM((near, 2 * DV), bf16),
        pltpu.VMEM((far, 2 * DV), bf16),
        pltpu.VMEM((count, near), f32),
        pltpu.VMEM((count, far), f32),
        pltpu.VMEM((count, LANES), f32),
    ]


def gate_columns(parts, some):
    total = parts[0][...]
    for part in parts[1:]:
        total = total + part[...]
    total = jax.nn.sigmoid(total)
    total = jnp.concatenate([total, jnp.zeros((LANES - 2 * QH, total.shape[1]), f32)], 0).T
    coarse_lane = lax.broadcasted_iota(jnp.int32, total.shape, 1) < QH
    return jnp.where(coarse_lane, total * some, total)


def fill_keys(even, odd, lanes, keys):
    even[:DK, lanes] = keys
    even[DK:, lanes] = jnp.zeros((PAD - DK, keys.shape[1]), bf16)
    odd[: PAD - DK, lanes] = jnp.zeros((PAD - DK, keys.shape[1]), bf16)
    odd[PAD - DK :, lanes] = keys


def query_rows(q, side, chunk):
    starts = [(chunk + j) * 2 * DK + side * LANES for j in range(GROUP)]
    return jnp.concatenate([q[:, start : start + PAD] for start in starts], 0)


def place_of(here, offset):
    block = here - offset
    return jnp.where(block >= 0, (block ^ here) >> 1, 0)


def early_kernel(slots, count, offsets, here_ref, q, bias, key_in, value_in, *refs):
    blocks, (shares, summed, tops) = refs[:slots], refs[slots : slots + 3]
    held, rows, even, odd, values = refs[slots + 3 :]
    here = here_ref[0]
    for i, block in enumerate(blocks):
        held[i] = block[...]
        unpack(block, rows, slots * count, i * count)
    near = len(offsets) * count
    for step, offset in enumerate(offsets):
        block = held[place_of(here, offset)]
        lanes = slice(step * count, (step + 1) * count)
        fill_keys(even, odd, lanes, block[:DK, :])
        values[lanes, :DV] = block[DK:, :]
    values[:, DV:] = jnp.ones((near, DV), bf16)
    shares[:, : 2 * LANES] = halves(rows, (0, 1), slots * count, key_in, DK)
    shares[:, 2 * LANES :] = halves(rows, (2,), slots * count, value_in, DV)
    for side in (0, 1):
        for chunk in range(0, QH // 2, GROUP):
            scores = dot(query_rows(q, side, chunk), (even, odd)[side][...])
            scores = scores.reshape(GROUP, count, near) + bias[:, :near][None]
            top = jnp.max(scores, axis=2, keepdims=True)
            weights = jnp.exp2((scores - top) * SCALE).astype(bf16)
            at = pl.ds((side * QH // 2 + chunk) * count, GROUP * count)
            summed[at, :] = dot(weights.reshape(GROUP * count, near), values[...])
            tops[at, :] = jnp.broadcast_to(top, (GROUP, count, LANES)).reshape(GROUP * count, LANES)


def late_kernel(
    buffers, slots, heads, count, offsets, done, here_ref, q, bias, some, second, key_in, value_in, shares, summed, tops, *refs
):
    came, parts, out = refs[:buffers], refs[buffers : buffers + heads], refs[buffers + heads]
    held, rows, even, odd, values, far_values, key_shares, value_shares, gates = refs[buffers + heads + 1 :]
    size = DK + DV
    blocks = [ref.at[pl.ds(at, size), :] for ref in came for at in range(0, ref.shape[0], size)]
    here = here_ref[0]
    strides = count // STRIDE
    for i, block in enumerate(blocks):
        held[i] = block[...]
        unpack(block, rows, slots * count, i * count)
    near = len(offsets) * count
    for step, offset in enumerate(offsets):
        block = held[place_of(here, offset)]
        lanes = slice(step * count, (step + 1) * count)
        fill_keys(even, odd, lanes, block[:DK, :])
        values[lanes, :DV] = block[DK:, :]
    values[:, DV:] = jnp.ones((near, DV), bf16)
    key_late = halves(rows, (0, 1), slots * count, key_in, DK)
    value_late = halves(rows, (2,), slots * count, value_in, DV)
    for i in range(slots):
        mine = slice(i * strides, (i + 1) * strides)
        at = pl.ds(pl.multiple_of((here ^ (2 * i)) * strides, strides), strides)
        key_shares[at, :] = shares[mine, : 2 * LANES]
        value_shares[at, :] = shares[mine, 2 * LANES :]
        at = pl.ds(pl.multiple_of((here ^ (2 * i + 1)) * strides, strides), strides)
        key_shares[at, :] = key_late[mine]
        value_shares[at, :] = value_late[mine]
    codes = 2 * slots * strides
    far = far_values.shape[0]
    key_hidden = hidden_of(key_shares[:, :LANES], key_shares[:, LANES:])
    code_keys = dot_t(second[:DK, :], key_hidden).astype(bf16)
    value_hidden = hidden_of(value_shares[:, :LANES], value_shares[:, LANES:])
    code_values = dot(value_hidden, second[DK:, :]).astype(bf16)
    if far > codes:
        code_keys = jnp.concatenate([code_keys, jnp.zeros((DK, far - codes), bf16)], 1)
        code_values = jnp.concatenate([code_values, jnp.zeros((far - codes, DV), bf16)], 0)
    fill_keys(even, odd, slice(near, near + far), code_keys)
    far_values[:, :DV] = code_values
    far_values[:, DV:] = jnp.ones((far, DV), bf16)
    gates[...] = gate_columns(parts, some[...])
    size = GROUP * count
    for side in (0, 1):
        for chunk in range(0, QH // 2, GROUP):
            at = pl.ds((side * QH // 2 + chunk) * count, size)
            scores = dot(query_rows(q, side, chunk), (even, odd)[side][...])
            scores = scores.reshape(GROUP, count, near + far) + bias[:, done:][None]
            local, coarse = scores[:, :, :near], scores[:, :, near:]
            before = tops[at, :].reshape(GROUP, count, LANES)
            top = jnp.maximum(before, jnp.max(local, axis=2, keepdims=True))
            tops_near = jnp.concatenate([top] * (near // LANES), 2)
            weights = jnp.exp2((local - tops_near) * SCALE).astype(bf16)
            fade = jnp.exp2((before - top) * SCALE).reshape(size, LANES)
            old = summed[at, :] * jnp.concatenate([fade] * (2 * DV // LANES), 1)
            new = old + dot(weights.reshape(size, near), values[...])
            local = new[:, :DV] / jnp.maximum(new[:, DV:], 1.0)
            top = jnp.max(coarse, axis=2, keepdims=True)
            weights = jnp.exp2((coarse - top) * SCALE).astype(bf16)
            new = dot(weights.reshape(size, far), far_values[...])
            coarse = new[:, :DV] / jnp.maximum(new[:, DV:], 1.0)
            for j in range(GROUP):
                head = 2 * (chunk + j) + side
                mine = slice(j * count, (j + 1) * count)
                mixed = (
                    gates[:, head : head + 1] * coarse[mine]
                    + gates[:, QH + head : QH + head + 1] * local[mine]
                )
                out[:, head * DV : (head + 1) * DV] = mixed.astype(bf16)


def join_kernel(*refs):
    *blocks, out = refs
    size = blocks[0].shape[0]
    for i, block in enumerate(blocks):
        out[i * size : (i + 1) * size, :] = block[...]


def join(blocks):
    size, count = blocks[0].shape
    vmem = pl.BlockSpec(memory_space=pltpu.VMEM)
    return pl.pallas_call(
        join_kernel,
        in_specs=[vmem] * len(blocks),
        out_specs=vmem,
        out_shape=jax.ShapeDtypeStruct((len(blocks) * size, count), bf16),
        compiler_params=pltpu.CompilerParams(vmem_limit_bytes=VMEM_LIMIT),
        name="join",
    )(*blocks)


def small_slab(here, group, positions, queries, block, features, gate_weight, weights, length, heads, reach):
    count = queries.shape[0]
    codes = length * count // STRIDE
    far = up(codes, LANES)
    first = tuple(range(reach - reach % 2, -1, -2))
    then = tuple(range(reach - (reach + 1) % 2, 0, -2))
    key_in, key_out, value_in, value_out = weights
    slots = {0: block}
    for d in range(2, length, 2):
        slots[d] = swap(block, "seq", d)
    parts, (bias, some, second, queries, key_in, value_in) = prepare(
        here, group, positions, features, gate_weight, heads, first + then, codes,
        (queries, key_in, value_in, key_out, value_out),
    )
    for d in range(2, length, 2):
        slots[d] = lax.optimization_barrier((slots[d], parts))[0]
    across = [swap(block, "seq", 1)]
    across.append(swap(join([slots[d] for d in range(2, min(length, 6), 2)]), "seq", 1))
    for d in range(6, length, 2):
        across.append(swap(slots[d], "seq", 1))
    parts = exchange(parts)
    half = length // 2
    smem, vmem = pl.BlockSpec(memory_space=pltpu.SMEM), pl.BlockSpec(memory_space=pltpu.VMEM)
    params = pltpu.CompilerParams(vmem_limit_bytes=VMEM_LIMIT)
    rows = [
        pltpu.VMEM((half, DK + DV, count), bf16),
        pltpu.VMEM((3 * half * count, LANES), f32),
    ]
    near = len(first) * count
    shares, summed, tops = pl.pallas_call(
        functools.partial(early_kernel, half, count, first),
        in_specs=[smem] + [vmem] * (4 + half),
        out_specs=[vmem] * 3,
        out_shape=[
            jax.ShapeDtypeStruct((codes // 2, 4 * LANES), f32),
            jax.ShapeDtypeStruct((QH * count, 2 * DV), f32),
            jax.ShapeDtypeStruct((QH * count, LANES), f32),
        ],
        scratch_shapes=rows
        + [pltpu.VMEM((PAD, near), bf16)] * 2
        + [pltpu.VMEM((near, 2 * DV), bf16)],
        compiler_params=params,
        cost_estimate=pl.CostEstimate(flops=4 << 30, transcendentals=1 << 20, bytes_accessed=1 << 22),
        name="early",
    )(here[None], queries, bias, key_in, value_in, *[slots[d] for d in range(0, length, 2)])
    done = near
    near = len(then) * count
    return pl.pallas_call(
        functools.partial(late_kernel, len(across), half, heads, count, then, done),
        in_specs=[smem] + [vmem] * (9 + len(across) + heads),
        out_specs=vmem,
        out_shape=jax.ShapeDtypeStruct((count, QH * DV), bf16),
        scratch_shapes=rows
        + [pltpu.VMEM((PAD, near + far), bf16)] * 2
        + [pltpu.VMEM((near, 2 * DV), bf16), pltpu.VMEM((far, 2 * DV), bf16)]
        + [pltpu.VMEM((codes, 2 * LANES), f32)] * 2
        + [pltpu.VMEM((count, LANES), f32)],
        compiler_params=params,
        name="late",
    )(
        here[None], queries, bias, some, second, key_in, value_in, shares, summed, tops,
        *across, *parts,
    )


def codes_kernel(before, block, key_in, key_out, value_in, value_out, out, rows):
    count = block.shape[1]
    unpack(before[...], rows, 2 * count, 0)
    unpack(block[...], rows, 2 * count, count)
    code_keys, code_values = codes_of(rows, 2 * count, key_in, key_out, value_in, value_out)
    out[:, :DK] = code_keys.astype(f32).T
    out[:, DK:] = code_values.astype(f32)


def near_kernel(heads, count, reach, codes, here_ref, *refs):
    positions, q = refs[:2]
    blocks = refs[2 : 3 + reach]
    code_keys, code_values = refs[3 + reach : 5 + reach]
    parts = refs[5 + reach : 5 + reach + heads]
    out = refs[5 + reach + heads]
    attend_body(
        here_ref[0], count, reach, lambda at, step: blocks[step][...], code_keys[...], code_values[...],
        codes, positions, q, parts, out, refs[6 + reach + heads :],
    )


def long_slab(here, positions, queries, block, weights, parts, reach, length):
    count = queries.shape[0]
    strides = count // STRIDE
    smem, vmem = pl.BlockSpec(memory_space=pltpu.SMEM), pl.BlockSpec(memory_space=pltpu.VMEM)
    earlier = [turn(block, "seq", reach - k) for k in range(reach)]
    made = pl.pallas_call(
        codes_kernel,
        in_specs=[vmem] * 6,
        out_specs=vmem,
        out_shape=jax.ShapeDtypeStruct((2 * strides, DK + DV), f32),
        scratch_shapes=[pltpu.VMEM((6 * count, LANES), f32)],
        name="codes",
    )(earlier[-1], block, *weights)
    mine = made[strides - 1 : 2 * strides - 1].astype(bf16)
    every = lax.all_gather(mine, "seq", axis=0, tiled=True)[1:]
    codes = length * count // STRIDE
    far = up(codes, LANES)
    every = jnp.concatenate([every, jnp.zeros((far - every.shape[0], DK + DV), bf16)], 0)
    return pl.pallas_call(
        functools.partial(near_kernel, len(parts), count, reach, codes),
        in_specs=[smem] + [vmem] * (5 + reach + len(parts)),
        out_specs=vmem,
        out_shape=jax.ShapeDtypeStruct((count, QH * DV), bf16),
        scratch_shapes=attend_scratch(count, reach, far),
        name="long_slab",
    )(here[None], positions[None, :], queries, *earlier, block, every[:, :DK].T, every[:, DK:], *parts)


def on_device(
    queries, keys, values, features, positions, gate_weight, key_in, key_out, value_in, value_out
):
    count = keys.shape[0]
    length, heads = lax.axis_size("seq"), lax.axis_size("head")
    here = lax.axis_index("seq")
    group = lax.axis_index("head")
    reach = -(-WINDOW // count)
    block = jnp.concatenate([keys.T, values], 0)
    weights = (key_in[0], key_out[0].T, value_in[0], value_out[0])
    if length <= MOST_SLOTS and length > 1 and length & (length - 1) == 0:
        return small_slab(
            here, group, positions, queries, block, features, gate_weight, weights, length, heads, reach
        )
    parts = exchange(gate_logits(features, gate_weight, group, heads))
    return long_slab(here, positions, queries, block, weights, parts, reach, length)


def solution(mesh):
    return jax.shard_map(
        on_device,
        mesh=mesh,
        in_specs=(
            P("seq", "head"),
            P("seq", "head"),
            P("seq", "head"),
            P("seq", "head"),
            P("seq"),
            P(),
            P("head", None, None),
            P("head", None, None),
            P("head", None, None),
            P("head", None, None),
        ),
        out_specs=P("seq", "head"),
        check_vma=False,
    )
```

```python
import functools

import jax
import jax.numpy as jnp
from jax import lax
from jax.experimental import pallas as pl
from jax.experimental.pallas import tpu as pltpu
from jax.sharding import PartitionSpec as P

QH = 16
DK = 192
DV = 128
STRIDE = 16
BLOCK = 32
WINDOW = 512
LANES = 128
PAD = 256
GROUP = 4
LATE_GROUP = 8
MID_BLOCKS = 3
VMEM_LIMIT = 24 << 20
MOST_SLOTS = 8

NEG = -1e30
SCALE = DK ** (-0.5) * 1.4426950408889634

f32 = jnp.float32
bf16 = jnp.bfloat16


def up(value, step):
    return -(-value // step) * step


def swap(value, axis, by):
    length = lax.axis_size(axis)
    return lax.ppermute(value, axis, [(i, i ^ by) for i in range(length)])


def turn(value, axis, by):
    length = lax.axis_size(axis)
    return lax.ppermute(value, axis, [(i, (i + by) % length) for i in range(length)])


def dot(left, right):
    return jnp.dot(left, right, preferred_element_type=f32)


def dot_t(left, right):
    return lax.dot_general(left, right, (((1,), (1,)), ((), ())), preferred_element_type=f32)


def place_hbm(value):
    return pltpu.with_memory_space_constraint(value, pltpu.HBM)


def logits_of(group, heads, features, columns, total, outs):
    total[...] = lax.dot_general(
        columns[...], features[...], (((0,), (1,)), ((), ())), preferred_element_type=f32
    )
    for step, out in enumerate(outs):
        other = group ^ step if heads & (heads - 1) == 0 else lax.rem(group + step, heads)
        out[...] = total[pl.ds(pl.multiple_of(other * (2 * QH), 2 * QH), 2 * QH), :]


def feature_copies(group, features_hbm, columns_hbm, features, columns, sems):
    depth = features.shape[1]
    first = pl.multiple_of(group * depth, LANES)
    return [
        pltpu.make_async_copy(features_hbm, features, sems.at[0]),
        pltpu.make_async_copy(columns_hbm.at[pl.ds(first, depth), :], columns, sems.at[1]),
    ]


def logit_kernel(heads, group, features_hbm, columns_hbm, *refs):
    outs, (features, columns, total, sems) = refs[:heads], refs[heads:]
    copies = feature_copies(group[0], features_hbm, columns_hbm, features, columns, sems)
    for copy in copies:
        copy.start()
    for copy in copies:
        copy.wait()
    logits_of(group[0], heads, features, columns, total, outs)


def prepare_kernel(heads, kept, offsets, codes, here_ref, group_ref, features_hbm, columns_hbm, positions_hbm, *refs):
    here, group = here_ref[0], group_ref[0]
    sources = refs[:kept]
    outs = refs[kept : kept + heads]
    bias, some, second = refs[kept + heads : kept + heads + 3]
    places = refs[kept + heads + 3 : 2 * kept + heads + 1]
    features, columns, total, positions, sems = refs[2 * kept + heads + 1 :]
    places = [*places, second.at[pl.ds(0, DK), :], second.at[pl.ds(DK, sources[-1].shape[0]), :]]
    copies = feature_copies(group, features_hbm, columns_hbm, features, columns, sems)
    copies.append(pltpu.make_async_copy(positions_hbm, positions, sems.at[2]))
    copies += [
        pltpu.make_async_copy(source, place, sems.at[3 + i])
        for i, (source, place) in enumerate(zip(sources, places))
    ]
    for copy in copies:
        copy.start()
    for copy in copies[:3]:
        copy.wait()
    logits_of(group, heads, features, columns, total, outs)
    count = positions.shape[1]
    lengths = jnp.broadcast_to(positions[...].astype(f32), (count, count)).T.astype(jnp.int32)
    token = here * count + lax.broadcasted_iota(jnp.int32, (count, count), 0)
    lane = lax.broadcasted_iota(jnp.int32, (count, count), 1)
    for step, offset in enumerate(offsets):
        key = (here - offset) * count + lane
        seen = (key <= token) & (key > token - WINDOW) & (key >= token - lengths) & (key >= 0)
        bias[:, step * count : (step + 1) * count] = jnp.where(seen, 0.0, NEG)
    near = len(offsets) * count
    most = jnp.full((count, LANES), NEG, f32)
    for start in range(near, bias.shape[1], LANES):
        code = start - near + lax.broadcasted_iota(jnp.int32, (count, LANES), 1)
        token = here * count + lax.broadcasted_iota(jnp.int32, (count, LANES), 0)
        length = lengths if count == LANES else jnp.broadcast_to(lengths[:, :1], (count, LANES))
        first = STRIDE * code
        seen = (first + (BLOCK - 1) <= token) & (first >= token - length) & (code < codes)
        part = jnp.where(seen, 0.0, NEG)
        bias[:, start : start + LANES] = part
        most = jnp.maximum(most, part)
    some[...] = jnp.where(
        jnp.broadcast_to(jnp.max(most, axis=1, keepdims=True), (count, LANES)) > 0.5 * NEG, 1.0, 0.0
    )
    for copy in copies[3:]:
        copy.wait()


def gate_shapes(count, depth, columns):
    return [
        pltpu.VMEM((count, depth), bf16),
        pltpu.VMEM((depth, columns), bf16),
        pltpu.VMEM((columns, count), f32),
    ]


def gate_logits(features, gate_weight, group, heads):
    count, depth = features.shape
    vmem, hbm = pl.BlockSpec(memory_space=pltpu.VMEM), pl.BlockSpec(memory_space=pltpu.HBM)
    return pl.pallas_call(
        functools.partial(logit_kernel, heads),
        in_specs=[pl.BlockSpec(memory_space=pltpu.SMEM), hbm, hbm],
        out_specs=[vmem] * heads,
        out_shape=[jax.ShapeDtypeStruct((2 * QH, count), f32)] * heads,
        scratch_shapes=gate_shapes(count, depth, gate_weight.shape[1])
        + [pltpu.SemaphoreType.DMA((2,))],
        compiler_params=pltpu.CompilerParams(vmem_limit_bytes=VMEM_LIMIT),
        name="gate_logits",
    )(group[None], features, gate_weight)


def prepare(here, group, positions, features, gate_weight, heads, offsets, codes, kept):
    count, depth = features.shape
    vmem, hbm = pl.BlockSpec(memory_space=pltpu.VMEM), pl.BlockSpec(memory_space=pltpu.HBM)
    wide = len(offsets) * count + up(codes, LANES)
    last = kept[-2:]
    made = pl.pallas_call(
        functools.partial(prepare_kernel, heads, len(kept), offsets, codes),
        in_specs=[pl.BlockSpec(memory_space=pltpu.SMEM)] * 2 + [hbm] * (3 + len(kept)),
        out_specs=[vmem] * (heads + 1 + len(kept)),
        out_shape=[jax.ShapeDtypeStruct((2 * QH, count), f32)] * heads
        + [
            jax.ShapeDtypeStruct((count, wide), f32),
            jax.ShapeDtypeStruct((count, LANES), f32),
            jax.ShapeDtypeStruct((last[0].shape[0] + last[1].shape[0], last[1].shape[1]), bf16),
        ]
        + [jax.ShapeDtypeStruct(value.shape, value.dtype) for value in kept[:-2]],
        scratch_shapes=gate_shapes(count, depth, gate_weight.shape[1])
        + [pltpu.VMEM((1, count), jnp.int32), pltpu.SemaphoreType.DMA((3 + len(kept),))],
        compiler_params=pltpu.CompilerParams(vmem_limit_bytes=VMEM_LIMIT),
        name="prepare",
    )(
        here[None],
        group[None],
        *[place_hbm(value) for value in (features, gate_weight, positions[None, :], *kept)],
    )
    return made[:heads], made[heads:]


def exchange(parts):
    heads = len(parts)
    if heads & (heads - 1) == 0:
        return [parts[0]] + [swap(parts[d], "head", d) for d in range(1, heads)]
    return [parts[0]] + [turn(parts[d], "head", d) for d in range(1, heads)]


def gelu(x):
    return 0.5 * x * (1.0 + jnp.tanh(0.7978845608028654 * (x + 0.044715 * x * x * x)))


def halves(rows, planes, size, weight, width):
    strides = size // STRIDE
    total = jnp.zeros((strides, 2 * LANES), f32)
    for place in range(STRIDE):
        part = jnp.concatenate(
            [rows[pl.ds(plane * size + place, strides, stride=STRIDE), :] for plane in planes], 1
        ).astype(bf16)[:, :width]
        both = jnp.concatenate(
            [
                weight[pl.ds(place * width, width), :],
                weight[pl.ds((STRIDE + place) * width, width), :],
            ],
            1,
        )
        total = total + dot(part, both)
    return total


def hidden_of(first, second):
    strides = first.shape[0]
    later = pltpu.roll(second, strides - 1, axis=0)
    last = lax.broadcasted_iota(jnp.int32, later.shape, 0) == strides - 1
    return gelu(first + jnp.where(last, 0.0, later)).astype(bf16)


def unpack(block, rows, size, at):
    count = block.shape[1]
    for plane in range(2):
        part = block[plane * LANES : min((plane + 1) * LANES, DK), :].astype(f32).T
        rows[pl.ds(plane * size + at, count), : part.shape[1]] = part
    rows[pl.ds(2 * size + at, count), :] = block[DK:, :].astype(f32)


def codes_of(rows, size, key_in, key_out, value_in, value_out):
    shares = halves(rows, (0, 1), size, key_in, DK)
    key_hidden = hidden_of(shares[:, :LANES], shares[:, LANES:])
    code_keys = dot_t(key_out[...], key_hidden).astype(bf16)
    shares = halves(rows, (2,), size, value_in, DV)
    value_hidden = hidden_of(shares[:, :LANES], shares[:, LANES:])
    code_values = dot(value_hidden, value_out[...]).astype(bf16)
    return code_keys, code_values


def attend_body(
    here, count, reach, get_block, code_keys, code_values, codes, positions, q, parts, out, scratch
):
    even, odd, near_values, far_values, near_bias, far_bias, gates = scratch
    near = (reach + 1) * count
    far = even.shape[1] - near
    lengths = jnp.broadcast_to(positions[...].astype(f32), (count, count)).T.astype(jnp.int32)

    def lens(width):
        return jnp.concatenate([lengths] * (width // count), 1) if width > count else lengths

    def ids(width, axis):
        return lax.broadcasted_iota(jnp.int32, (count, width), axis)

    token = here * count + ids(near, 0)
    key = (here - reach) * count + ids(near, 1)
    seen = (key <= token) & (key > token - WINDOW) & (key >= token - lens(near)) & (key >= 0)
    near_bias[...] = jnp.where(seen, 0.0, NEG)
    token = here * count + ids(far, 0)
    first = STRIDE * ids(far, 1)
    seen = (first + (BLOCK - 1) <= token) & (first >= token - lens(far)) & (ids(far, 1) < codes)
    far_bias[...] = jnp.where(seen, 0.0, NEG)
    some = jnp.max(jnp.where(seen, 1.0, 0.0), axis=1, keepdims=True)

    total = parts[0][...]
    for part in parts[1:]:
        total = total + part[...]
    total = jax.nn.sigmoid(total)
    total = jnp.concatenate([total, jnp.zeros((LANES - 2 * QH, count), f32)], 0).T
    coarse_lane = lax.broadcasted_iota(jnp.int32, total.shape, 1) < QH
    gates[...] = jnp.where(coarse_lane, total * some, total)

    even[DK:, :] = jnp.zeros((PAD - DK, near + far), bf16)
    odd[: PAD - DK, :] = jnp.zeros((PAD - DK, near + far), bf16)
    near_values[:, DV:] = jnp.ones((near, DV), bf16)
    far_values[:, DV:] = jnp.ones((far, DV), bf16)
    for step in range(reach + 1):
        block = get_block(jnp.maximum(here - reach + step, 0), step)
        lanes = slice(step * count, (step + 1) * count)
        even[:DK, lanes] = block[:DK, :]
        odd[PAD - DK :, lanes] = block[:DK, :]
        near_values[lanes, :DV] = block[DK:, :]
    even[:DK, near:] = code_keys
    odd[PAD - DK :, near:] = code_keys
    far_values[:, :DV] = code_values

    pair = 2 * DK
    for side in (0, 1):
        keys = (even, odd)[side]
        for chunk in range(0, QH // 2, GROUP):
            rows = jnp.concatenate(
                [
                    q[:, (chunk + j) * pair + side * LANES : (chunk + j) * pair + side * LANES + PAD]
                    for j in range(GROUP)
                ],
                0,
            )
            scores = dot(rows, keys[...])

            def branch(scores, bias, values):
                width = scores.shape[1]
                scores = scores.reshape(GROUP, count, width) + bias[...][None]
                top = jnp.max(scores, axis=2, keepdims=True)
                weights = jnp.exp2((scores - top) * SCALE).astype(bf16)
                summed = dot(weights.reshape(GROUP * count, width), values[...])
                return summed[:, :DV] / jnp.maximum(summed[:, DV:], 1.0)

            local = branch(scores[:, :near], near_bias, near_values)
            coarse = branch(scores[:, near:], far_bias, far_values)
            for j in range(GROUP):
                head = 2 * (chunk + j) + side
                at = slice(j * count, (j + 1) * count)
                mixed = (
                    gates[:, head : head + 1] * coarse[at]
                    + gates[:, QH + head : QH + head + 1] * local[at]
                )
                out[:, head * DV : (head + 1) * DV] = mixed.astype(bf16)


def attend_scratch(count, reach, far):
    near = (reach + 1) * count
    return [
        pltpu.VMEM((PAD, near + far), bf16),
        pltpu.VMEM((PAD, near + far), bf16),
        pltpu.VMEM((near, 2 * DV), bf16),
        pltpu.VMEM((far, 2 * DV), bf16),
        pltpu.VMEM((count, near), f32),
        pltpu.VMEM((count, far), f32),
        pltpu.VMEM((count, LANES), f32),
    ]


def gate_columns(parts, some):
    total = parts[0][...]
    for part in parts[1:]:
        total = total + part[...]
    total = jax.nn.sigmoid(total)
    total = jnp.concatenate([total, jnp.zeros((LANES - 2 * QH, total.shape[1]), f32)], 0).T
    coarse_lane = lax.broadcasted_iota(jnp.int32, total.shape, 1) < QH
    return jnp.where(coarse_lane, total * some, total)


def fill_keys(even, odd, lanes, keys):
    even[:DK, lanes] = keys
    even[DK:, lanes] = jnp.zeros((PAD - DK, keys.shape[1]), bf16)
    odd[: PAD - DK, lanes] = jnp.zeros((PAD - DK, keys.shape[1]), bf16)
    odd[PAD - DK :, lanes] = keys


def query_rows(q, side, chunk, heads):
    starts = [(chunk + j) * 2 * DK + side * LANES for j in range(heads)]
    return jnp.concatenate([q[:, start : start + PAD] for start in starts], 0)


def place_of(here, offset):
    block = here - offset
    return jnp.where(block >= 0, (block ^ here) >> 1, 0)


def early_kernel(slots, count, offsets, here_ref, q, bias, key_in, value_in, *refs):
    blocks, (shares, summed, tops) = refs[:slots], refs[slots : slots + 3]
    held, rows, even, odd, values = refs[slots + 3 :]
    here = here_ref[0]
    for i, block in enumerate(blocks):
        held[i] = block[...]
        unpack(block, rows, slots * count, i * count)
    near = len(offsets) * count
    for step, offset in enumerate(offsets):
        block = held[place_of(here, offset)]
        lanes = slice(step * count, (step + 1) * count)
        fill_keys(even, odd, lanes, block[:DK, :])
        values[lanes, :DV] = block[DK:, :]
    values[:, DV:] = jnp.ones((near, DV), bf16)
    shares[:, : 2 * LANES] = halves(rows, (0, 1), slots * count, key_in, DK)
    shares[:, 2 * LANES :] = halves(rows, (2,), slots * count, value_in, DV)
    for side in (0, 1):
        for chunk in range(0, QH // 2, GROUP):
            scores = dot(query_rows(q, side, chunk, GROUP), (even, odd)[side][...])
            scores = scores.reshape(GROUP, count, near) + bias[:, :near][None]
            top = jnp.max(scores, axis=2, keepdims=True)
            weights = jnp.exp2((scores - top) * SCALE).astype(bf16)
            at = pl.ds((side * QH // 2 + chunk) * count, GROUP * count)
            summed[at, :] = dot(weights.reshape(GROUP * count, near), values[...])
            tops[at, :] = jnp.broadcast_to(top, (GROUP, count, LANES)).reshape(GROUP * count, LANES)


def split(refs):
    size = DK + DV
    return [ref.at[pl.ds(at, size), :] for ref in refs for at in range(0, ref.shape[0], size)]


def codes_from(key_shares, value_shares, second, far):
    key_hidden = hidden_of(key_shares[:, :LANES], key_shares[:, LANES:])
    keys = dot_t(second[:DK, :], key_hidden).astype(bf16)
    value_hidden = hidden_of(value_shares[:, :LANES], value_shares[:, LANES:])
    values = dot(value_hidden, second[DK:, :]).astype(bf16)
    codes = values.shape[0]
    if far > codes:
        keys = jnp.concatenate([keys, jnp.zeros((DK, far - codes), bf16)], 1)
        values = jnp.concatenate([values, jnp.zeros((far - codes, DV), bf16)], 0)
    return keys, values


def share_rows(here, slot, strides):
    return pl.ds(pl.multiple_of((here ^ slot) * strides, strides), strides)


def mid_kernel(buffers, slots, count, here_ref, second, key_in, value_in, shares, *refs):
    blocks = split(refs[:buffers])
    key_shares, value_shares, code_keys, code_values, rows = refs[buffers:]
    here = here_ref[0]
    strides = count // STRIDE
    total = len(blocks) * count
    for i, block in enumerate(blocks):
        unpack(block, rows, total, i * count)
    key_mid = halves(rows, (0, 1), total, key_in, DK)
    value_mid = halves(rows, (2,), total, value_in, DV)
    for i in range(slots):
        mine = slice(i * strides, (i + 1) * strides)
        at = share_rows(here, 2 * i, strides)
        key_shares[at, :] = shares[mine, : 2 * LANES]
        value_shares[at, :] = shares[mine, 2 * LANES :]
        at = share_rows(here, 2 * i + 1, strides)
        known = i < len(blocks)
        key_shares[at, :] = key_mid[mine] if known else jnp.zeros((strides, 2 * LANES), f32)
        value_shares[at, :] = value_mid[mine] if known else jnp.zeros((strides, 2 * LANES), f32)
    code_keys[...], code_values[...] = codes_from(key_shares, value_shares, second, code_values.shape[0])


def late_kernel(
    buffers, slots, heads, count, offsets, done, here_ref, q, bias, some, second, key_in, value_in,
    mid_key_shares, mid_value_shares, code_keys, code_values, summed, tops, *refs
):
    came, parts, out = refs[:buffers], refs[buffers : buffers + heads], refs[buffers + heads]
    held, rows, even, odd, values, far_values, key_shares, value_shares, gates = refs[buffers + heads + 1 :]
    blocks = split(came)
    here = here_ref[0]
    strides = count // STRIDE
    for i, block in enumerate(blocks):
        held[i] = block[...]
    near = len(offsets) * count
    for step, offset in enumerate(offsets):
        block = held[place_of(here, offset)]
        lanes = slice(step * count, (step + 1) * count)
        fill_keys(even, odd, lanes, block[:DK, :])
        values[lanes, :DV] = block[DK:, :]
    values[:, DV:] = jnp.ones((near, DV), bf16)
    far = far_values.shape[0]
    far_values[:, DV:] = jnp.ones((far, DV), bf16)

    def put(keys, found):
        fill_keys(even, odd, slice(near, near + far), keys)
        far_values[:, :DV] = found

    last = [i for i in range(slots) if i >= MID_BLOCKS]
    needed = functools.reduce(jnp.logical_or, [(here ^ (2 * i + 1)) < here for i in last], False)

    @pl.when(needed)
    def _():
        total = len(last) * count
        for j, i in enumerate(last):
            unpack(blocks[i], rows, total, j * count)
        key_last = halves(rows, (0, 1), total, key_in, DK)
        value_last = halves(rows, (2,), total, value_in, DV)
        key_shares[...] = mid_key_shares[...]
        value_shares[...] = mid_value_shares[...]
        for j, i in enumerate(last):
            at = share_rows(here, 2 * i + 1, strides)
            key_shares[at, :] = key_last[j * strides : (j + 1) * strides]
            value_shares[at, :] = value_last[j * strides : (j + 1) * strides]
        put(*codes_from(key_shares, value_shares, second, far))

    @pl.when(jnp.logical_not(needed))
    def _():
        put(code_keys[...], code_values[...])

    gates[...] = gate_columns(parts, some[...])
    size = LATE_GROUP * count
    for side in (0, 1):
        for chunk in range(0, QH // 2, LATE_GROUP):
            at = pl.ds((side * QH // 2 + chunk) * count, size)
            scores = dot(query_rows(q, side, chunk, LATE_GROUP), (even, odd)[side][...])
            scores = scores.reshape(LATE_GROUP, count, near + far) + bias[:, done:][None]
            local, coarse = scores[:, :, :near], scores[:, :, near:]
            before = tops[at, :].reshape(LATE_GROUP, count, LANES)
            top = jnp.maximum(before, jnp.max(local, axis=2, keepdims=True))
            tops_near = jnp.concatenate([top] * (near // LANES), 2)
            weights = jnp.exp2((local - tops_near) * SCALE).astype(bf16)
            fade = jnp.exp2((before - top) * SCALE).reshape(size, LANES)
            old = summed[at, :] * jnp.concatenate([fade] * (2 * DV // LANES), 1)
            new = old + dot(weights.reshape(size, near), values[...])
            local = new[:, :DV] / jnp.maximum(new[:, DV:], 1.0)
            top = jnp.max(coarse, axis=2, keepdims=True)
            weights = jnp.exp2((coarse - top) * SCALE).astype(bf16)
            new = dot(weights.reshape(size, far), far_values[...])
            coarse = new[:, :DV] / jnp.maximum(new[:, DV:], 1.0)
            for j in range(LATE_GROUP):
                head = 2 * (chunk + j) + side
                mine = slice(j * count, (j + 1) * count)
                mixed = (
                    gates[:, head : head + 1] * coarse[mine]
                    + gates[:, QH + head : QH + head + 1] * local[mine]
                )
                out[:, head * DV : (head + 1) * DV] = mixed.astype(bf16)


def join_kernel(*refs):
    *blocks, out = refs
    size = blocks[0].shape[0]
    for i, block in enumerate(blocks):
        out[i * size : (i + 1) * size, :] = block[...]


def join(blocks):
    size, count = blocks[0].shape
    vmem = pl.BlockSpec(memory_space=pltpu.VMEM)
    return pl.pallas_call(
        join_kernel,
        in_specs=[vmem] * len(blocks),
        out_specs=vmem,
        out_shape=jax.ShapeDtypeStruct((len(blocks) * size, count), bf16),
        compiler_params=pltpu.CompilerParams(vmem_limit_bytes=VMEM_LIMIT),
        name="join",
    )(*blocks)


def small_slab(here, group, positions, queries, block, features, gate_weight, weights, length, heads, reach):
    count = queries.shape[0]
    codes = length * count // STRIDE
    far = up(codes, LANES)
    first = tuple(range(reach - reach % 2, -1, -2))
    then = tuple(range(reach - (reach + 1) % 2, 0, -2))
    key_in, key_out, value_in, value_out = weights
    slots = {0: block}
    for d in range(2, length, 2):
        slots[d] = swap(block, "seq", d)
    parts, (bias, some, second, queries, key_in, value_in) = prepare(
        here, group, positions, features, gate_weight, heads, first + then, codes,
        (queries, key_in, value_in, key_out, value_out),
    )
    for d in range(2, length, 2):
        slots[d] = lax.optimization_barrier((slots[d], parts))[0]
    across = [swap(block, "seq", 1)]
    across.append(swap(join([slots[d] for d in range(2, min(length, 6), 2)]), "seq", 1))
    for d in range(6, length, 2):
        across.append(swap(slots[d], "seq", 1))
    parts = exchange(parts)
    half = length // 2
    smem, vmem = pl.BlockSpec(memory_space=pltpu.SMEM), pl.BlockSpec(memory_space=pltpu.VMEM)
    params = pltpu.CompilerParams(vmem_limit_bytes=VMEM_LIMIT)
    rows = [
        pltpu.VMEM((half, DK + DV, count), bf16),
        pltpu.VMEM((3 * half * count, LANES), f32),
    ]
    near = len(first) * count
    shares, summed, tops = pl.pallas_call(
        functools.partial(early_kernel, half, count, first),
        in_specs=[smem] + [vmem] * (4 + half),
        out_specs=[vmem] * 3,
        out_shape=[
            jax.ShapeDtypeStruct((codes // 2, 4 * LANES), f32),
            jax.ShapeDtypeStruct((QH * count, 2 * DV), f32),
            jax.ShapeDtypeStruct((QH * count, LANES), f32),
        ],
        scratch_shapes=rows
        + [pltpu.VMEM((PAD, near), bf16)] * 2
        + [pltpu.VMEM((near, 2 * DV), bf16)],
        compiler_params=params,
        cost_estimate=pl.CostEstimate(flops=4 << 30, transcendentals=1 << 20, bytes_accessed=1 << 22),
        name="early",
    )(here[None], queries, bias, key_in, value_in, *[slots[d] for d in range(0, length, 2)])
    done = near
    near = len(then) * count
    ahead = [value for value in across if value is not across[-1]] if len(across) > 2 else across
    made = pl.pallas_call(
        functools.partial(mid_kernel, len(ahead), half, count),
        in_specs=[smem] + [vmem] * (4 + len(ahead)),
        out_specs=[vmem] * 4,
        out_shape=[jax.ShapeDtypeStruct((codes, 2 * LANES), f32)] * 2
        + [jax.ShapeDtypeStruct((DK, far), bf16), jax.ShapeDtypeStruct((far, DV), bf16)],
        scratch_shapes=[pltpu.VMEM((3 * half * count, LANES), f32)],
        compiler_params=params,
        name="mid",
    )(here[None], second, key_in, value_in, shares, *ahead)
    return pl.pallas_call(
        functools.partial(late_kernel, len(across), half, heads, count, then, done),
        in_specs=[smem] + [vmem] * (12 + len(across) + heads),
        out_specs=vmem,
        out_shape=jax.ShapeDtypeStruct((count, QH * DV), bf16),
        scratch_shapes=rows
        + [pltpu.VMEM((PAD, near + far), bf16)] * 2
        + [pltpu.VMEM((near, 2 * DV), bf16), pltpu.VMEM((far, 2 * DV), bf16)]
        + [pltpu.VMEM((codes, 2 * LANES), f32)] * 2
        + [pltpu.VMEM((count, LANES), f32)],
        compiler_params=params,
        name="late",
    )(
        here[None], queries, bias, some, second, key_in, value_in, *made, summed, tops,
        *across, *parts,
    )


def codes_kernel(before, block, key_in, key_out, value_in, value_out, out, rows):
    count = block.shape[1]
    unpack(before[...], rows, 2 * count, 0)
    unpack(block[...], rows, 2 * count, count)
    code_keys, code_values = codes_of(rows, 2 * count, key_in, key_out, value_in, value_out)
    out[:, :DK] = code_keys.astype(f32).T
    out[:, DK:] = code_values.astype(f32)


def near_kernel(heads, count, reach, codes, here_ref, *refs):
    positions, q = refs[:2]
    blocks = refs[2 : 3 + reach]
    code_keys, code_values = refs[3 + reach : 5 + reach]
    parts = refs[5 + reach : 5 + reach + heads]
    out = refs[5 + reach + heads]
    attend_body(
        here_ref[0], count, reach, lambda at, step: blocks[step][...], code_keys[...], code_values[...],
        codes, positions, q, parts, out, refs[6 + reach + heads :],
    )


def long_slab(here, positions, queries, block, weights, parts, reach, length):
    count = queries.shape[0]
    strides = count // STRIDE
    smem, vmem = pl.BlockSpec(memory_space=pltpu.SMEM), pl.BlockSpec(memory_space=pltpu.VMEM)
    earlier = [turn(block, "seq", reach - k) for k in range(reach)]
    made = pl.pallas_call(
        codes_kernel,
        in_specs=[vmem] * 6,
        out_specs=vmem,
        out_shape=jax.ShapeDtypeStruct((2 * strides, DK + DV), f32),
        scratch_shapes=[pltpu.VMEM((6 * count, LANES), f32)],
        name="codes",
    )(earlier[-1], block, *weights)
    mine = made[strides - 1 : 2 * strides - 1].astype(bf16)
    every = lax.all_gather(mine, "seq", axis=0, tiled=True)[1:]
    codes = length * count // STRIDE
    far = up(codes, LANES)
    every = jnp.concatenate([every, jnp.zeros((far - every.shape[0], DK + DV), bf16)], 0)
    return pl.pallas_call(
        functools.partial(near_kernel, len(parts), count, reach, codes),
        in_specs=[smem] + [vmem] * (5 + reach + len(parts)),
        out_specs=vmem,
        out_shape=jax.ShapeDtypeStruct((count, QH * DV), bf16),
        scratch_shapes=attend_scratch(count, reach, far),
        name="long_slab",
    )(here[None], positions[None, :], queries, *earlier, block, every[:, :DK].T, every[:, DK:], *parts)


def on_device(
    queries, keys, values, features, positions, gate_weight, key_in, key_out, value_in, value_out
):
    count = keys.shape[0]
    length, heads = lax.axis_size("seq"), lax.axis_size("head")
    here = lax.axis_index("seq")
    group = lax.axis_index("head")
    reach = -(-WINDOW // count)
    block = jnp.concatenate([keys.T, values], 0)
    weights = (key_in[0], key_out[0].T, value_in[0], value_out[0])
    if length <= MOST_SLOTS and length > 1 and length & (length - 1) == 0:
        return small_slab(
            here, group, positions, queries, block, features, gate_weight, weights, length, heads, reach
        )
    parts = exchange(gate_logits(features, gate_weight, group, heads))
    return long_slab(here, positions, queries, block, weights, parts, reach, length)


def solution(mesh):
    return jax.shard_map(
        on_device,
        mesh=mesh,
        in_specs=(
            P("seq", "head"),
            P("seq", "head"),
            P("seq", "head"),
            P("seq", "head"),
            P("seq"),
            P(),
            P("head", None, None),
            P("head", None, None),
            P("head", None, None),
            P("head", None, None),
        ),
        out_specs=P("seq", "head"),
        check_vma=False,
    )
```

```python
import functools

import jax
import jax.numpy as jnp
from jax import lax
from jax.experimental import pallas as pl
from jax.experimental.pallas import tpu as pltpu
from jax.sharding import PartitionSpec as P

QH = 16
DK = 192
DV = 128
STRIDE = 16
BLOCK = 32
WINDOW = 512
LANES = 128
PAD = 256
GROUP = 4
LATE_GROUP = 8
MID_BLOCKS = 3
VMEM_LIMIT = 24 << 20
MOST_SLOTS = 8

NEG = -1e30
SCALE = DK ** (-0.5) * 1.4426950408889634

f32 = jnp.float32
bf16 = jnp.bfloat16


def up(value, step):
    return -(-value // step) * step


def swap(value, axis, by):
    length = lax.axis_size(axis)
    return lax.ppermute(value, axis, [(i, i ^ by) for i in range(length)])


def turn(value, axis, by):
    length = lax.axis_size(axis)
    return lax.ppermute(value, axis, [(i, (i + by) % length) for i in range(length)])


def dot(left, right):
    return jnp.dot(left, right, preferred_element_type=f32)


def dot_t(left, right):
    return lax.dot_general(left, right, (((1,), (1,)), ((), ())), preferred_element_type=f32)


def place_hbm(value):
    return pltpu.with_memory_space_constraint(value, pltpu.HBM)


def logits_of(group, heads, features, columns, total, outs):
    total[...] = lax.dot_general(
        columns[...], features[...], (((0,), (1,)), ((), ())), preferred_element_type=f32
    )
    for step, out in enumerate(outs):
        other = group ^ step if heads & (heads - 1) == 0 else lax.rem(group + step, heads)
        out[...] = total[pl.ds(pl.multiple_of(other * (2 * QH), 2 * QH), 2 * QH), :]


def feature_copies(group, features_hbm, columns_hbm, features, columns, sems):
    depth = features.shape[1]
    first = pl.multiple_of(group * depth, LANES)
    return [
        pltpu.make_async_copy(features_hbm, features, sems.at[0]),
        pltpu.make_async_copy(columns_hbm.at[pl.ds(first, depth), :], columns, sems.at[1]),
    ]


def logit_kernel(heads, group, features_hbm, columns_hbm, *refs):
    outs, (features, columns, total, sems) = refs[:heads], refs[heads:]
    copies = feature_copies(group[0], features_hbm, columns_hbm, features, columns, sems)
    for copy in copies:
        copy.start()
    for copy in copies:
        copy.wait()
    logits_of(group[0], heads, features, columns, total, outs)


def prepare_kernel(heads, kept, offsets, codes, here_ref, group_ref, features_hbm, columns_hbm, positions_hbm, *refs):
    here, group = here_ref[0], group_ref[0]
    sources = refs[:kept]
    outs = refs[kept : kept + heads]
    bias, some, second = refs[kept + heads : kept + heads + 3]
    places = refs[kept + heads + 3 : 2 * kept + heads + 1]
    features, columns, total, positions, sems = refs[2 * kept + heads + 1 :]
    places = [*places, second.at[pl.ds(0, DK), :], second.at[pl.ds(DK, sources[-1].shape[0]), :]]
    copies = feature_copies(group, features_hbm, columns_hbm, features, columns, sems)
    copies.append(pltpu.make_async_copy(positions_hbm, positions, sems.at[2]))
    copies += [
        pltpu.make_async_copy(source, place, sems.at[3 + i])
        for i, (source, place) in enumerate(zip(sources, places))
    ]
    for copy in copies:
        copy.start()
    for copy in copies[:3]:
        copy.wait()
    logits_of(group, heads, features, columns, total, outs)
    count = positions.shape[1]
    lengths = jnp.broadcast_to(positions[...].astype(f32), (count, count)).T.astype(jnp.int32)
    token = here * count + lax.broadcasted_iota(jnp.int32, (count, count), 0)
    lane = lax.broadcasted_iota(jnp.int32, (count, count), 1)
    for step, offset in enumerate(offsets):
        key = (here - offset) * count + lane
        seen = (key <= token) & (key > token - WINDOW) & (key >= token - lengths) & (key >= 0)
        bias[:, step * count : (step + 1) * count] = jnp.where(seen, 0.0, NEG)
    near = len(offsets) * count
    most = jnp.full((count, LANES), NEG, f32)
    for start in range(near, bias.shape[1], LANES):
        code = start - near + lax.broadcasted_iota(jnp.int32, (count, LANES), 1)
        token = here * count + lax.broadcasted_iota(jnp.int32, (count, LANES), 0)
        length = lengths if count == LANES else jnp.broadcast_to(lengths[:, :1], (count, LANES))
        first = STRIDE * code
        seen = (first + (BLOCK - 1) <= token) & (first >= token - length) & (code < codes)
        part = jnp.where(seen, 0.0, NEG)
        bias[:, start : start + LANES] = part
        most = jnp.maximum(most, part)
    some[...] = jnp.where(
        jnp.broadcast_to(jnp.max(most, axis=1, keepdims=True), (count, LANES)) > 0.5 * NEG, 1.0, 0.0
    )
    for copy in copies[3:]:
        copy.wait()


def gate_shapes(count, depth, columns):
    return [
        pltpu.VMEM((count, depth), bf16),
        pltpu.VMEM((depth, columns), bf16),
        pltpu.VMEM((columns, count), f32),
    ]


def gate_logits(features, gate_weight, group, heads):
    count, depth = features.shape
    vmem, hbm = pl.BlockSpec(memory_space=pltpu.VMEM), pl.BlockSpec(memory_space=pltpu.HBM)
    return pl.pallas_call(
        functools.partial(logit_kernel, heads),
        in_specs=[pl.BlockSpec(memory_space=pltpu.SMEM), hbm, hbm],
        out_specs=[vmem] * heads,
        out_shape=[jax.ShapeDtypeStruct((2 * QH, count), f32)] * heads,
        scratch_shapes=gate_shapes(count, depth, gate_weight.shape[1])
        + [pltpu.SemaphoreType.DMA((2,))],
        compiler_params=pltpu.CompilerParams(vmem_limit_bytes=VMEM_LIMIT),
        name="gate_logits",
    )(group[None], features, gate_weight)


def prepare(here, group, positions, features, gate_weight, heads, offsets, codes, kept):
    count, depth = features.shape
    vmem, hbm = pl.BlockSpec(memory_space=pltpu.VMEM), pl.BlockSpec(memory_space=pltpu.HBM)
    wide = len(offsets) * count + up(codes, LANES)
    last = kept[-2:]
    made = pl.pallas_call(
        functools.partial(prepare_kernel, heads, len(kept), offsets, codes),
        in_specs=[pl.BlockSpec(memory_space=pltpu.SMEM)] * 2 + [hbm] * (3 + len(kept)),
        out_specs=[vmem] * (heads + 1 + len(kept)),
        out_shape=[jax.ShapeDtypeStruct((2 * QH, count), f32)] * heads
        + [
            jax.ShapeDtypeStruct((count, wide), f32),
            jax.ShapeDtypeStruct((count, LANES), f32),
            jax.ShapeDtypeStruct((last[0].shape[0] + last[1].shape[0], last[1].shape[1]), bf16),
        ]
        + [jax.ShapeDtypeStruct(value.shape, value.dtype) for value in kept[:-2]],
        scratch_shapes=gate_shapes(count, depth, gate_weight.shape[1])
        + [pltpu.VMEM((1, count), jnp.int32), pltpu.SemaphoreType.DMA((3 + len(kept),))],
        compiler_params=pltpu.CompilerParams(vmem_limit_bytes=VMEM_LIMIT),
        name="prepare",
    )(
        here[None],
        group[None],
        *[place_hbm(value) for value in (features, gate_weight, positions[None, :], *kept)],
    )
    return made[:heads], made[heads:]


def exchange(parts):
    heads = len(parts)
    if heads & (heads - 1) == 0:
        return [parts[0]] + [swap(parts[d], "head", d) for d in range(1, heads)]
    return [parts[0]] + [turn(parts[d], "head", d) for d in range(1, heads)]


def gelu(x):
    return 0.5 * x * (1.0 + jnp.tanh(0.7978845608028654 * (x + 0.044715 * x * x * x)))


def halves(rows, planes, size, weight, width):
    strides = size // STRIDE
    total = jnp.zeros((strides, 2 * LANES), f32)
    for place in range(STRIDE):
        part = jnp.concatenate(
            [rows[pl.ds(plane * size + place, strides, stride=STRIDE), :] for plane in planes], 1
        ).astype(bf16)[:, :width]
        both = jnp.concatenate(
            [
                weight[pl.ds(place * width, width), :],
                weight[pl.ds((STRIDE + place) * width, width), :],
            ],
            1,
        )
        total = total + dot(part, both)
    return total


def hidden_of(first, second):
    strides = first.shape[0]
    later = pltpu.roll(second, strides - 1, axis=0)
    last = lax.broadcasted_iota(jnp.int32, later.shape, 0) == strides - 1
    return gelu(first + jnp.where(last, 0.0, later)).astype(bf16)


def unpack(block, rows, size, at):
    count = block.shape[1]
    for plane in range(2):
        part = block[plane * LANES : min((plane + 1) * LANES, DK), :].astype(f32).T
        rows[pl.ds(plane * size + at, count), : part.shape[1]] = part
    rows[pl.ds(2 * size + at, count), :] = block[DK:, :].astype(f32)


def codes_of(rows, size, key_in, key_out, value_in, value_out):
    shares = halves(rows, (0, 1), size, key_in, DK)
    key_hidden = hidden_of(shares[:, :LANES], shares[:, LANES:])
    code_keys = dot_t(key_out[...], key_hidden).astype(bf16)
    shares = halves(rows, (2,), size, value_in, DV)
    value_hidden = hidden_of(shares[:, :LANES], shares[:, LANES:])
    code_values = dot(value_hidden, value_out[...]).astype(bf16)
    return code_keys, code_values


def attend_body(
    here, count, reach, get_block, code_keys, code_values, codes, positions, q, parts, out, scratch
):
    even, odd, near_values, far_values, near_bias, far_bias, gates = scratch
    near = (reach + 1) * count
    far = even.shape[1] - near
    lengths = jnp.broadcast_to(positions[...].astype(f32), (count, count)).T.astype(jnp.int32)

    def lens(width):
        return jnp.concatenate([lengths] * (width // count), 1) if width > count else lengths

    def ids(width, axis):
        return lax.broadcasted_iota(jnp.int32, (count, width), axis)

    token = here * count + ids(near, 0)
    key = (here - reach) * count + ids(near, 1)
    seen = (key <= token) & (key > token - WINDOW) & (key >= token - lens(near)) & (key >= 0)
    near_bias[...] = jnp.where(seen, 0.0, NEG)
    token = here * count + ids(far, 0)
    first = STRIDE * ids(far, 1)
    seen = (first + (BLOCK - 1) <= token) & (first >= token - lens(far)) & (ids(far, 1) < codes)
    far_bias[...] = jnp.where(seen, 0.0, NEG)
    some = jnp.max(jnp.where(seen, 1.0, 0.0), axis=1, keepdims=True)

    total = parts[0][...]
    for part in parts[1:]:
        total = total + part[...]
    total = jax.nn.sigmoid(total)
    total = jnp.concatenate([total, jnp.zeros((LANES - 2 * QH, count), f32)], 0).T
    coarse_lane = lax.broadcasted_iota(jnp.int32, total.shape, 1) < QH
    gates[...] = jnp.where(coarse_lane, total * some, total)

    even[DK:, :] = jnp.zeros((PAD - DK, near + far), bf16)
    odd[: PAD - DK, :] = jnp.zeros((PAD - DK, near + far), bf16)
    near_values[:, DV:] = jnp.ones((near, DV), bf16)
    far_values[:, DV:] = jnp.ones((far, DV), bf16)
    for step in range(reach + 1):
        block = get_block(jnp.maximum(here - reach + step, 0), step)
        lanes = slice(step * count, (step + 1) * count)
        even[:DK, lanes] = block[:DK, :]
        odd[PAD - DK :, lanes] = block[:DK, :]
        near_values[lanes, :DV] = block[DK:, :]
    even[:DK, near:] = code_keys
    odd[PAD - DK :, near:] = code_keys
    far_values[:, :DV] = code_values

    pair = 2 * DK
    for side in (0, 1):
        keys = (even, odd)[side]
        for chunk in range(0, QH // 2, GROUP):
            rows = jnp.concatenate(
                [
                    q[:, (chunk + j) * pair + side * LANES : (chunk + j) * pair + side * LANES + PAD]
                    for j in range(GROUP)
                ],
                0,
            )
            scores = dot(rows, keys[...])

            def branch(scores, bias, values):
                width = scores.shape[1]
                scores = scores.reshape(GROUP, count, width) + bias[...][None]
                top = jnp.max(scores, axis=2, keepdims=True)
                weights = jnp.exp2((scores - top) * SCALE).astype(bf16)
                summed = dot(weights.reshape(GROUP * count, width), values[...])
                return summed[:, :DV] / jnp.maximum(summed[:, DV:], 1.0)

            local = branch(scores[:, :near], near_bias, near_values)
            coarse = branch(scores[:, near:], far_bias, far_values)
            for j in range(GROUP):
                head = 2 * (chunk + j) + side
                at = slice(j * count, (j + 1) * count)
                mixed = (
                    gates[:, head : head + 1] * coarse[at]
                    + gates[:, QH + head : QH + head + 1] * local[at]
                )
                out[:, head * DV : (head + 1) * DV] = mixed.astype(bf16)


def attend_scratch(count, reach, far):
    near = (reach + 1) * count
    return [
        pltpu.VMEM((PAD, near + far), bf16),
        pltpu.VMEM((PAD, near + far), bf16),
        pltpu.VMEM((near, 2 * DV), bf16),
        pltpu.VMEM((far, 2 * DV), bf16),
        pltpu.VMEM((count, near), f32),
        pltpu.VMEM((count, far), f32),
        pltpu.VMEM((count, LANES), f32),
    ]


def gate_columns(parts, some):
    total = parts[0][...]
    for part in parts[1:]:
        total = total + part[...]
    total = jax.nn.sigmoid(total)
    total = jnp.concatenate([total, jnp.zeros((LANES - 2 * QH, total.shape[1]), f32)], 0).T
    coarse_lane = lax.broadcasted_iota(jnp.int32, total.shape, 1) < QH
    return jnp.where(coarse_lane, total * some, total)


def fill_keys(even, odd, lanes, keys):
    even[:DK, lanes] = keys
    even[DK:, lanes] = jnp.zeros((PAD - DK, keys.shape[1]), bf16)
    odd[: PAD - DK, lanes] = jnp.zeros((PAD - DK, keys.shape[1]), bf16)
    odd[PAD - DK :, lanes] = keys


def query_rows(q, side, chunk, heads):
    starts = [(chunk + j) * 2 * DK + side * LANES for j in range(heads)]
    return jnp.concatenate([q[:, start : start + PAD] for start in starts], 0)


def place_of(here, offset):
    block = here - offset
    return jnp.where(block >= 0, (block ^ here) >> 1, 0)


def early_kernel(slots, count, offsets, here_ref, q, bias, key_in, value_in, *refs):
    blocks, (shares, summed, tops) = refs[:slots], refs[slots : slots + 3]
    held, rows, even, odd, values = refs[slots + 3 :]
    here = here_ref[0]
    for i, block in enumerate(blocks):
        held[i] = block[...]
        unpack(block, rows, slots * count, i * count)
    near = len(offsets) * count
    for step, offset in enumerate(offsets):
        block = held[place_of(here, offset)]
        lanes = slice(step * count, (step + 1) * count)
        fill_keys(even, odd, lanes, block[:DK, :])
        values[lanes, :DV] = block[DK:, :]
    values[:, DV:] = jnp.ones((near, DV), bf16)
    shares[:, : 2 * LANES] = halves(rows, (0, 1), slots * count, key_in, DK)
    shares[:, 2 * LANES :] = halves(rows, (2,), slots * count, value_in, DV)
    for side in (0, 1):
        for chunk in range(0, QH // 2, GROUP):
            scores = dot(query_rows(q, side, chunk, GROUP), (even, odd)[side][...])
            scores = scores.reshape(GROUP, count, near) + bias[:, :near][None]
            top = jnp.max(scores, axis=2, keepdims=True)
            weights = jnp.exp2((scores - top) * SCALE).astype(bf16)
            at = pl.ds((side * QH // 2 + chunk) * count, GROUP * count)
            summed[at, :] = dot(weights.reshape(GROUP * count, near), values[...])
            tops[at, :] = jnp.broadcast_to(top, (GROUP, count, LANES)).reshape(GROUP * count, LANES)


def split(refs):
    size = DK + DV
    return [ref.at[pl.ds(at, size), :] for ref in refs for at in range(0, ref.shape[0], size)]


def codes_from(key_shares, value_shares, second, far):
    key_hidden = hidden_of(key_shares[:, :LANES], key_shares[:, LANES:])
    keys = dot_t(second[:DK, :], key_hidden).astype(bf16)
    value_hidden = hidden_of(value_shares[:, :LANES], value_shares[:, LANES:])
    values = dot(value_hidden, second[DK:, :]).astype(bf16)
    codes = values.shape[0]
    if far > codes:
        keys = jnp.concatenate([keys, jnp.zeros((DK, far - codes), bf16)], 1)
        values = jnp.concatenate([values, jnp.zeros((far - codes, DV), bf16)], 0)
    return keys, values


def share_rows(here, slot, strides):
    return pl.ds(pl.multiple_of((here ^ slot) * strides, strides), strides)


def mid_kernel(buffers, slots, count, here_ref, second, key_in, value_in, shares, *refs):
    blocks = split(refs[:buffers])
    key_shares, value_shares, code_keys, code_values, rows = refs[buffers:]
    here = here_ref[0]
    strides = count // STRIDE
    total = len(blocks) * count
    for i, block in enumerate(blocks):
        unpack(block, rows, total, i * count)
    key_mid = halves(rows, (0, 1), total, key_in, DK)
    value_mid = halves(rows, (2,), total, value_in, DV)
    for i in range(slots):
        mine = slice(i * strides, (i + 1) * strides)
        at = share_rows(here, 2 * i, strides)
        key_shares[at, :] = shares[mine, : 2 * LANES]
        value_shares[at, :] = shares[mine, 2 * LANES :]
        at = share_rows(here, 2 * i + 1, strides)
        known = i < len(blocks)
        key_shares[at, :] = key_mid[mine] if known else jnp.zeros((strides, 2 * LANES), f32)
        value_shares[at, :] = value_mid[mine] if known else jnp.zeros((strides, 2 * LANES), f32)
    code_keys[...], code_values[...] = codes_from(key_shares, value_shares, second, code_values.shape[0])


def late_kernel(
    buffers, slots, heads, count, offsets, done, here_ref, q, bias, some, second, key_in, value_in,
    mid_key_shares, mid_value_shares, code_keys, code_values, summed, tops, *refs
):
    came, parts, out = refs[:buffers], refs[buffers : buffers + heads], refs[buffers + heads]
    held, rows, even, odd, values, far_values, key_shares, value_shares, gates = refs[buffers + heads + 1 :]
    blocks = split(came)
    here = here_ref[0]
    strides = count // STRIDE
    for i, block in enumerate(blocks):
        held[i] = block[...]
    near = len(offsets) * count
    for step, offset in enumerate(offsets):
        block = held[place_of(here, offset)]
        lanes = slice(step * count, (step + 1) * count)
        fill_keys(even, odd, lanes, block[:DK, :])
        values[lanes, :DV] = block[DK:, :]
    values[:, DV:] = jnp.ones((near, DV), bf16)
    far = far_values.shape[0]
    far_values[:, DV:] = jnp.ones((far, DV), bf16)

    def put(keys, found):
        fill_keys(even, odd, slice(near, near + far), keys)
        far_values[:, :DV] = found

    last = [i for i in range(slots) if i >= MID_BLOCKS]
    needed = functools.reduce(jnp.logical_or, [(here ^ (2 * i + 1)) < here for i in last], False)

    @pl.when(needed)
    def _():
        total = len(last) * count
        for j, i in enumerate(last):
            unpack(blocks[i], rows, total, j * count)
        key_last = halves(rows, (0, 1), total, key_in, DK)
        value_last = halves(rows, (2,), total, value_in, DV)
        key_shares[...] = mid_key_shares[...]
        value_shares[...] = mid_value_shares[...]
        for j, i in enumerate(last):
            at = share_rows(here, 2 * i + 1, strides)
            key_shares[at, :] = key_last[j * strides : (j + 1) * strides]
            value_shares[at, :] = value_last[j * strides : (j + 1) * strides]
        put(*codes_from(key_shares, value_shares, second, far))

    @pl.when(jnp.logical_not(needed))
    def _():
        put(code_keys[...], code_values[...])

    gates[...] = gate_columns(parts, some[...])
    size = LATE_GROUP * count

    def normal(summed):
        return summed[:, :DV] / jnp.maximum(summed[:, DV:], 1.0)

    def attend():
        for side in (0, 1):
            for chunk in range(0, QH // 2, LATE_GROUP):
                at = pl.ds((side * QH // 2 + chunk) * count, size)
                scores = dot(query_rows(q, side, chunk, LATE_GROUP), (even, odd)[side][...])
                scores = scores.reshape(LATE_GROUP, count, near + far) + bias[:, done:][None]
                local, coarse = scores[:, :, :near], scores[:, :, near:]
                before = tops[at, :].reshape(LATE_GROUP, count, LANES)
                top = jnp.maximum(before, jnp.max(local, axis=2, keepdims=True))
                tops_near = jnp.concatenate([top] * (near // LANES), 2)
                weights = jnp.exp2((local - tops_near) * SCALE).astype(bf16)
                fade = jnp.exp2((before - top) * SCALE).reshape(size, LANES)
                old = summed[at, :] * jnp.concatenate([fade] * (2 * DV // LANES), 1)
                local = normal(old + dot(weights.reshape(size, near), values[...]))
                top = jnp.max(coarse, axis=2, keepdims=True)
                weights = jnp.exp2((coarse - top) * SCALE).astype(bf16)
                coarse = normal(dot(weights.reshape(size, far), far_values[...]))
                for j in range(LATE_GROUP):
                    head = 2 * (chunk + j) + side
                    at = slice(j * count, (j + 1) * count)
                    mixed = (
                        gates[:, head : head + 1] * coarse[at]
                        + gates[:, QH + head : QH + head + 1] * local[at]
                    )
                    out[:, head * DV : (head + 1) * DV] = mixed.astype(bf16)

    pl.when(here >= 0)(attend)


def join_kernel(*refs):
    *blocks, out = refs
    size = blocks[0].shape[0]
    for i, block in enumerate(blocks):
        out[i * size : (i + 1) * size, :] = block[...]


def join(blocks):
    size, count = blocks[0].shape
    vmem = pl.BlockSpec(memory_space=pltpu.VMEM)
    return pl.pallas_call(
        join_kernel,
        in_specs=[vmem] * len(blocks),
        out_specs=vmem,
        out_shape=jax.ShapeDtypeStruct((len(blocks) * size, count), bf16),
        compiler_params=pltpu.CompilerParams(vmem_limit_bytes=VMEM_LIMIT),
        name="join",
    )(*blocks)


def small_slab(here, group, positions, queries, block, features, gate_weight, weights, length, heads, reach):
    count = queries.shape[0]
    codes = length * count // STRIDE
    far = up(codes, LANES)
    first = tuple(range(reach - reach % 2, -1, -2))
    then = tuple(range(reach - (reach + 1) % 2, 0, -2))
    key_in, key_out, value_in, value_out = weights
    slots = {0: block}
    for d in range(2, length, 2):
        slots[d] = swap(block, "seq", d)
    parts, (bias, some, second, queries, key_in, value_in) = prepare(
        here, group, positions, features, gate_weight, heads, first + then, codes,
        (queries, key_in, value_in, key_out, value_out),
    )
    for d in range(2, length, 2):
        slots[d] = lax.optimization_barrier((slots[d], parts))[0]
    across = [swap(block, "seq", 1)]
    across.append(swap(join([slots[d] for d in range(2, min(length, 6), 2)]), "seq", 1))
    for d in range(6, length, 2):
        across.append(swap(slots[d], "seq", 1))
    parts = exchange(parts)
    half = length // 2
    smem, vmem = pl.BlockSpec(memory_space=pltpu.SMEM), pl.BlockSpec(memory_space=pltpu.VMEM)
    params = pltpu.CompilerParams(vmem_limit_bytes=VMEM_LIMIT)
    rows = [
        pltpu.VMEM((half, DK + DV, count), bf16),
        pltpu.VMEM((3 * half * count, LANES), f32),
    ]
    near = len(first) * count
    shares, summed, tops = pl.pallas_call(
        functools.partial(early_kernel, half, count, first),
        in_specs=[smem] + [vmem] * (4 + half),
        out_specs=[vmem] * 3,
        out_shape=[
            jax.ShapeDtypeStruct((codes // 2, 4 * LANES), f32),
            jax.ShapeDtypeStruct((QH * count, 2 * DV), f32),
            jax.ShapeDtypeStruct((QH * count, LANES), f32),
        ],
        scratch_shapes=rows
        + [pltpu.VMEM((PAD, near), bf16)] * 2
        + [pltpu.VMEM((near, 2 * DV), bf16)],
        compiler_params=params,
        cost_estimate=pl.CostEstimate(flops=4 << 30, transcendentals=1 << 20, bytes_accessed=1 << 22),
        name="early",
    )(here[None], queries, bias, key_in, value_in, *[slots[d] for d in range(0, length, 2)])
    done = near
    near = len(then) * count
    ahead = [value for value in across if value is not across[-1]] if len(across) > 2 else across
    made = pl.pallas_call(
        functools.partial(mid_kernel, len(ahead), half, count),
        in_specs=[smem] + [vmem] * (4 + len(ahead)),
        out_specs=[vmem] * 4,
        out_shape=[jax.ShapeDtypeStruct((codes, 2 * LANES), f32)] * 2
        + [jax.ShapeDtypeStruct((DK, far), bf16), jax.ShapeDtypeStruct((far, DV), bf16)],
        scratch_shapes=[pltpu.VMEM((3 * half * count, LANES), f32)],
        compiler_params=params,
        name="mid",
    )(here[None], second, key_in, value_in, shares, *ahead)
    return pl.pallas_call(
        functools.partial(late_kernel, len(across), half, heads, count, then, done),
        in_specs=[smem] + [vmem] * (12 + len(across) + heads),
        out_specs=vmem,
        out_shape=jax.ShapeDtypeStruct((count, QH * DV), bf16),
        scratch_shapes=rows
        + [pltpu.VMEM((PAD, near + far), bf16)] * 2
        + [pltpu.VMEM((near, 2 * DV), bf16), pltpu.VMEM((far, 2 * DV), bf16)]
        + [pltpu.VMEM((codes, 2 * LANES), f32)] * 2
        + [pltpu.VMEM((count, LANES), f32)],
        compiler_params=params,
        name="late",
    )(
        here[None], queries, bias, some, second, key_in, value_in, *made, summed, tops,
        *across, *parts,
    )


def codes_kernel(before, block, key_in, key_out, value_in, value_out, out, rows):
    count = block.shape[1]
    unpack(before[...], rows, 2 * count, 0)
    unpack(block[...], rows, 2 * count, count)
    code_keys, code_values = codes_of(rows, 2 * count, key_in, key_out, value_in, value_out)
    out[:, :DK] = code_keys.astype(f32).T
    out[:, DK:] = code_values.astype(f32)


def near_kernel(heads, count, reach, codes, here_ref, *refs):
    positions, q = refs[:2]
    blocks = refs[2 : 3 + reach]
    code_keys, code_values = refs[3 + reach : 5 + reach]
    parts = refs[5 + reach : 5 + reach + heads]
    out = refs[5 + reach + heads]
    attend_body(
        here_ref[0], count, reach, lambda at, step: blocks[step][...], code_keys[...], code_values[...],
        codes, positions, q, parts, out, refs[6 + reach + heads :],
    )


def long_slab(here, positions, queries, block, weights, parts, reach, length):
    count = queries.shape[0]
    strides = count // STRIDE
    smem, vmem = pl.BlockSpec(memory_space=pltpu.SMEM), pl.BlockSpec(memory_space=pltpu.VMEM)
    earlier = [turn(block, "seq", reach - k) for k in range(reach)]
    made = pl.pallas_call(
        codes_kernel,
        in_specs=[vmem] * 6,
        out_specs=vmem,
        out_shape=jax.ShapeDtypeStruct((2 * strides, DK + DV), f32),
        scratch_shapes=[pltpu.VMEM((6 * count, LANES), f32)],
        name="codes",
    )(earlier[-1], block, *weights)
    mine = made[strides - 1 : 2 * strides - 1].astype(bf16)
    every = lax.all_gather(mine, "seq", axis=0, tiled=True)[1:]
    codes = length * count // STRIDE
    far = up(codes, LANES)
    every = jnp.concatenate([every, jnp.zeros((far - every.shape[0], DK + DV), bf16)], 0)
    return pl.pallas_call(
        functools.partial(near_kernel, len(parts), count, reach, codes),
        in_specs=[smem] + [vmem] * (5 + reach + len(parts)),
        out_specs=vmem,
        out_shape=jax.ShapeDtypeStruct((count, QH * DV), bf16),
        scratch_shapes=attend_scratch(count, reach, far),
        name="long_slab",
    )(here[None], positions[None, :], queries, *earlier, block, every[:, :DK].T, every[:, DK:], *parts)


def on_device(
    queries, keys, values, features, positions, gate_weight, key_in, key_out, value_in, value_out
):
    count = keys.shape[0]
    length, heads = lax.axis_size("seq"), lax.axis_size("head")
    here = lax.axis_index("seq")
    group = lax.axis_index("head")
    reach = -(-WINDOW // count)
    block = jnp.concatenate([keys.T, values], 0)
    weights = (key_in[0], key_out[0].T, value_in[0], value_out[0])
    if length <= MOST_SLOTS and length > 1 and length & (length - 1) == 0:
        return small_slab(
            here, group, positions, queries, block, features, gate_weight, weights, length, heads, reach
        )
    parts = exchange(gate_logits(features, gate_weight, group, heads))
    return long_slab(here, positions, queries, block, weights, parts, reach, length)


def solution(mesh):
    return jax.shard_map(
        on_device,
        mesh=mesh,
        in_specs=(
            P("seq", "head"),
            P("seq", "head"),
            P("seq", "head"),
            P("seq", "head"),
            P("seq"),
            P(),
            P("head", None, None),
            P("head", None, None),
            P("head", None, None),
            P("head", None, None),
        ),
        out_specs=P("seq", "head"),
        check_vma=False,
    )
```

```python
import functools

import jax
import jax.numpy as jnp
from jax import lax
from jax.experimental import pallas as pl
from jax.experimental.pallas import tpu as pltpu
from jax.sharding import PartitionSpec as P

QH = 16
DK = 192
DV = 128
STRIDE = 16
BLOCK = 32
WINDOW = 512
LANES = 128
PAD = 256
GROUP = 2
LATE_GROUP = 8
MID_BLOCKS = 3
VMEM_LIMIT = 24 << 20
MOST_SLOTS = 8

NEG = -1e30
SCALE = DK ** (-0.5) * 1.4426950408889634

f32 = jnp.float32
bf16 = jnp.bfloat16


def up(value, step):
    return -(-value // step) * step


def swap(value, axis, by):
    length = lax.axis_size(axis)
    return lax.ppermute(value, axis, [(i, i ^ by) for i in range(length)])


def turn(value, axis, by):
    length = lax.axis_size(axis)
    return lax.ppermute(value, axis, [(i, (i + by) % length) for i in range(length)])


def dot(left, right):
    return jnp.dot(left, right, preferred_element_type=f32)


def dot_t(left, right):
    return lax.dot_general(left, right, (((1,), (1,)), ((), ())), preferred_element_type=f32)


def place_hbm(value):
    return pltpu.with_memory_space_constraint(value, pltpu.HBM)


def logits_of(features, columns, total):
    total[...] = lax.dot_general(
        columns[...], features[...], (((0,), (1,)), ((), ())), preferred_element_type=f32
    )


def halve(bit, rows, keep, send):
    size = keep.shape[0]
    keep[...] = rows[pl.ds(pl.multiple_of(bit * size, size), size), :]
    send[...] = rows[pl.ds(pl.multiple_of((1 - bit) * size, size), size), :]


def feature_copies(group, features_hbm, columns_hbm, features, columns, sems):
    depth = features.shape[1]
    first = pl.multiple_of(group * depth, LANES)
    return [
        pltpu.make_async_copy(features_hbm, features, sems.at[0]),
        pltpu.make_async_copy(columns_hbm.at[pl.ds(first, depth), :], columns, sems.at[1]),
    ]


def logit_kernel(heads, group, features_hbm, columns_hbm, *refs):
    outs, (features, columns, total, sems) = refs[:heads], refs[heads:]
    copies = feature_copies(group[0], features_hbm, columns_hbm, features, columns, sems)
    for copy in copies:
        copy.start()
    for copy in copies:
        copy.wait()
    logits_of(features, columns, total)
    for step, out in enumerate(outs):
        other = group[0] ^ step if heads & (heads - 1) == 0 else lax.rem(group[0] + step, heads)
        out[...] = total[pl.ds(pl.multiple_of(other * (2 * QH), 2 * QH), 2 * QH), :]


def prepare_kernel(kept, offsets, codes, here_ref, group_ref, features_hbm, columns_hbm, positions_hbm, *refs):
    here, group = here_ref[0], group_ref[0]
    sources = refs[:kept]
    keep, send = refs[kept : kept + 2]
    bias, some, second = refs[kept + 2 : kept + 2 + 3]
    places = refs[kept + 2 + 3 : 2 * kept + 2 + 1]
    features, columns, total, positions, sems = refs[2 * kept + 2 + 1 :]
    places = [*places, second.at[pl.ds(0, DK), :], second.at[pl.ds(DK, sources[-1].shape[0]), :]]
    copies = feature_copies(group, features_hbm, columns_hbm, features, columns, sems)
    copies.append(pltpu.make_async_copy(positions_hbm, positions, sems.at[2]))
    copies += [
        pltpu.make_async_copy(source, place, sems.at[3 + i])
        for i, (source, place) in enumerate(zip(sources, places))
    ]
    for copy in copies:
        copy.start()
    for copy in copies[:3]:
        copy.wait()
    logits_of(features, columns, total)
    halve(group // (keep.shape[0] // (2 * QH)), total, keep, send)
    count = positions.shape[1]
    lengths = jnp.broadcast_to(positions[...].astype(f32), (count, count)).T.astype(jnp.int32)
    token = here * count + lax.broadcasted_iota(jnp.int32, (count, count), 0)
    lane = lax.broadcasted_iota(jnp.int32, (count, count), 1)
    for step, offset in enumerate(offsets):
        key = (here - offset) * count + lane
        seen = (key <= token) & (key > token - WINDOW) & (key >= token - lengths) & (key >= 0)
        bias[:, step * count : (step + 1) * count] = jnp.where(seen, 0.0, NEG)
    near = len(offsets) * count
    most = jnp.full((count, LANES), NEG, f32)
    for start in range(near, bias.shape[1], LANES):
        code = start - near + lax.broadcasted_iota(jnp.int32, (count, LANES), 1)
        token = here * count + lax.broadcasted_iota(jnp.int32, (count, LANES), 0)
        length = lengths if count == LANES else jnp.broadcast_to(lengths[:, :1], (count, LANES))
        first = STRIDE * code
        seen = (first + (BLOCK - 1) <= token) & (first >= token - length) & (code < codes)
        part = jnp.where(seen, 0.0, NEG)
        bias[:, start : start + LANES] = part
        most = jnp.maximum(most, part)
    some[...] = jnp.where(
        jnp.broadcast_to(jnp.max(most, axis=1, keepdims=True), (count, LANES)) > 0.5 * NEG, 1.0, 0.0
    )
    for copy in copies[3:]:
        copy.wait()


def gate_shapes(count, depth, columns):
    return [
        pltpu.VMEM((count, depth), bf16),
        pltpu.VMEM((depth, columns), bf16),
        pltpu.VMEM((columns, count), f32),
    ]


def gate_logits(features, gate_weight, group, heads):
    count, depth = features.shape
    vmem, hbm = pl.BlockSpec(memory_space=pltpu.VMEM), pl.BlockSpec(memory_space=pltpu.HBM)
    return pl.pallas_call(
        functools.partial(logit_kernel, heads),
        in_specs=[pl.BlockSpec(memory_space=pltpu.SMEM), hbm, hbm],
        out_specs=[vmem] * heads,
        out_shape=[jax.ShapeDtypeStruct((2 * QH, count), f32)] * heads,
        scratch_shapes=gate_shapes(count, depth, gate_weight.shape[1])
        + [pltpu.SemaphoreType.DMA((2,))],
        compiler_params=pltpu.CompilerParams(vmem_limit_bytes=VMEM_LIMIT),
        name="gate_logits",
    )(group[None], features, gate_weight)


def prepare(here, group, positions, features, gate_weight, heads, offsets, codes, kept):
    count, depth = features.shape
    vmem, hbm = pl.BlockSpec(memory_space=pltpu.VMEM), pl.BlockSpec(memory_space=pltpu.HBM)
    wide = len(offsets) * count + up(codes, LANES)
    last = kept[-2:]
    made = pl.pallas_call(
        functools.partial(prepare_kernel, len(kept), offsets, codes),
        in_specs=[pl.BlockSpec(memory_space=pltpu.SMEM)] * 2 + [hbm] * (3 + len(kept)),
        out_specs=[vmem] * (3 + len(kept)),
        out_shape=[jax.ShapeDtypeStruct((heads * QH, count), f32)] * 2
        + [
            jax.ShapeDtypeStruct((count, wide), f32),
            jax.ShapeDtypeStruct((count, LANES), f32),
            jax.ShapeDtypeStruct((last[0].shape[0] + last[1].shape[0], last[1].shape[1]), bf16),
        ]
        + [jax.ShapeDtypeStruct(value.shape, value.dtype) for value in kept[:-2]],
        scratch_shapes=gate_shapes(count, depth, gate_weight.shape[1])
        + [pltpu.VMEM((1, count), jnp.int32), pltpu.SemaphoreType.DMA((3 + len(kept),))],
        compiler_params=pltpu.CompilerParams(vmem_limit_bytes=VMEM_LIMIT),
        name="prepare",
    )(
        here[None],
        group[None],
        *[place_hbm(value) for value in (features, gate_weight, positions[None, :], *kept)],
    )
    return made[:2], made[2:]


def exchange(parts):
    heads = len(parts)
    if heads & (heads - 1) == 0:
        return [parts[0]] + [swap(parts[d], "head", d) for d in range(1, heads)]
    return [parts[0]] + [turn(parts[d], "head", d) for d in range(1, heads)]


def gelu(x):
    return 0.5 * x * (1.0 + jnp.tanh(0.7978845608028654 * (x + 0.044715 * x * x * x)))


def halves(rows, planes, size, weight, width):
    strides = size // STRIDE
    total = jnp.zeros((strides, 2 * LANES), f32)
    for place in range(STRIDE):
        part = jnp.concatenate(
            [rows[pl.ds(plane * size + place, strides, stride=STRIDE), :] for plane in planes], 1
        ).astype(bf16)[:, :width]
        both = jnp.concatenate(
            [
                weight[pl.ds(place * width, width), :],
                weight[pl.ds((STRIDE + place) * width, width), :],
            ],
            1,
        )
        total = total + dot(part, both)
    return total


def hidden_of(first, second):
    strides = first.shape[0]
    later = pltpu.roll(second, strides - 1, axis=0)
    last = lax.broadcasted_iota(jnp.int32, later.shape, 0) == strides - 1
    return gelu(first + jnp.where(last, 0.0, later)).astype(bf16)


def unpack(block, rows, size, at):
    count = block.shape[1]
    for plane in range(2):
        part = block[plane * LANES : min((plane + 1) * LANES, DK), :].astype(f32).T
        rows[pl.ds(plane * size + at, count), : part.shape[1]] = part
    rows[pl.ds(2 * size + at, count), :] = block[DK:, :].astype(f32)


def codes_of(rows, size, key_in, key_out, value_in, value_out):
    shares = halves(rows, (0, 1), size, key_in, DK)
    key_hidden = hidden_of(shares[:, :LANES], shares[:, LANES:])
    code_keys = dot_t(key_out[...], key_hidden).astype(bf16)
    shares = halves(rows, (2,), size, value_in, DV)
    value_hidden = hidden_of(shares[:, :LANES], shares[:, LANES:])
    code_values = dot(value_hidden, value_out[...]).astype(bf16)
    return code_keys, code_values


def attend_body(
    here, count, reach, get_block, code_keys, code_values, codes, positions, q, parts, out, scratch
):
    even, odd, near_values, far_values, near_bias, far_bias, gates = scratch
    near = (reach + 1) * count
    far = even.shape[1] - near
    lengths = jnp.broadcast_to(positions[...].astype(f32), (count, count)).T.astype(jnp.int32)

    def lens(width):
        return jnp.concatenate([lengths] * (width // count), 1) if width > count else lengths

    def ids(width, axis):
        return lax.broadcasted_iota(jnp.int32, (count, width), axis)

    token = here * count + ids(near, 0)
    key = (here - reach) * count + ids(near, 1)
    seen = (key <= token) & (key > token - WINDOW) & (key >= token - lens(near)) & (key >= 0)
    near_bias[...] = jnp.where(seen, 0.0, NEG)
    token = here * count + ids(far, 0)
    first = STRIDE * ids(far, 1)
    seen = (first + (BLOCK - 1) <= token) & (first >= token - lens(far)) & (ids(far, 1) < codes)
    far_bias[...] = jnp.where(seen, 0.0, NEG)
    some = jnp.max(jnp.where(seen, 1.0, 0.0), axis=1, keepdims=True)

    total = parts[0][...]
    for part in parts[1:]:
        total = total + part[...]
    total = jax.nn.sigmoid(total)
    total = jnp.concatenate([total, jnp.zeros((LANES - 2 * QH, count), f32)], 0).T
    coarse_lane = lax.broadcasted_iota(jnp.int32, total.shape, 1) < QH
    gates[...] = jnp.where(coarse_lane, total * some, total)

    even[DK:, :] = jnp.zeros((PAD - DK, near + far), bf16)
    odd[: PAD - DK, :] = jnp.zeros((PAD - DK, near + far), bf16)
    near_values[:, DV:] = jnp.ones((near, DV), bf16)
    far_values[:, DV:] = jnp.ones((far, DV), bf16)
    for step in range(reach + 1):
        block = get_block(jnp.maximum(here - reach + step, 0), step)
        lanes = slice(step * count, (step + 1) * count)
        even[:DK, lanes] = block[:DK, :]
        odd[PAD - DK :, lanes] = block[:DK, :]
        near_values[lanes, :DV] = block[DK:, :]
    even[:DK, near:] = code_keys
    odd[PAD - DK :, near:] = code_keys
    far_values[:, :DV] = code_values

    pair = 2 * DK
    for side in (0, 1):
        keys = (even, odd)[side]
        for chunk in range(0, QH // 2, GROUP):
            rows = jnp.concatenate(
                [
                    q[:, (chunk + j) * pair + side * LANES : (chunk + j) * pair + side * LANES + PAD]
                    for j in range(GROUP)
                ],
                0,
            )
            scores = dot(rows, keys[...])

            def branch(scores, bias, values):
                width = scores.shape[1]
                scores = scores.reshape(GROUP, count, width) + bias[...][None]
                top = jnp.max(scores, axis=2, keepdims=True)
                weights = jnp.exp2((scores - top) * SCALE).astype(bf16)
                summed = dot(weights.reshape(GROUP * count, width), values[...])
                return summed[:, :DV] / jnp.maximum(summed[:, DV:], 1.0)

            local = branch(scores[:, :near], near_bias, near_values)
            coarse = branch(scores[:, near:], far_bias, far_values)
            for j in range(GROUP):
                head = 2 * (chunk + j) + side
                at = slice(j * count, (j + 1) * count)
                mixed = (
                    gates[:, head : head + 1] * coarse[at]
                    + gates[:, QH + head : QH + head + 1] * local[at]
                )
                out[:, head * DV : (head + 1) * DV] = mixed.astype(bf16)


def attend_scratch(count, reach, far):
    near = (reach + 1) * count
    return [
        pltpu.VMEM((PAD, near + far), bf16),
        pltpu.VMEM((PAD, near + far), bf16),
        pltpu.VMEM((near, 2 * DV), bf16),
        pltpu.VMEM((far, 2 * DV), bf16),
        pltpu.VMEM((count, near), f32),
        pltpu.VMEM((count, far), f32),
        pltpu.VMEM((count, LANES), f32),
    ]


def gate_columns(parts, some):
    total = parts[0][...]
    for part in parts[1:]:
        total = total + part[...]
    total = jax.nn.sigmoid(total)
    total = jnp.concatenate([total, jnp.zeros((LANES - 2 * QH, total.shape[1]), f32)], 0).T
    coarse_lane = lax.broadcasted_iota(jnp.int32, total.shape, 1) < QH
    return jnp.where(coarse_lane, total * some, total)


def fill_keys(even, odd, lanes, keys):
    even[:DK, lanes] = keys
    even[DK:, lanes] = jnp.zeros((PAD - DK, keys.shape[1]), bf16)
    odd[: PAD - DK, lanes] = jnp.zeros((PAD - DK, keys.shape[1]), bf16)
    odd[PAD - DK :, lanes] = keys


def query_rows(q, side, chunk, heads):
    starts = [(chunk + j) * 2 * DK + side * LANES for j in range(heads)]
    return jnp.concatenate([q[:, start : start + PAD] for start in starts], 0)


def place_of(here, offset):
    block = here - offset
    return jnp.where(block >= 0, (block ^ here) >> 1, 0)


def early_kernel(slots, count, offsets, here_ref, q, bias, *refs):
    blocks, (summed, tops) = refs[:slots], refs[slots : slots + 2]
    held, even, odd, values = refs[slots + 2 :]
    here = here_ref[0]
    for i, block in enumerate(blocks):
        held[i] = block[...]
    near = len(offsets) * count
    for step, offset in enumerate(offsets):
        block = held[place_of(here, offset)]
        lanes = slice(step * count, (step + 1) * count)
        fill_keys(even, odd, lanes, block[:DK, :])
        values[lanes, :DV] = block[DK:, :]
    values[:, DV:] = jnp.ones((near, DV), bf16)
    for side in (0, 1):
        for chunk in range(0, QH // 2, GROUP):
            scores = dot(query_rows(q, side, chunk, GROUP), (even, odd)[side][...])
            scores = scores.reshape(GROUP, count, near) + bias[:, :near][None]
            top = jnp.max(scores, axis=2, keepdims=True)
            weights = jnp.exp2((scores - top) * SCALE).astype(bf16)
            at = pl.ds((side * QH // 2 + chunk) * count, GROUP * count)
            summed[at, :] = dot(weights.reshape(GROUP * count, near), values[...])
            tops[at, :] = jnp.broadcast_to(top, (GROUP, count, LANES)).reshape(GROUP * count, LANES)


def split(refs):
    size = DK + DV
    return [ref.at[pl.ds(at, size), :] for ref in refs for at in range(0, ref.shape[0], size)]


def codes_from(key_shares, value_shares, second, far):
    key_hidden = hidden_of(key_shares[:, :LANES], key_shares[:, LANES:])
    keys = dot_t(second[:DK, :], key_hidden).astype(bf16)
    value_hidden = hidden_of(value_shares[:, :LANES], value_shares[:, LANES:])
    values = dot(value_hidden, second[DK:, :]).astype(bf16)
    codes = values.shape[0]
    if far > codes:
        keys = jnp.concatenate([keys, jnp.zeros((DK, far - codes), bf16)], 1)
        values = jnp.concatenate([values, jnp.zeros((far - codes, DV), bf16)], 0)
    return keys, values


def share_rows(here, slot, strides):
    return pl.ds(pl.multiple_of((here ^ slot) * strides, strides), strides)


def mid_kernel(buffers, slots, count, here_ref, second, key_in, value_in, *refs):
    blocks = list(refs[:slots]) + split(refs[slots : slots + buffers])
    key_shares, value_shares, code_keys, code_values, rows = refs[slots + buffers :]
    here = here_ref[0]
    strides = count // STRIDE
    total = len(blocks) * count
    for i, block in enumerate(blocks):
        unpack(block, rows, total, i * count)
    key_mid = halves(rows, (0, 1), total, key_in, DK)
    value_mid = halves(rows, (2,), total, value_in, DV)
    for i in range(2 * slots):
        mine = slice(i * strides, (i + 1) * strides)
        at = share_rows(here, 2 * i if i < slots else 2 * (i - slots) + 1, strides)
        known = i < len(blocks)
        key_shares[at, :] = key_mid[mine] if known else jnp.zeros((strides, 2 * LANES), f32)
        value_shares[at, :] = value_mid[mine] if known else jnp.zeros((strides, 2 * LANES), f32)
    code_keys[...], code_values[...] = codes_from(key_shares, value_shares, second, code_values.shape[0])


def late_kernel(
    buffers, slots, heads, count, offsets, done, here_ref, q, bias, some, second, key_in, value_in,
    mid_key_shares, mid_value_shares, code_keys, code_values, summed, tops, *refs
):
    came, parts, out = refs[:buffers], refs[buffers : buffers + heads], refs[buffers + heads]
    held, rows, even, odd, values, far_values, key_shares, value_shares, gates = refs[buffers + heads + 1 :]
    blocks = split(came)
    here = here_ref[0]
    strides = count // STRIDE
    for i, block in enumerate(blocks):
        held[i] = block[...]
    near = len(offsets) * count
    for step, offset in enumerate(offsets):
        block = held[place_of(here, offset)]
        lanes = slice(step * count, (step + 1) * count)
        fill_keys(even, odd, lanes, block[:DK, :])
        values[lanes, :DV] = block[DK:, :]
    values[:, DV:] = jnp.ones((near, DV), bf16)
    far = far_values.shape[0]
    far_values[:, DV:] = jnp.ones((far, DV), bf16)

    def put(keys, found):
        fill_keys(even, odd, slice(near, near + far), keys)
        far_values[:, :DV] = found

    last = [i for i in range(slots) if i >= MID_BLOCKS]
    needed = functools.reduce(jnp.logical_or, [(here ^ (2 * i + 1)) < here for i in last], False)

    @pl.when(needed)
    def _():
        total = len(last) * count
        for j, i in enumerate(last):
            unpack(blocks[i], rows, total, j * count)
        key_last = halves(rows, (0, 1), total, key_in, DK)
        value_last = halves(rows, (2,), total, value_in, DV)
        key_shares[...] = mid_key_shares[...]
        value_shares[...] = mid_value_shares[...]
        for j, i in enumerate(last):
            at = share_rows(here, 2 * i + 1, strides)
            key_shares[at, :] = key_last[j * strides : (j + 1) * strides]
            value_shares[at, :] = value_last[j * strides : (j + 1) * strides]
        put(*codes_from(key_shares, value_shares, second, far))

    @pl.when(jnp.logical_not(needed))
    def _():
        put(code_keys[...], code_values[...])

    gates[...] = gate_columns(parts, some[...])
    size = LATE_GROUP * count

    def normal(summed):
        return summed[:, :DV] / jnp.maximum(summed[:, DV:], 1.0)

    def attend():
        for side in (0, 1):
            for chunk in range(0, QH // 2, LATE_GROUP):
                at = pl.ds((side * QH // 2 + chunk) * count, size)
                scores = dot(query_rows(q, side, chunk, LATE_GROUP), (even, odd)[side][...])
                scores = scores.reshape(LATE_GROUP, count, near + far) + bias[:, done:][None]
                local, coarse = scores[:, :, :near], scores[:, :, near:]
                before = tops[at, :].reshape(LATE_GROUP, count, LANES)
                top = jnp.maximum(before, jnp.max(local, axis=2, keepdims=True))
                tops_near = jnp.concatenate([top] * (near // LANES), 2)
                weights = jnp.exp2((local - tops_near) * SCALE).astype(bf16)
                fade = jnp.exp2((before - top) * SCALE).reshape(size, LANES)
                old = summed[at, :] * jnp.concatenate([fade] * (2 * DV // LANES), 1)
                local = normal(old + dot(weights.reshape(size, near), values[...]))
                top = jnp.max(coarse, axis=2, keepdims=True)
                weights = jnp.exp2((coarse - top) * SCALE).astype(bf16)
                coarse = normal(dot(weights.reshape(size, far), far_values[...]))
                for j in range(LATE_GROUP):
                    head = 2 * (chunk + j) + side
                    at = slice(j * count, (j + 1) * count)
                    mixed = (
                        gates[:, head : head + 1] * coarse[at]
                        + gates[:, QH + head : QH + head + 1] * local[at]
                    )
                    out[:, head * DV : (head + 1) * DV] = mixed.astype(bf16)

    pl.when(here >= 0)(attend)


def hold_kernel(value, out):
    out[...] = value[...]


def hold(value):
    vmem = pl.BlockSpec(memory_space=pltpu.VMEM)
    return pl.pallas_call(
        hold_kernel,
        in_specs=[vmem],
        out_specs=vmem,
        out_shape=jax.ShapeDtypeStruct(value.shape, value.dtype),
        compiler_params=pltpu.CompilerParams(vmem_limit_bytes=VMEM_LIMIT),
        name="hold",
    )(value)


def fold_kernel(bit, mine, came, keep, send, total):
    total[...] = mine[...] + came[...]
    halve((lax.axis_index("head") >> bit) & 1, total, keep, send)


def fold(bit, mine, came):
    rows, count = mine.shape
    vmem = pl.BlockSpec(memory_space=pltpu.VMEM)
    return pl.pallas_call(
        functools.partial(fold_kernel, bit),
        in_specs=[vmem] * 2,
        out_specs=[vmem] * 2,
        out_shape=[jax.ShapeDtypeStruct((rows // 2, count), f32)] * 2,
        scratch_shapes=[pltpu.VMEM((rows, count), f32)],
        compiler_params=pltpu.CompilerParams(vmem_limit_bytes=VMEM_LIMIT),
        name="fold",
    )(mine, came)


def join_kernel(*refs):
    *blocks, out = refs
    size = blocks[0].shape[0]
    for i, block in enumerate(blocks):
        out[i * size : (i + 1) * size, :] = block[...]


def join(blocks):
    size, count = blocks[0].shape
    vmem = pl.BlockSpec(memory_space=pltpu.VMEM)
    return pl.pallas_call(
        join_kernel,
        in_specs=[vmem] * len(blocks),
        out_specs=vmem,
        out_shape=jax.ShapeDtypeStruct((len(blocks) * size, count), bf16),
        compiler_params=pltpu.CompilerParams(vmem_limit_bytes=VMEM_LIMIT),
        name="join",
    )(*blocks)


def small_slab(here, group, positions, queries, block, features, gate_weight, weights, length, heads, reach):
    count = queries.shape[0]
    codes = length * count // STRIDE
    far = up(codes, LANES)
    first = tuple(range(reach - reach % 2, -1, -2))
    then = tuple(range(reach - (reach + 1) % 2, 0, -2))
    key_in, key_out, value_in, value_out = weights
    slots = {0: block}
    for d in range(2, length, 2):
        slots[d] = swap(block, "seq", d)
    parts, (bias, some, second, queries, key_in, value_in) = prepare(
        here, group, positions, features, gate_weight, heads, first + then, codes,
        (queries, key_in, value_in, key_out, value_out),
    )
    for d in range(2, length, 2):
        slots[d] = lax.optimization_barrier((slots[d], parts))[0]
    across = [swap(block, "seq", 1)]
    across.append(swap(join([slots[d] for d in range(2, min(length, 6), 2)]), "seq", 1))
    for d in range(6, length, 2):
        across.append(swap(slots[d], "seq", 1))
    for bit in reversed(range(heads.bit_length() - 1)):
        mine, send = (parts[0], hold(parts[1])) if 2 << bit == heads else fold(bit, *parts)
        parts = [mine, swap(send, "head", 1 << bit)]
    half = length // 2
    smem, vmem = pl.BlockSpec(memory_space=pltpu.SMEM), pl.BlockSpec(memory_space=pltpu.VMEM)
    params = pltpu.CompilerParams(vmem_limit_bytes=VMEM_LIMIT)
    rows = [
        pltpu.VMEM((half, DK + DV, count), bf16),
        pltpu.VMEM((3 * half * count, LANES), f32),
    ]
    near = len(first) * count
    summed, tops = pl.pallas_call(
        functools.partial(early_kernel, half, count, first),
        in_specs=[smem] + [vmem] * (2 + half),
        out_specs=[vmem] * 2,
        out_shape=[
            jax.ShapeDtypeStruct((QH * count, 2 * DV), f32),
            jax.ShapeDtypeStruct((QH * count, LANES), f32),
        ],
        scratch_shapes=rows[:1]
        + [pltpu.VMEM((PAD, near), bf16)] * 2
        + [pltpu.VMEM((near, 2 * DV), bf16)],
        compiler_params=params,
        cost_estimate=pl.CostEstimate(flops=4 << 30, transcendentals=1 << 20, bytes_accessed=1 << 22),
        name="early",
    )(here[None], queries, bias, *[slots[d] for d in range(0, length, 2)])
    done = near
    near = len(then) * count
    ahead = [value for value in across if value is not across[-1]] if len(across) > 2 else across
    made = pl.pallas_call(
        functools.partial(mid_kernel, len(ahead), half, count),
        in_specs=[smem] + [vmem] * (3 + half + len(ahead)),
        out_specs=[vmem] * 4,
        out_shape=[jax.ShapeDtypeStruct((codes, 2 * LANES), f32)] * 2
        + [jax.ShapeDtypeStruct((DK, far), bf16), jax.ShapeDtypeStruct((far, DV), bf16)],
        scratch_shapes=[pltpu.VMEM((3 * 2 * half * count, LANES), f32)],
        compiler_params=params,
        name="mid",
    )(here[None], second, key_in, value_in, *[slots[d] for d in range(0, length, 2)], *ahead)
    return pl.pallas_call(
        functools.partial(late_kernel, len(across), half, len(parts), count, then, done),
        in_specs=[smem] + [vmem] * (12 + len(across) + len(parts)),
        out_specs=vmem,
        out_shape=jax.ShapeDtypeStruct((count, QH * DV), bf16),
        scratch_shapes=rows
        + [pltpu.VMEM((PAD, near + far), bf16)] * 2
        + [pltpu.VMEM((near, 2 * DV), bf16), pltpu.VMEM((far, 2 * DV), bf16)]
        + [pltpu.VMEM((codes, 2 * LANES), f32)] * 2
        + [pltpu.VMEM((count, LANES), f32)],
        compiler_params=params,
        name="late",
    )(
        here[None], queries, bias, some, second, key_in, value_in, *made, summed, tops,
        *across, *parts,
    )


def codes_kernel(before, block, key_in, key_out, value_in, value_out, out, rows):
    count = block.shape[1]
    unpack(before[...], rows, 2 * count, 0)
    unpack(block[...], rows, 2 * count, count)
    code_keys, code_values = codes_of(rows, 2 * count, key_in, key_out, value_in, value_out)
    out[:, :DK] = code_keys.astype(f32).T
    out[:, DK:] = code_values.astype(f32)


def near_kernel(heads, count, reach, codes, here_ref, *refs):
    positions, q = refs[:2]
    blocks = refs[2 : 3 + reach]
    code_keys, code_values = refs[3 + reach : 5 + reach]
    parts = refs[5 + reach : 5 + reach + heads]
    out = refs[5 + reach + heads]
    attend_body(
        here_ref[0], count, reach, lambda at, step: blocks[step][...], code_keys[...], code_values[...],
        codes, positions, q, parts, out, refs[6 + reach + heads :],
    )


def long_slab(here, positions, queries, block, weights, parts, reach, length):
    count = queries.shape[0]
    strides = count // STRIDE
    smem, vmem = pl.BlockSpec(memory_space=pltpu.SMEM), pl.BlockSpec(memory_space=pltpu.VMEM)
    earlier = [turn(block, "seq", reach - k) for k in range(reach)]
    made = pl.pallas_call(
        codes_kernel,
        in_specs=[vmem] * 6,
        out_specs=vmem,
        out_shape=jax.ShapeDtypeStruct((2 * strides, DK + DV), f32),
        scratch_shapes=[pltpu.VMEM((6 * count, LANES), f32)],
        name="codes",
    )(earlier[-1], block, *weights)
    mine = made[strides - 1 : 2 * strides - 1].astype(bf16)
    every = lax.all_gather(mine, "seq", axis=0, tiled=True)[1:]
    codes = length * count // STRIDE
    far = up(codes, LANES)
    every = jnp.concatenate([every, jnp.zeros((far - every.shape[0], DK + DV), bf16)], 0)
    return pl.pallas_call(
        functools.partial(near_kernel, len(parts), count, reach, codes),
        in_specs=[smem] + [vmem] * (5 + reach + len(parts)),
        out_specs=vmem,
        out_shape=jax.ShapeDtypeStruct((count, QH * DV), bf16),
        scratch_shapes=attend_scratch(count, reach, far),
        name="long_slab",
    )(here[None], positions[None, :], queries, *earlier, block, every[:, :DK].T, every[:, DK:], *parts)


def on_device(
    queries, keys, values, features, positions, gate_weight, key_in, key_out, value_in, value_out
):
    count = keys.shape[0]
    length, heads = lax.axis_size("seq"), lax.axis_size("head")
    here = lax.axis_index("seq")
    group = lax.axis_index("head")
    reach = -(-WINDOW // count)
    block = jnp.concatenate([keys.T, values], 0)
    weights = (key_in[0], key_out[0].T, value_in[0], value_out[0])
    if 1 < length <= MOST_SLOTS and length & (length - 1) == 0 and heads > 1 and heads & (heads - 1) == 0:
        return small_slab(
            here, group, positions, queries, block, features, gate_weight, weights, length, heads, reach
        )
    parts = exchange(gate_logits(features, gate_weight, group, heads))
    return long_slab(here, positions, queries, block, weights, parts, reach, length)


def solution(mesh):
    return jax.shard_map(
        on_device,
        mesh=mesh,
        in_specs=(
            P("seq", "head"),
            P("seq", "head"),
            P("seq", "head"),
            P("seq", "head"),
            P("seq"),
            P(),
            P("head", None, None),
            P("head", None, None),
            P("head", None, None),
            P("head", None, None),
        ),
        out_specs=P("seq", "head"),
        check_vma=False,
    )
```
